16 devices in a mesh: dp: 2 (over y, z), ep: 8 (over x, core).
Axes of the slice: x: 4, y: 2, z: 1, core: 2. Of those that a mesh axis runs over, the one named last changes fastest.
The devices are a block of a 4x4x8 slice.
Arguments:
- tokens: bfloat16 [65536, 768], P(('dp', 'ep')), parts along dimension 0
- topk_idx: int32 [65536, 1], P(('dp', 'ep')), parts along dimension 0
- topk_w: float32 [65536, 1], P(('dp', 'ep')), parts along dimension 0
- w_up: bfloat16 [8, 17, 768, 3072], P('ep')
- w_down: bfloat16 [8, 17, 3072, 768], P('ep')
- slot_expert: int32 [8, 17], replicated
Outputs:
- output: bfloat16 [65536, 768], P(('dp', 'ep')), parts along dimension 0
There are 2 independent parts. The reference program is written for one: setup_inputs(seed, part) draws one part's arguments, and reference() takes and returns one part's arrays. A program takes and returns all parts, laid end to end along the dimension named above; an argument that names none is the same for every part.
All inputs are finite; a program needn't handle non-finite values.
Results may differ from the reference program's by a relative error of at most 0.001.
Values are sent between devices in bfloat16 or wider.
A program may use at most 768 MiB of HBM per device.

```python
import jax
import jax.numpy as jnp
from jax import lax
import numpy as np

GROUP = 8
TOK_DEV = 4096
D_MODEL = 768
D_FF = 3072
EXPERTS = 128
TOP = 1

PER_DEV = EXPERTS // GROUP
SLOTS = PER_DEV + 1
N_UNITS = GROUP * SLOTS
PAIRS_DEV = TOK_DEV * TOP
BASE_LOAD = PAIRS_DEV // N_UNITS
BLOCK = max(8, (GROUP * PAIRS_DEV) // N_UNITS)
N_BLOCKS = (GROUP * PAIRS_DEV) // BLOCK + EXPERTS


def base_table():
    dev_ids = np.arange(GROUP)
    hot_dev = (3 * (dev_ids // 3) + 3) % GROUP
    spare_exp = hot_dev * PER_DEV + PER_DEV - 1
    primary = np.arange(EXPERTS).reshape(GROUP, PER_DEV)
    return np.concatenate([primary, spare_exp[:, None]], axis=1).astype(np.int32)


def draw_table(key_tab):
    key_dev, key_col, key_lab = jax.random.split(key_tab, 3)
    relabel = jax.random.permutation(key_lab, EXPERTS).astype(jnp.int32)
    dev_perm = jax.random.permutation(key_dev, GROUP)
    col_perm = jax.random.permutation(key_col, SLOTS)
    slot_table = jnp.asarray(base_table())[dev_perm][:, col_perm]
    return relabel[slot_table], relabel


def draw_loads(key_load):
    key_perm, key_shift = jax.random.split(key_load)
    unit_order = 1 + jax.random.permutation(key_perm, N_UNITS - 1)
    shift_amt = jax.random.randint(key_shift, ((N_UNITS - 2) // 2,), 0, BASE_LOAD // 2 + 1, dtype=jnp.int32)
    spread = BASE_LOAD // 2 + 1
    unit_loads = jnp.full((N_UNITS,), BASE_LOAD, jnp.int32)
    unit_loads = unit_loads.at[0].add(spread).at[unit_order[0]].add(-spread)
    unit_loads = unit_loads.at[unit_order[1::2]].add(shift_amt).at[unit_order[2::2]].add(-shift_amt)
    return unit_loads.at[unit_order[:PAIRS_DEV - N_UNITS * BASE_LOAD]].add(1)


def draw_routing(key_src, unit_expert):
    key_load, key_tok = jax.random.split(key_src)
    counts = jax.ops.segment_sum(draw_loads(key_load), unit_expert, num_segments=EXPERTS)
    bounds = jnp.cumsum(counts)
    sorted_exp = jnp.searchsorted(bounds, jnp.arange(PAIRS_DEV, dtype=jnp.int32), side='right').astype(jnp.int32)
    routes = sorted_exp.reshape(TOP, TOK_DEV).T
    return routes[jax.random.permutation(key_tok, TOK_DEV)]


def setup_inputs(seed: int = 0, part: int = 0) -> dict:
    root_key = jax.random.key(seed)
    key_tab, key_up, key_down, key_part = jax.random.split(root_key, 4)
    slot_expert, relabel = draw_table(key_tab)
    unit_expert = relabel[jnp.asarray(base_table()).reshape(-1)]
    up_base = jax.random.normal(key_up, (EXPERTS, D_MODEL, D_FF), jnp.float32) * D_MODEL ** -0.5
    down_base = jax.random.normal(key_down, (EXPERTS, D_FF, D_MODEL), jnp.float32) * D_FF ** -0.5
    key_grp = jax.random.fold_in(key_part, part)
    key_tokens, key_gate, key_route = jax.random.split(key_grp, 3)
    tokens = jax.random.normal(key_tokens, (GROUP * TOK_DEV, D_MODEL), jnp.float32)
    topk_w = jax.random.uniform(key_gate, (GROUP * TOK_DEV, TOP), jnp.float32, 0.3, 1.0)
    src_keys = jax.random.split(key_route, GROUP)
    topk_idx = jax.vmap(draw_routing, in_axes=(0, None))(src_keys, unit_expert)
    return {'tokens': tokens.astype(jnp.bfloat16), 'topk_idx': topk_idx.reshape(GROUP * TOK_DEV, TOP), 'topk_w': topk_w, 'w_up': up_base.astype(jnp.bfloat16)[slot_expert], 'w_down': down_base.astype(jnp.bfloat16)[slot_expert], 'slot_expert': slot_expert}


def reference(tokens, topk_idx, topk_w, w_up, w_down, slot_expert):
    n_tok = tokens.shape[0]
    n_pairs = n_tok * TOP
    table_flat = slot_expert.reshape(-1)
    first_slot = jax.ops.segment_min(jnp.arange(N_UNITS, dtype=jnp.int32), table_flat, num_segments=EXPERTS)
    up_flat = w_up.reshape(N_UNITS, D_MODEL, D_FF)
    down_flat = w_down.reshape(N_UNITS, D_FF, D_MODEL)
    flat_exp = topk_idx.reshape(-1)
    flat_gate = topk_w.reshape(-1)
    pair_order = jnp.argsort(flat_exp, stable=True)
    counts = jnp.bincount(flat_exp, length=EXPERTS)
    starts = jnp.cumsum(counts) - counts
    exp_blocks = (counts + BLOCK - 1) // BLOCK
    block_end = jnp.cumsum(exp_blocks)
    block_start = block_end - exp_blocks
    lane_ids = jnp.arange(BLOCK)

    def block_step(acc_sum, block_id):
        exp_id = jnp.minimum(jnp.searchsorted(block_end, block_id, side='right'), EXPERTS - 1)
        offsets = (block_id - block_start[exp_id]) * BLOCK + lane_ids
        is_valid = (offsets < counts[exp_id]) & (block_id < block_end[EXPERTS - 1])
        pair_ids = pair_order[jnp.clip(starts[exp_id] + offsets, 0, n_pairs - 1)]
        tok_ids = pair_ids // TOP
        slot_id = first_slot[exp_id]
        pre_act = jnp.dot(tokens[tok_ids], up_flat[slot_id], preferred_element_type=jnp.float32)
        hidden = jax.nn.gelu(pre_act, approximate=True).astype(jnp.bfloat16)
        expert_out = jnp.dot(hidden, down_flat[slot_id], preferred_element_type=jnp.float32).astype(jnp.bfloat16)
        gate_vals = jnp.where(is_valid, flat_gate[pair_ids], 0.0)
        return acc_sum.at[tok_ids].add(gate_vals[:, None] * expert_out.astype(jnp.float32)), None

    acc_out, _ = lax.scan(block_step, jnp.zeros((n_tok, D_MODEL), jnp.float32), jnp.arange(N_BLOCKS))
    return acc_out.astype(jnp.bfloat16)
```

```python
import functools
import math

import jax
import jax.numpy as jnp
from jax import lax
from jax.experimental import pallas as pl
from jax.experimental.pallas import tpu as pltpu
from jax.sharding import PartitionSpec as P

MESH = pl.DeviceIdType.MESH
LANES = 128
SUB = 8
PACK = 16
USTRIDE = 32
WIN = 64


def div_small(x, c):
    third = lax.shift_right_logical(x * 171, 9)
    quarter = lax.shift_right_logical(x, 2)
    half = lax.shift_right_logical(x, 1)
    return jnp.where(c == 1, x, jnp.where(c == 2, half, jnp.where(c == 3, third, quarter)))


def up_to(x, m):
    return -(-x // m) * m


def group_barrier(n_dev, me):
    barrier = pltpu.get_barrier_semaphore()
    for k in range(1, n_dev):
        pl.semaphore_signal(barrier, inc=1, device_id={'ep': lax.rem(me + k, n_dev)}, device_id_type=MESH)
    pl.semaphore_wait(barrier, n_dev - 1)


def route_kernel(n_dev, n_slot, stride, lo_bound, hi_bound, idx, table, addr, meta, flag, hsend, hall, tabcol, ssem, rsem):
    me = lax.axis_index('ep')
    f32, bf16, i32 = jnp.float32, jnp.bfloat16, jnp.int32
    n_rows = idx.shape[0]
    n_units = n_dev * USTRIDE
    group_barrier(n_dev, me)
    sub_e = lax.broadcasted_iota(i32, (LANES, LANES), 0)
    lane_e = lax.broadcasted_iota(i32, (LANES, LANES), 1)

    def count_row(r, acc):
        return acc + (sub_e == idx[pl.ds(r, 1), :]).astype(f32)

    seen = lax.fori_loop(0, n_rows, count_row, jnp.zeros((LANES, LANES), f32))
    hist = lax.dot_general(jnp.ones((SUB, LANES), bf16), seen.astype(bf16), (((1,), (1,)), ((), ())), preferred_element_type=f32)
    hsend[...] = hist.astype(i32)
    hall[me] = hist.astype(i32)
    sends = []
    for k in range(1, n_dev):
        copy = pltpu.make_async_remote_copy(src_ref=hsend, dst_ref=hall.at[me], send_sem=ssem.at[k], recv_sem=rsem.at[k], device_id={'ep': lax.rem(me + k, n_dev)}, device_id_type=MESH)
        copy.start()
        sends.append(copy)

    lane_u = lax.broadcasted_iota(i32, (1, n_units), 1)
    tabrow = jnp.full((1, n_units), -1, i32)
    tabcol[...] = jnp.full(tabcol.shape, -1, i32)
    for d in range(n_dev):
        for s in range(n_slot):
            u = d * USTRIDE + s
            tabrow = jnp.where(lane_u == u, table[d, s], tabrow)
            tabcol[u:u + 1, :] = jnp.full((1, LANES), table[d, s], i32)
    tcol = tabcol[...]
    unit_exp = (tcol == lax.broadcasted_iota(i32, (n_units, LANES), 1)).astype(bf16)
    same = jnp.concatenate([tcol] * (n_units // LANES), axis=1) == tabrow
    su = lax.broadcasted_iota(i32, (n_units, n_units), 0)
    lu = lax.broadcasted_iota(i32, (n_units, n_units), 1)
    copy_rank = jnp.sum(jnp.where(same & (su < lu), 1.0, 0.0), axis=0, keepdims=True).astype(i32)
    copies = jnp.sum(jnp.where(same, 1.0, 0.0), axis=0, keepdims=True).astype(i32)
    valid = tabrow >= 0
    before = ((su < lu) & (lax.shift_right_logical(su, 5) == lax.shift_right_logical(lu, 5))).astype(bf16)

    def slot_loads(h):
        per_unit = lax.dot_general(h.astype(bf16), unit_exp, (((1,), (1,)), ((), ())), preferred_element_type=f32).astype(i32)
        loads = jnp.where(valid, div_small(per_unit - copy_rank + copies - 1, copies), 0)
        starts = jnp.dot(loads.astype(bf16), before, preferred_element_type=f32).astype(i32)
        return loads, starts

    _, own_starts = slot_loads(hist)
    block = lax.rem(lax.shift_right_logical(lane_u, 5) + n_dev - me, n_dev)
    first = jnp.concatenate([own_starts, own_starts], axis=0) + block * stride
    row16 = lax.broadcasted_iota(i32, (2 * SUB, n_units), 0)
    part = jnp.where(row16 < 4, lax.shift_right_logical(first, 6), jnp.where(row16 < 8, first & 63, copies))
    chosen = (copy_rank == (row16 & 3)) & valid & (row16 < 9)
    exp_tab = jnp.dot(jnp.where(chosen, part, 0).astype(bf16), unit_exp, preferred_element_type=f32).astype(bf16)
    tri = (sub_e < lane_e).astype(bf16)
    ones = jnp.ones((LANES, LANES), bf16)

    def place_row(r, run):
        hot = sub_e == idx[pl.ds(r, 1), :]
        hot_b = hot.astype(bf16)
        prefix = jnp.dot(hot_b, tri, preferred_element_type=f32) + run
        rank = jnp.sum(jnp.where(hot, prefix, 0.0), axis=0, keepdims=True).astype(i32)
        got = jnp.dot(exp_tab, hot_b, preferred_element_type=f32).astype(i32)
        c = got[8:9]
        quot = div_small(rank, c)
        kk = rank - quot * c
        hi = jnp.where(kk == 0, got[0:1], jnp.where(kk == 1, got[1:2], jnp.where(kk == 2, got[2:3], got[3:4])))
        lo = jnp.where(kk == 0, got[4:5], jnp.where(kk == 1, got[5:6], jnp.where(kk == 2, got[6:7], got[7:8])))
        pos = hi * 64 + lo + quot
        addr[pl.ds(r, 1), :] = pos + lax.shift_right_logical(pos, 3) * 40
        return run + jnp.dot(hot_b, ones, preferred_element_type=f32)

    lax.fori_loop(0, n_rows, place_row, jnp.zeros((LANES, LANES), f32))

    for k in range(1, n_dev):
        src = lax.rem(me + n_dev - k, n_dev)
        pltpu.make_async_remote_copy(src_ref=hsend, dst_ref=hall.at[src], send_sem=ssem.at[k], recv_sem=rsem.at[k], device_id={'ep': src}, device_id_type=MESH).wait_recv()
    every = jnp.concatenate([hall[p, 0:1, :] for p in range(n_dev)], axis=0)
    loads, starts = slot_loads(every.astype(f32))
    meta[0:n_dev, :] = loads
    meta[n_dev:2 * n_dev, :] = starts
    slot_id = lane_u & (USTRIDE - 1)
    low = jnp.zeros((1, n_units), i32)
    high = jnp.zeros((1, n_units), i32)
    for s in range(n_slot):
        low = jnp.where(slot_id == s, lo_bound[s], low)
        high = jnp.where(slot_id == s, hi_bound[s], high)
    ends = loads + starts
    bad = jnp.where(valid & ((ends < low) | (ends > high)), 1.0, 0.0)
    flag[...] = jnp.broadcast_to(jnp.max(jnp.max(bad, axis=1, keepdims=True), axis=0, keepdims=True), flag.shape).astype(i32)
    for copy in sends:
        copy.wait_send()


def pack_kernel(addr, tok, send, wide, tmp):
    n_rows, n_col = addr.shape
    d_tiles = tok.shape[1] // LANES
    step = SUB * d_tiles

    @pl.loop(0, wide.shape[0] // step)
    def _(b):
        wide[pl.ds(pl.multiple_of(b * step, step), step), :] = jnp.zeros((step, LANES), jnp.float32)

    @pl.loop(0, n_rows)
    def _(r):
        @pl.loop(0, n_col // PACK)
        def _(c):
            row0 = pl.multiple_of(r * n_col + c * PACK, PACK)
            x = tok[pl.ds(row0, PACK), :].astype(jnp.float32)
            for h in range(PACK // SUB):
                for j in range(d_tiles):
                    tmp[h * step + j * SUB:h * step + (j + 1) * SUB, :] = x[h * SUB:(h + 1) * SUB, j * LANES:(j + 1) * LANES]
            for i in range(PACK):
                a = addr[r, c * PACK + i]
                wide[pl.ds(a, d_tiles, stride=SUB), :] = tmp[pl.ds((i // SUB) * step + i % SUB, d_tiles, stride=SUB), :]

    @pl.loop(0, send.shape[0] // PACK)
    def _(b):
        base = b * (2 * step)
        row0 = pl.multiple_of(b * PACK, PACK)
        for j in range(d_tiles):
            top = wide[pl.ds(base + j * SUB, SUB), :]
            bot = wide[pl.ds(base + step + j * SUB, SUB), :]
            send[pl.ds(row0, PACK), j * LANES:(j + 1) * LANES] = jnp.concatenate([top, bot], axis=0).astype(jnp.bfloat16)


def unpack_kernel(addr, gate, back, out, wide, tmp):
    n_rows, n_col = addr.shape
    d_tiles = out.shape[1] // LANES
    step = SUB * d_tiles

    @pl.loop(0, back.shape[0] // PACK)
    def _(b):
        base = b * (2 * step)
        row0 = pl.multiple_of(b * PACK, PACK)
        for j in range(d_tiles):
            x = back[pl.ds(row0, PACK), j * LANES:(j + 1) * LANES].astype(jnp.float32)
            wide[pl.ds(base + j * SUB, SUB), :] = x[:SUB]
            wide[pl.ds(base + step + j * SUB, SUB), :] = x[SUB:]

    @pl.loop(0, n_rows)
    def _(r):
        @pl.loop(0, n_col // PACK)
        def _(c):
            row0 = pl.multiple_of(r * n_col + c * PACK, PACK)
            for i in range(PACK):
                a = addr[r, c * PACK + i]
                g = gate[r, c * PACK + i]
                tmp[pl.ds((i // SUB) * step + i % SUB, d_tiles, stride=SUB), :] = wide[pl.ds(a, d_tiles, stride=SUB), :] * g
            for j in range(d_tiles):
                top = tmp[j * SUB:(j + 1) * SUB, :]
                bot = tmp[step + j * SUB:step + (j + 1) * SUB, :]
                out[pl.ds(row0, PACK), j * LANES:(j + 1) * LANES] = jnp.concatenate([top, bot], axis=0).astype(jnp.bfloat16)


def gelu(x):
    return x * (0.5 * (1.0 + jnp.tanh(0.7978845608028654 * (x + 0.044715 * (x * x * x)))))


def expert_kernel(cfg, meta, send, up_hbm, down_hbm, back, recv, xbuf, ybuf, up, down, hid, xs, win, dsend, drecv, rsend, rrecv, wsem):
    n_dev, n_slot, part = cfg['n_dev'], cfg['n_slot'], cfg['part']
    m_rows = n_dev * part
    d_model, d_ff = up_hbm.shape[1], up_hbm.shape[2]
    last, disp, ret, ret_lo = cfg['last'], cfg['disp'], cfg['ret'], cfg['ret_lo']
    n_grp = len(last)
    f32, bf16, i32 = jnp.float32, jnp.bfloat16, jnp.int32
    me = lax.axis_index('ep')

    def fetch(s, b):
        return (pltpu.make_async_copy(up_hbm.at[s], up.at[b], wsem.at[0, b]), pltpu.make_async_copy(down_hbm.at[s], down.at[b], wsem.at[1, b]))

    group_barrier(n_dev, me)

    def dispatch(j, k, peer):
        rows = pl.ds(disp[j], disp[j + 1] - disp[j])
        return pltpu.make_async_remote_copy(src_ref=send.at[k, rows], dst_ref=recv.at[k, rows], send_sem=dsend.at[j, k], recv_sem=drecv.at[j, k], device_id={'ep': peer}, device_id_type=MESH)

    def dispatch_own(j):
        rows = pl.ds(disp[j], disp[j + 1] - disp[j])
        return pltpu.make_async_copy(send.at[0, rows], recv.at[0, rows], drecv.at[j, 0])

    order = sorted(range(1, n_dev), key=lambda k: (abs(k - n_dev // 2), k))
    for j in range(n_grp):
        for k in order:
            dispatch(j, k, lax.rem(me + k, n_dev)).start()
        dispatch_own(j).start()
        if j == 0:
            for s in range(2):
                for copy in fetch(s, s):
                    copy.start()

    @pl.loop(0, n_dev)
    def _(k):
        @pl.loop(0, xbuf.shape[1])
        def _(b):
            xbuf[k, b] = jnp.zeros((PACK, d_model), bf16)

    def ffn(s, b):
        unit = me * USTRIDE + s
        lane = lax.broadcasted_iota(i32, (1, n_dev * WIN), 1)
        which = lax.shift_right_logical(lane, 6)
        off = jnp.zeros((1, n_dev * WIN), i32)
        num = jnp.zeros((1, n_dev * WIN), i32)
        for k in range(n_dev):
            src = lax.rem(me + n_dev - k, n_dev)
            load, start = meta[src, unit], meta[n_dev + src, unit]
            blk = lax.shift_right_logical(start, 4)
            base = blk * PACK
            for q in range(WIN // PACK):
                win[k * WIN + q * PACK:k * WIN + (q + 1) * PACK, :] = xbuf[k, blk + q]
            off = jnp.where(which == k, base - start, off)
            num = jnp.where(which == k, load, num)
        nth = (lane & (WIN - 1)) + off
        target = jnp.where((nth >= 0) & (nth < num), nth + which * part, -1)
        pick = (lax.broadcasted_iota(i32, (m_rows, n_dev * WIN), 0) == target).astype(bf16)
        xs[...] = jnp.dot(pick, win[...], preferred_element_type=f32).astype(bf16)
        tile = 512
        for t in range(d_ff // tile):
            pre = jnp.dot(xs[...], up[b, :, t * tile:(t + 1) * tile], preferred_element_type=f32)
            hid[:, t * tile:(t + 1) * tile] = gelu(pre).astype(bf16)
        tile = 256
        for t in range(d_model // tile):
            o = jnp.dot(hid[...], down[b, :, t * tile:(t + 1) * tile], preferred_element_type=f32).astype(bf16)
            for k in range(n_dev):
                ybuf[k, pl.ds(pl.multiple_of(s * part, PACK), part), t * tile:(t + 1) * tile] = o[k * part:(k + 1) * part]

    def give_back(j, k):
        rows = pl.ds(ret[j], ret[j + 1] - ret[j])
        peer = lax.rem(me + n_dev - k, n_dev)
        return pltpu.make_async_remote_copy(src_ref=recv.at[k, rows], dst_ref=back.at[k, rows], send_sem=rsend.at[j, k], recv_sem=rrecv.at[j, k], device_id={'ep': peer}, device_id_type=MESH)

    def give_own(j):
        rows = pl.ds(ret[j], ret[j + 1] - ret[j])
        return pltpu.make_async_copy(recv.at[0, rows], back.at[0, rows], rrecv.at[j, 0])

    def combine(j):
        n_rows = ret[j + 1] - ret[j]
        n_win = last[j] + 1 - ret_lo[j]
        width = n_win * part

        @pl.loop(0, n_dev)
        def _(i):
            k = lax.rem(n_dev // 2 + 3 * i, n_dev)
            src = lax.rem(me + n_dev - k, n_dev)
            lane = lax.broadcasted_iota(i32, (1, width), 1)
            target = jnp.full((1, width), -1, i32)
            for w in range(n_win):
                unit = me * USTRIDE + ret_lo[j] + w
                load, start = meta[src, unit], meta[n_dev + src, unit]
                nth = lane - w * part
                target = jnp.where((nth >= 0) & (nth < load), nth + start, target)
            pick = (lax.broadcasted_iota(i32, (n_rows, width), 0) + ret[j] == target).astype(bf16)
            rows = ybuf[k, ret_lo[j] * part:(last[j] + 1) * part, :]
            recv[k, ret[j]:ret[j + 1], :] = jnp.dot(pick, rows, preferred_element_type=f32).astype(bf16)

            @pl.when(k == 0)
            def _():
                give_own(j).start()

            @pl.when(k != 0)
            def _():
                give_back(j, k).start()

    @pl.loop(0, n_slot)
    def _(s):
        for j in range(n_grp):
            @pl.when(s == (0 if j == 0 else last[j - 1] + 1))
            def _():
                for k in range(1, n_dev):
                    dispatch(j, k, lax.rem(me + n_dev - k, n_dev)).wait_recv()
                dispatch_own(j).wait()

                @pl.loop(0, n_dev)
                def _(k):
                    @pl.loop(disp[j] // PACK, disp[j + 1] // PACK)
                    def _(b):
                        xbuf[k, b] = recv[k, pl.ds(pl.multiple_of(b * PACK, PACK), PACK), :]

        b = lax.rem(s, 2)
        for copy in fetch(s, b):
            copy.wait()
        ffn(s, b)

        @pl.when(s + 2 < n_slot)
        def _():
            for copy in fetch(s + 2, b):
                copy.start()

        for j in range(n_grp):
            @pl.when(s == last[j])
            def _():
                combine(j)

    for j in range(n_grp):
        for k in range(1, n_dev):
            dispatch(j, k, lax.rem(me + k, n_dev)).wait_send()
            give_back(j, k).wait_send()
            give_back(j, k).wait_recv()
        give_own(j).wait()


def plan(n_dev, n_slot, n_pairs, bound, z, lasts):
    stride = up_to(n_slot * bound, PACK)
    mean = n_pairs / (n_dev * n_slot)
    spread = 9.3 * mean / 30.1
    if z is None:
        hi = [bound * (s + 1) for s in range(n_slot)]
        lo = [0] * n_slot
    else:
        hi = [min(bound * (s + 1), math.ceil(mean * (s + 1) + z * spread * math.sqrt(s + 1))) for s in range(n_slot)]
        lo = [max(0, math.floor(mean * (s + 1) - z * spread * math.sqrt(s + 1))) for s in range(n_slot)]
        lo[-1] = 0
    cap = min(stride, up_to(hi[-1], PACK))
    hi[-1] = min(cap, n_slot * bound)
    disp = [0] + [up_to(hi[s], PACK) for s in lasts]
    disp[-1] = cap
    ret = [0] + [lo[s] // PACK * PACK for s in lasts]
    ret[-1] = cap
    ret_lo = [min(s for s in range(n_slot) if hi[s] > ret[j]) for j in range(len(lasts))]
    return dict(n_dev=n_dev, n_slot=n_slot, cap=cap, stride=stride, lo=lo, hi=hi, last=list(lasts), disp=disp, ret=ret, ret_lo=ret_lo, part=up_to(bound, PACK))


def solution(mesh):
    n_dev = mesh.shape['ep']

    def group_layer(tokens, topk_idx, topk_w, w_up, w_down, slot_expert):
        n_tok, d_model = tokens.shape
        n_slot = slot_expert.shape[1]
        d_ff = w_up.shape[3]
        n_pairs = n_tok * topk_idx.shape[1]
        base_load = n_pairs // (n_dev * n_slot)
        bound = base_load + base_load // 2 + 1
        fast = plan(n_dev, n_slot, n_pairs, bound, 3.33, [n_slot * 4 // 17 - 1, n_slot * 8 // 17 - 1, n_slot * 12 // 17 - 1, n_slot * 15 // 17 - 1, n_slot - 1])
        slow = plan(n_dev, n_slot, n_pairs, bound, None, [n_slot - 1])
        stride = fast['stride']
        n_rows = n_pairs // LANES
        n_units = n_dev * USTRIDE
        f32, bf16, i32 = jnp.float32, jnp.bfloat16, jnp.int32
        vmem = pl.BlockSpec(memory_space=pltpu.VMEM)
        smem = pl.BlockSpec(memory_space=pltpu.SMEM)
        hbm = pl.BlockSpec(memory_space=pl.ANY)
        big = 63 * 1024 * 1024

        addr, meta, flag = pl.pallas_call(
            functools.partial(route_kernel, n_dev, n_slot, stride, fast['lo'], fast['hi']),
            out_shape=[jax.ShapeDtypeStruct((n_rows, LANES), i32), jax.ShapeDtypeStruct((2 * n_dev, n_units), i32), jax.ShapeDtypeStruct((SUB, LANES), i32)],
            in_specs=[vmem, smem],
            out_specs=[vmem, vmem, vmem],
            scratch_shapes=[pltpu.VMEM((SUB, LANES), i32), pltpu.VMEM((n_dev, SUB, LANES), i32), pltpu.VMEM((n_units, LANES), i32), pltpu.SemaphoreType.DMA((n_dev,)), pltpu.SemaphoreType.DMA((n_dev,))],
            compiler_params=pltpu.CompilerParams(collective_id=0, has_side_effects=True),
            name='route',
        )(topk_idx.reshape(n_rows, LANES), slot_expert)

        d_tiles = d_model // LANES
        wide = pltpu.VMEM((n_dev * stride * d_tiles, LANES), f32)
        tmp = pltpu.VMEM((PACK * d_tiles, LANES), f32)
        send = pl.pallas_call(
            pack_kernel,
            out_shape=jax.ShapeDtypeStruct((n_dev * stride, d_model), bf16),
            in_specs=[smem, vmem],
            out_specs=vmem,
            scratch_shapes=[wide, tmp],
            compiler_params=pltpu.CompilerParams(vmem_limit_bytes=big),
            name='pack',
        )(addr, tokens).reshape(n_dev, stride, d_model)

        def run(cfg, meta, send, w_up, w_down):
            n_grp = len(cfg['last'])
            part, cap = cfg['part'], cfg['cap']
            m_rows = n_dev * part
            dma = pltpu.SemaphoreType.DMA((n_grp, n_dev))
            return pl.pallas_call(
                functools.partial(expert_kernel, cfg),
                out_shape=jax.ShapeDtypeStruct((n_dev, stride, d_model), bf16),
                in_specs=[smem, hbm, hbm, hbm],
                out_specs=hbm,
                scratch_shapes=[
                    pltpu.VMEM((n_dev, cap, d_model), bf16),
                    pltpu.VMEM((n_dev, (cap + WIN) // PACK, PACK, d_model), bf16),
                    pltpu.VMEM((n_dev, n_slot * part, d_model), bf16),
                    pltpu.VMEM((2, d_model, d_ff), bf16),
                    pltpu.VMEM((2, d_ff, d_model), bf16),
                    pltpu.VMEM((m_rows, d_ff), bf16),
                    pltpu.VMEM((m_rows, d_model), bf16),
                    pltpu.VMEM((n_dev * WIN, d_model), bf16),
                    dma, dma, dma, dma,
                    pltpu.SemaphoreType.DMA((2, 2)),
                ],
                compiler_params=pltpu.CompilerParams(collective_id=1, has_side_effects=True, vmem_limit_bytes=big),
                name='experts',
            )(meta, send, w_up, w_down)

        back = lax.cond(flag[0, 0] == 0, functools.partial(run, fast), functools.partial(run, slow), meta, send, w_up[0], w_down[0])

        return pl.pallas_call(
            unpack_kernel,
            out_shape=jax.ShapeDtypeStruct((n_tok, d_model), bf16),
            in_specs=[smem, smem, vmem],
            out_specs=vmem,
            scratch_shapes=[wide, tmp],
            compiler_params=pltpu.CompilerParams(vmem_limit_bytes=big),
            name='unpack',
        )(addr, topk_w.reshape(n_rows, LANES), back.reshape(n_dev * stride, d_model))

    row_spec = P(('dp', 'ep'), None)
    weight_spec = P('ep', None, None, None)
    return jax.shard_map(group_layer, mesh=mesh, in_specs=(row_spec, row_spec, row_spec, weight_spec, weight_spec, P(None, None)), out_specs=row_spec, check_vma=False)
```

```python
import functools
import math

import jax
import jax.numpy as jnp
from jax import lax
from jax.experimental import pallas as pl
from jax.experimental.pallas import tpu as pltpu
from jax.sharding import PartitionSpec as P

MESH = pl.DeviceIdType.MESH
LANES = 128
SUB = 8
PACK = 16
USTRIDE = 32
WIN = 64


def div_small(x, c):
    third = lax.shift_right_logical(x * 171, 9)
    quarter = lax.shift_right_logical(x, 2)
    half = lax.shift_right_logical(x, 1)
    return jnp.where(c == 1, x, jnp.where(c == 2, half, jnp.where(c == 3, third, quarter)))


def up_to(x, m):
    return -(-x // m) * m


def group_barrier(n_dev, me):
    barrier = pltpu.get_barrier_semaphore()
    for k in range(1, n_dev):
        pl.semaphore_signal(barrier, inc=1, device_id={'ep': lax.rem(me + k, n_dev)}, device_id_type=MESH)
    pl.semaphore_wait(barrier, n_dev - 1)


def route_kernel(n_dev, n_slot, stride, lo_bound, hi_bound, idx, table, addr, meta, flag, hsend, hall, tabcol, ssem, rsem):
    me = lax.axis_index('ep')
    f32, bf16, i32 = jnp.float32, jnp.bfloat16, jnp.int32
    n_rows = idx.shape[0]
    n_units = n_dev * USTRIDE
    group_barrier(n_dev, me)
    sub_e = lax.broadcasted_iota(i32, (LANES, LANES), 0)
    lane_e = lax.broadcasted_iota(i32, (LANES, LANES), 1)

    def count_row(r, acc):
        return acc + (sub_e == idx[pl.ds(r, 1), :]).astype(f32)

    seen = lax.fori_loop(0, n_rows, count_row, jnp.zeros((LANES, LANES), f32))
    hist = lax.dot_general(jnp.ones((SUB, LANES), bf16), seen.astype(bf16), (((1,), (1,)), ((), ())), preferred_element_type=f32)
    hsend[...] = hist.astype(i32)
    hall[me] = hist.astype(i32)
    sends = []
    for k in range(1, n_dev):
        copy = pltpu.make_async_remote_copy(src_ref=hsend, dst_ref=hall.at[me], send_sem=ssem.at[k], recv_sem=rsem.at[k], device_id={'ep': lax.rem(me + k, n_dev)}, device_id_type=MESH)
        copy.start()
        sends.append(copy)

    lane_u = lax.broadcasted_iota(i32, (1, n_units), 1)
    tabrow = jnp.full((1, n_units), -1, i32)
    tabcol[...] = jnp.full(tabcol.shape, -1, i32)
    for d in range(n_dev):
        for s in range(n_slot):
            u = d * USTRIDE + s
            tabrow = jnp.where(lane_u == u, table[d, s], tabrow)
            tabcol[u:u + 1, :] = jnp.full((1, LANES), table[d, s], i32)
    tcol = tabcol[...]
    unit_exp = (tcol == lax.broadcasted_iota(i32, (n_units, LANES), 1)).astype(bf16)
    same = jnp.concatenate([tcol] * (n_units // LANES), axis=1) == tabrow
    su = lax.broadcasted_iota(i32, (n_units, n_units), 0)
    lu = lax.broadcasted_iota(i32, (n_units, n_units), 1)
    copy_rank = jnp.sum(jnp.where(same & (su < lu), 1.0, 0.0), axis=0, keepdims=True).astype(i32)
    copies = jnp.sum(jnp.where(same, 1.0, 0.0), axis=0, keepdims=True).astype(i32)
    valid = tabrow >= 0
    before = ((su < lu) & (lax.shift_right_logical(su, 5) == lax.shift_right_logical(lu, 5))).astype(bf16)

    def slot_loads(h):
        per_unit = lax.dot_general(h.astype(bf16), unit_exp, (((1,), (1,)), ((), ())), preferred_element_type=f32).astype(i32)
        loads = jnp.where(valid, div_small(per_unit - copy_rank + copies - 1, copies), 0)
        starts = jnp.dot(loads.astype(bf16), before, preferred_element_type=f32).astype(i32)
        return loads, starts

    _, own_starts = slot_loads(hist)
    block = lax.rem(lax.shift_right_logical(lane_u, 5) + n_dev - me, n_dev)
    first = jnp.concatenate([own_starts, own_starts], axis=0) + block * stride
    row16 = lax.broadcasted_iota(i32, (2 * SUB, n_units), 0)
    part = jnp.where(row16 < 4, lax.shift_right_logical(first, 6), jnp.where(row16 < 8, first & 63, copies))
    chosen = (copy_rank == (row16 & 3)) & valid & (row16 < 9)
    exp_tab = jnp.dot(jnp.where(chosen, part, 0).astype(bf16), unit_exp, preferred_element_type=f32).astype(bf16)
    tri = (sub_e < lane_e).astype(bf16)
    ones = jnp.ones((LANES, LANES), bf16)

    def place_row(r, run):
        hot = sub_e == idx[pl.ds(r, 1), :]
        hot_b = hot.astype(bf16)
        prefix = jnp.dot(hot_b, tri, preferred_element_type=f32) + run
        rank = jnp.sum(jnp.where(hot, prefix, 0.0), axis=0, keepdims=True).astype(i32)
        got = jnp.dot(exp_tab, hot_b, preferred_element_type=f32).astype(i32)
        c = got[8:9]
        quot = div_small(rank, c)
        kk = rank - quot * c
        hi = jnp.where(kk == 0, got[0:1], jnp.where(kk == 1, got[1:2], jnp.where(kk == 2, got[2:3], got[3:4])))
        lo = jnp.where(kk == 0, got[4:5], jnp.where(kk == 1, got[5:6], jnp.where(kk == 2, got[6:7], got[7:8])))
        pos = hi * 64 + lo + quot
        addr[pl.ds(r, 1), :] = pos + lax.shift_right_logical(pos, 3) * 40
        return run + jnp.dot(hot_b, ones, preferred_element_type=f32)

    lax.fori_loop(0, n_rows, place_row, jnp.zeros((LANES, LANES), f32))

    for k in range(1, n_dev):
        src = lax.rem(me + n_dev - k, n_dev)
        pltpu.make_async_remote_copy(src_ref=hsend, dst_ref=hall.at[src], send_sem=ssem.at[k], recv_sem=rsem.at[k], device_id={'ep': src}, device_id_type=MESH).wait_recv()
    every = jnp.concatenate([hall[p, 0:1, :] for p in range(n_dev)], axis=0)
    loads, starts = slot_loads(every.astype(f32))
    meta[0:n_dev, :] = loads
    meta[n_dev:2 * n_dev, :] = starts
    slot_id = lane_u & (USTRIDE - 1)
    low = jnp.zeros((1, n_units), i32)
    high = jnp.zeros((1, n_units), i32)
    for s in range(n_slot):
        low = jnp.where(slot_id == s, lo_bound[s], low)
        high = jnp.where(slot_id == s, hi_bound[s], high)
    ends = loads + starts
    bad = jnp.where(valid & ((ends < low) | (ends > high)), 1.0, 0.0)
    flag[...] = jnp.broadcast_to(jnp.max(jnp.max(bad, axis=1, keepdims=True), axis=0, keepdims=True), flag.shape).astype(i32)
    for copy in sends:
        copy.wait_send()


def pack_kernel(cap, addr, flag, tok_hbm, send, tok, wide, tmp, stage, tsem, ssem):
    n_rows, n_col = addr.shape
    n_dev, stride = stage.shape[0], stage.shape[1]
    d_tiles = tok.shape[1] // LANES
    step = SUB * d_tiles
    load = pltpu.make_async_copy(tok_hbm, tok, tsem)
    load.start()
    zero_rows = 4 * step

    @pl.loop(0, wide.shape[0] // zero_rows)
    def _(b):
        wide[pl.ds(pl.multiple_of(b * zero_rows, zero_rows), zero_rows), :] = jnp.zeros((zero_rows, LANES), jnp.float32)

    load.wait()

    @pl.loop(0, n_rows)
    def _(r):
        for c in range(n_col // PACK):
            at = c * 2 * step
            x = tok[pl.ds(pl.multiple_of(r * n_col + c * PACK, PACK), PACK), :].astype(jnp.float32)
            for h in range(PACK // SUB):
                for j in range(d_tiles):
                    tmp[at + h * step + j * SUB:at + h * step + (j + 1) * SUB, :] = x[h * SUB:(h + 1) * SUB, j * LANES:(j + 1) * LANES]
            for i in range(PACK):
                a = addr[r, c * PACK + i]
                wide[pl.ds(a, d_tiles, stride=SUB), :] = tmp[pl.ds(at + (i // SUB) * step + i % SUB, d_tiles, stride=SUB), :]

    def narrow(k, b):
        base = (k * (stride // PACK) + b) * (2 * step)
        rows = pl.ds(pl.multiple_of(b * PACK, PACK), PACK)
        for j in range(d_tiles):
            top = wide[pl.ds(base + j * SUB, SUB), :]
            bot = wide[pl.ds(base + step + j * SUB, SUB), :]
            stage[k, rows, j * LANES:(j + 1) * LANES] = jnp.concatenate([top, bot], axis=0).astype(jnp.bfloat16)

    def store(k, lo, hi):
        return pltpu.make_async_copy(stage.at[k, pl.ds(lo, hi - lo)], send.at[k, pl.ds(lo, hi - lo)], ssem.at[k])

    @pl.loop(0, n_dev)
    def _(k):
        @pl.loop(0, cap // PACK, unroll=4)
        def _(b):
            narrow(k, b)

        store(k, 0, cap).start()

    @pl.loop(0, n_dev)
    def _(k):
        store(k, 0, cap).wait()

    @pl.when(flag[0, 0] != 0)
    def _():
        @pl.loop(0, n_dev)
        def _(k):
            @pl.loop(cap // PACK, stride // PACK)
            def _(b):
                narrow(k, b)

            rest = store(k, cap, stride)
            rest.start()
            rest.wait()


def unpack_kernel(cap, addr, flag, gate, back_hbm, out_hbm, back, wide, tmp, out, bsem, osem):
    n_rows, n_col = addr.shape
    n_dev, stride = back.shape[0], back.shape[1]
    d_tiles = out.shape[1] // LANES
    step = SUB * d_tiles

    def load(k, lo, hi):
        return pltpu.make_async_copy(back_hbm.at[k, pl.ds(lo, hi - lo)], back.at[k, pl.ds(lo, hi - lo)], bsem.at[k])

    def widen(k, b):
        base = (k * (stride // PACK) + b) * (2 * step)
        rows = pl.ds(pl.multiple_of(b * PACK, PACK), PACK)
        for j in range(d_tiles):
            x = back[k, rows, j * LANES:(j + 1) * LANES].astype(jnp.float32)
            wide[pl.ds(base + j * SUB, SUB), :] = x[:SUB]
            wide[pl.ds(base + step + j * SUB, SUB), :] = x[SUB:]

    @pl.loop(0, n_dev)
    def _(k):
        load(k, 0, cap).start()

    @pl.loop(0, n_dev)
    def _(k):
        load(k, 0, cap).wait()

        @pl.loop(0, cap // PACK, unroll=4)
        def _(b):
            widen(k, b)

    @pl.when(flag[0, 0] != 0)
    def _():
        @pl.loop(0, n_dev)
        def _(k):
            rest = load(k, cap, stride)
            rest.start()
            rest.wait()

            @pl.loop(cap // PACK, stride // PACK)
            def _(b):
                widen(k, b)

    def give(g):
        rows = pl.ds(pl.multiple_of(g * n_col, n_col), n_col)
        return pltpu.make_async_copy(out.at[rows], out_hbm.at[rows], osem)

    @pl.loop(0, n_rows)
    def _(r):
        for c in range(n_col // PACK):
            at = c * 2 * step
            for i in range(PACK):
                a = addr[r, c * PACK + i]
                g = gate[r, c * PACK + i]
                tmp[pl.ds(at + (i // SUB) * step + i % SUB, d_tiles, stride=SUB), :] = wide[pl.ds(a, d_tiles, stride=SUB), :] * g
            rows = pl.ds(pl.multiple_of(r * n_col + c * PACK, PACK), PACK)
            for j in range(d_tiles):
                top = tmp[at + j * SUB:at + (j + 1) * SUB, :]
                bot = tmp[at + step + j * SUB:at + step + (j + 1) * SUB, :]
                out[rows, j * LANES:(j + 1) * LANES] = jnp.concatenate([top, bot], axis=0).astype(jnp.bfloat16)
        give(r).start()

    @pl.loop(0, n_rows)
    def _(r):
        give(r).wait()


def gelu(x):
    return x * (0.5 * (1.0 + jnp.tanh(0.7978845608028654 * (x + 0.044715 * (x * x * x)))))


def expert_kernel(cfg, meta, send, up_hbm, down_hbm, back, recv, xbuf, ybuf, up, down, hid, xs, win, dsend, drecv, rsend, rrecv, wsem):
    n_dev, n_slot, part = cfg['n_dev'], cfg['n_slot'], cfg['part']
    m_rows = n_dev * part
    d_model, d_ff = up_hbm.shape[1], up_hbm.shape[2]
    last, disp, ret, ret_lo = cfg['last'], cfg['disp'], cfg['ret'], cfg['ret_lo']
    n_grp = len(last)
    f32, bf16, i32 = jnp.float32, jnp.bfloat16, jnp.int32
    me = lax.axis_index('ep')

    def fetch(s, b):
        return (pltpu.make_async_copy(up_hbm.at[s], up.at[b], wsem.at[0, b]), pltpu.make_async_copy(down_hbm.at[s], down.at[b], wsem.at[1, b]))

    group_barrier(n_dev, me)

    def dispatch(j, k, peer):
        rows = pl.ds(disp[j], disp[j + 1] - disp[j])
        return pltpu.make_async_remote_copy(src_ref=send.at[k, rows], dst_ref=recv.at[k, rows], send_sem=dsend.at[j, k], recv_sem=drecv.at[j, k], device_id={'ep': peer}, device_id_type=MESH)

    def dispatch_own(j):
        rows = pl.ds(disp[j], disp[j + 1] - disp[j])
        return pltpu.make_async_copy(send.at[0, rows], recv.at[0, rows], drecv.at[j, 0])

    order = sorted(range(1, n_dev), key=lambda k: (abs(k - n_dev // 2), k))
    for j in range(n_grp):
        for k in order:
            dispatch(j, k, lax.rem(me + k, n_dev)).start()
        dispatch_own(j).start()
        if j == 0:
            for s in range(2):
                for copy in fetch(s, s):
                    copy.start()

    @pl.loop(0, n_dev)
    def _(k):
        @pl.loop(0, xbuf.shape[1])
        def _(b):
            xbuf[k, b] = jnp.zeros((PACK, d_model), bf16)

    def ffn(s, b):
        unit = me * USTRIDE + s
        lane = lax.broadcasted_iota(i32, (1, n_dev * WIN), 1)
        which = lax.shift_right_logical(lane, 6)
        off = jnp.zeros((1, n_dev * WIN), i32)
        num = jnp.zeros((1, n_dev * WIN), i32)
        for k in range(n_dev):
            src = lax.rem(me + n_dev - k, n_dev)
            load, start = meta[src, unit], meta[n_dev + src, unit]
            blk = lax.shift_right_logical(start, 4)
            base = blk * PACK
            for q in range(WIN // PACK):
                win[k * WIN + q * PACK:k * WIN + (q + 1) * PACK, :] = xbuf[k, blk + q]
            off = jnp.where(which == k, base - start, off)
            num = jnp.where(which == k, load, num)
        nth = (lane & (WIN - 1)) + off
        target = jnp.where((nth >= 0) & (nth < num), nth + which * part, -1)
        pick = (lax.broadcasted_iota(i32, (m_rows, n_dev * WIN), 0) == target).astype(bf16)
        xs[...] = jnp.dot(pick, win[...], preferred_element_type=f32).astype(bf16)
        tile = 512
        for t in range(d_ff // tile):
            pre = jnp.dot(xs[...], up[b, :, t * tile:(t + 1) * tile], preferred_element_type=f32)
            hid[:, t * tile:(t + 1) * tile] = gelu(pre).astype(bf16)
        tile = 256
        for t in range(d_model // tile):
            o = jnp.dot(hid[...], down[b, :, t * tile:(t + 1) * tile], preferred_element_type=f32).astype(bf16)
            for k in range(n_dev):
                ybuf[k, pl.ds(pl.multiple_of(s * part, PACK), part), t * tile:(t + 1) * tile] = o[k * part:(k + 1) * part]

    def give_back(j, k):
        rows = pl.ds(ret[j], ret[j + 1] - ret[j])
        peer = lax.rem(me + n_dev - k, n_dev)
        return pltpu.make_async_remote_copy(src_ref=recv.at[k, rows], dst_ref=back.at[k, rows], send_sem=rsend.at[j, k], recv_sem=rrecv.at[j, k], device_id={'ep': peer}, device_id_type=MESH)

    def give_own(j):
        rows = pl.ds(ret[j], ret[j + 1] - ret[j])
        return pltpu.make_async_copy(recv.at[0, rows], back.at[0, rows], rrecv.at[j, 0])

    def combine(j):
        n_rows = ret[j + 1] - ret[j]
        n_win = last[j] + 1 - ret_lo[j]
        width = n_win * part

        @pl.loop(0, n_dev)
        def _(i):
            k = lax.rem(n_dev // 2 + 3 * i, n_dev)
            src = lax.rem(me + n_dev - k, n_dev)
            lane = lax.broadcasted_iota(i32, (1, width), 1)
            target = jnp.full((1, width), -1, i32)
            for w in range(n_win):
                unit = me * USTRIDE + ret_lo[j] + w
                load, start = meta[src, unit], meta[n_dev + src, unit]
                nth = lane - w * part
                target = jnp.where((nth >= 0) & (nth < load), nth + start, target)
            pick = (lax.broadcasted_iota(i32, (n_rows, width), 0) + ret[j] == target).astype(bf16)
            rows = ybuf[k, ret_lo[j] * part:(last[j] + 1) * part, :]
            recv[k, ret[j]:ret[j + 1], :] = jnp.dot(pick, rows, preferred_element_type=f32).astype(bf16)

            @pl.when(k == 0)
            def _():
                give_own(j).start()

            @pl.when(k != 0)
            def _():
                give_back(j, k).start()

    @pl.loop(0, n_slot)
    def _(s):
        for j in range(n_grp):
            @pl.when(s == (0 if j == 0 else last[j - 1] + 1))
            def _():
                for k in range(1, n_dev):
                    dispatch(j, k, lax.rem(me + n_dev - k, n_dev)).wait_recv()
                dispatch_own(j).wait()

                @pl.loop(0, n_dev)
                def _(k):
                    @pl.loop(disp[j] // PACK, disp[j + 1] // PACK)
                    def _(b):
                        xbuf[k, b] = recv[k, pl.ds(pl.multiple_of(b * PACK, PACK), PACK), :]

        b = lax.rem(s, 2)
        for copy in fetch(s, b):
            copy.wait()
        ffn(s, b)

        @pl.when(s + 2 < n_slot)
        def _():
            for copy in fetch(s + 2, b):
                copy.start()

        for j in range(n_grp):
            @pl.when(s == last[j])
            def _():
                combine(j)

    for j in range(n_grp):
        for k in range(1, n_dev):
            dispatch(j, k, lax.rem(me + k, n_dev)).wait_send()
            give_back(j, k).wait_send()
            give_back(j, k).wait_recv()
        give_own(j).wait()


def plan(n_dev, n_slot, n_pairs, bound, z, z_cap, lasts):
    stride = up_to(n_slot * bound, PACK)
    mean = n_pairs / (n_dev * n_slot)
    spread = 9.3 * mean / 30.1
    if z is None:
        hi = [bound * (s + 1) for s in range(n_slot)]
        lo = [0] * n_slot
    else:
        hi = [min(bound * (s + 1), math.ceil(mean * (s + 1) + z * spread * math.sqrt(s + 1))) for s in range(n_slot)]
        lo = [max(0, math.floor(mean * (s + 1) - z * spread * math.sqrt(s + 1))) for s in range(n_slot)]
        lo[-1] = 0
    cap = stride if z is None else min(stride, up_to(math.ceil(mean * n_slot + z_cap * spread * math.sqrt(n_slot)), PACK))
    hi = [min(h, cap) for h in hi]
    disp = [0] + [up_to(hi[s], PACK) for s in lasts]
    disp = [min(d, cap) for d in disp[:-1]] + [cap]
    ret = [0] + [lo[s] // PACK * PACK for s in lasts]
    ret[-1] = cap
    ret_lo = [min(s for s in range(n_slot) if hi[s] > ret[j]) for j in range(len(lasts))]
    return dict(n_dev=n_dev, n_slot=n_slot, cap=cap, stride=stride, lo=lo, hi=hi, last=list(lasts), disp=disp, ret=ret, ret_lo=ret_lo, part=up_to(bound, PACK))


def solution(mesh):
    n_dev = mesh.shape['ep']

    def group_layer(tokens, topk_idx, topk_w, w_up, w_down, slot_expert):
        n_tok, d_model = tokens.shape
        n_slot = slot_expert.shape[1]
        d_ff = w_up.shape[3]
        n_pairs = n_tok * topk_idx.shape[1]
        base_load = n_pairs // (n_dev * n_slot)
        bound = base_load + base_load // 2 + 1
        fast = plan(n_dev, n_slot, n_pairs, bound, 3.6, 2.9, [n_slot * 4 // 17 - 1, n_slot * 8 // 17 - 1, n_slot * 12 // 17 - 1, n_slot * 15 // 17 - 1, n_slot - 1])
        slow = plan(n_dev, n_slot, n_pairs, bound, None, None, [n_slot - 1])
        stride = fast['stride']
        n_rows = n_pairs // LANES
        n_units = n_dev * USTRIDE
        f32, bf16, i32 = jnp.float32, jnp.bfloat16, jnp.int32
        vmem = pl.BlockSpec(memory_space=pltpu.VMEM)
        smem = pl.BlockSpec(memory_space=pltpu.SMEM)
        hbm = pl.BlockSpec(memory_space=pl.ANY)
        big = 63 * 1024 * 1024

        addr, meta, flag = pl.pallas_call(
            functools.partial(route_kernel, n_dev, n_slot, stride, fast['lo'], fast['hi']),
            out_shape=[jax.ShapeDtypeStruct((n_rows, LANES), i32), jax.ShapeDtypeStruct((2 * n_dev, n_units), i32), jax.ShapeDtypeStruct((SUB, LANES), i32)],
            in_specs=[vmem, smem],
            out_specs=[vmem, vmem, vmem],
            scratch_shapes=[pltpu.VMEM((SUB, LANES), i32), pltpu.VMEM((n_dev, SUB, LANES), i32), pltpu.VMEM((n_units, LANES), i32), pltpu.SemaphoreType.DMA((n_dev,)), pltpu.SemaphoreType.DMA((n_dev,))],
            compiler_params=pltpu.CompilerParams(collective_id=0, has_side_effects=True),
            name='route',
        )(topk_idx.reshape(n_rows, LANES), slot_expert)

        d_tiles = d_model // LANES
        wide = pltpu.VMEM((n_dev * stride * d_tiles, LANES), f32)
        tmp = pltpu.VMEM((LANES * d_tiles, LANES), f32)
        block = pltpu.VMEM((n_dev, stride, d_model), bf16)
        rows_vmem = pltpu.VMEM((n_tok, d_model), bf16)
        sem, sems = pltpu.SemaphoreType.DMA, pltpu.SemaphoreType.DMA((n_dev,))
        send = pl.pallas_call(
            functools.partial(pack_kernel, fast['cap']),
            out_shape=jax.ShapeDtypeStruct((n_dev, stride, d_model), bf16),
            in_specs=[smem, smem, hbm],
            out_specs=hbm,
            scratch_shapes=[rows_vmem, wide, tmp, block, sem, sems],
            compiler_params=pltpu.CompilerParams(vmem_limit_bytes=big),
            name='pack',
        )(addr, flag, tokens)

        def run(cfg, meta, send, w_up, w_down):
            n_grp = len(cfg['last'])
            part, cap = cfg['part'], cfg['cap']
            m_rows = n_dev * part
            dma = pltpu.SemaphoreType.DMA((n_grp, n_dev))
            return pl.pallas_call(
                functools.partial(expert_kernel, cfg),
                out_shape=jax.ShapeDtypeStruct((n_dev, stride, d_model), bf16),
                in_specs=[smem, hbm, hbm, hbm],
                out_specs=hbm,
                scratch_shapes=[
                    pltpu.VMEM((n_dev, cap, d_model), bf16),
                    pltpu.VMEM((n_dev, (cap + WIN) // PACK, PACK, d_model), bf16),
                    pltpu.VMEM((n_dev, n_slot * part, d_model), bf16),
                    pltpu.VMEM((2, d_model, d_ff), bf16),
                    pltpu.VMEM((2, d_ff, d_model), bf16),
                    pltpu.VMEM((m_rows, d_ff), bf16),
                    pltpu.VMEM((m_rows, d_model), bf16),
                    pltpu.VMEM((n_dev * WIN, d_model), bf16),
                    dma, dma, dma, dma,
                    pltpu.SemaphoreType.DMA((2, 2)),
                ],
                compiler_params=pltpu.CompilerParams(collective_id=1, has_side_effects=True, vmem_limit_bytes=big),
                name='experts',
            )(meta, send, w_up, w_down)

        back = lax.cond(flag[0, 0] == 0, functools.partial(run, fast), functools.partial(run, slow), meta, send, w_up[0], w_down[0])

        return pl.pallas_call(
            functools.partial(unpack_kernel, fast['cap']),
            out_shape=jax.ShapeDtypeStruct((n_tok, d_model), bf16),
            in_specs=[smem, smem, smem, hbm],
            out_specs=hbm,
            scratch_shapes=[block, wide, tmp, rows_vmem, sems, sem],
            compiler_params=pltpu.CompilerParams(vmem_limit_bytes=big),
            name='unpack',
        )(addr, flag, topk_w.reshape(n_rows, LANES), back)

    row_spec = P(('dp', 'ep'), None)
    weight_spec = P('ep', None, None, None)
    return jax.shard_map(group_layer, mesh=mesh, in_specs=(row_spec, row_spec, row_spec, weight_spec, weight_spec, P(None, None)), out_specs=row_spec, check_vma=False)
```

```python
import functools
import math

import jax
import jax.numpy as jnp
from jax import lax
from jax.experimental import pallas as pl
from jax.experimental.pallas import tpu as pltpu
from jax.sharding import PartitionSpec as P

MESH = pl.DeviceIdType.MESH
LANES = 128
SUB = 8
PACK = 16
USTRIDE = 32
WIN = 64
TIERS = (1.125, 1.156, 1.1875, 1.25)


def up_to(x, m):
    return -(-x // m) * m


def group_barrier(n_dev, me):
    barrier = pltpu.get_barrier_semaphore()
    for k in range(1, n_dev):
        pl.semaphore_signal(barrier, inc=1, device_id={'ep': lax.rem(me + k, n_dev)}, device_id_type=MESH)
    pl.semaphore_wait(barrier, n_dev - 1)


def level_copies(loads, where, copies, bound):
    n_copy = len(where)
    f32, bf16 = jnp.float32, jnp.bfloat16
    share = [jnp.where(k < copies, loads / jnp.maximum(copies, 1.0), 0.0) for k in range(n_copy)]
    for _ in range(2):
        block = sum(lax.dot_general(share[k].astype(bf16), where[k], (((1,), (1,)), ((), ())), preferred_element_type=f32) for k in range(n_copy))
        there = [jnp.where(k < copies, jnp.dot(block.astype(bf16), where[k], preferred_element_type=f32), 0.0) for k in range(n_copy)]
        mean = sum(there) / jnp.maximum(copies, 1.0)
        share = [jnp.where(k < copies, jnp.clip(share[k] + 0.5 * (mean - there[k]), 0.0, bound), 0.0) for k in range(n_copy)]
    left, taken = loads, []
    for k in range(n_copy):
        after = jnp.maximum(copies - (k + 1), 0.0)
        want = jnp.floor(share[k] + 0.5)
        got = jnp.minimum(jnp.maximum(want, jnp.maximum(left - bound * after, 0.0)), jnp.minimum(left, bound))
        got = jnp.where(k < copies, got, 0.0)
        taken.append(got)
        left = left - got
    return taken


def route_kernel(n_dev, n_slot, stride, bound, low, high, caps, idx, table, addr, meta, flag, hsend, hall, hrow, tabcol, cums, ssem, rsem):
    me = lax.axis_index('ep')
    f32, bf16, i32 = jnp.float32, jnp.bfloat16, jnp.int32
    n_rows = idx.shape[0]
    n_units = n_dev * USTRIDE
    n_copy = 4
    nt = (((1,), (1,)), ((), ()))
    group_barrier(n_dev, me)
    sub_e = lax.broadcasted_iota(i32, (LANES, LANES), 0)
    lane_e = lax.broadcasted_iota(i32, (LANES, LANES), 1)
    ones = jnp.ones((SUB, LANES), bf16)

    @pl.loop(0, n_rows // SUB)
    def _(g):
        base = pl.multiple_of(g * SUB, SUB)
        rows = idx[pl.ds(base, SUB), :]
        parts = []
        for r in range(SUB):
            hot = (sub_e == rows[r:r + 1, :]).astype(bf16)
            parts.append(lax.dot_general(ones, hot, nt, preferred_element_type=f32)[0:1])
        hrow[pl.ds(base, SUB), :] = jnp.concatenate(parts, axis=0)

    hrows = hrow[...]
    hist = jnp.broadcast_to(jnp.sum(hrows, axis=0, keepdims=True), (SUB, LANES)).astype(i32)
    hsend[...] = hist
    hall[me] = hist
    sends = []
    for k in range(1, n_dev):
        copy = pltpu.make_async_remote_copy(src_ref=hsend, dst_ref=hall.at[me], send_sem=ssem.at[k], recv_sem=rsem.at[k], device_id={'ep': lax.rem(me + k, n_dev)}, device_id_type=MESH)
        copy.start()
        sends.append(copy)

    rr = lax.broadcasted_iota(i32, (n_rows, n_rows), 0)
    cc = lax.broadcasted_iota(i32, (n_rows, n_rows), 1)
    hrow[...] = jnp.dot((cc < rr).astype(bf16), hrows.astype(bf16), preferred_element_type=f32)
    tri = (sub_e < lane_e).astype(bf16)

    @pl.loop(0, n_rows // SUB)
    def _(g):
        base = pl.multiple_of(g * SUB, SUB)
        rows = idx[pl.ds(base, SUB), :]
        runs = hrow[pl.ds(base, SUB), :].astype(bf16)
        parts = []
        for r in range(SUB):
            hot = sub_e == rows[r:r + 1, :]
            hot_b = hot.astype(bf16)
            prefix = jnp.dot(hot_b, tri, preferred_element_type=f32)
            run = jnp.dot(runs, hot_b, preferred_element_type=f32)[r:r + 1]
            parts.append(jnp.sum(jnp.where(hot, prefix, 0.0), axis=0, keepdims=True) + run)
        addr[pl.ds(base, SUB), :] = jnp.concatenate(parts, axis=0).astype(i32)

    lane_u = lax.broadcasted_iota(i32, (1, n_units), 1)
    tabrow = jnp.full((1, n_units), -1, i32)
    tabcol[...] = jnp.full(tabcol.shape, -1, i32)
    for d in range(n_dev):
        for s in range(n_slot):
            u = d * USTRIDE + s
            tabrow = jnp.where(lane_u == u, table[d, s], tabrow)
            tabcol[u:u + 1, :] = jnp.full((1, LANES), table[d, s], i32)
    tcol = tabcol[...]
    unit_exp = (tcol == lax.broadcasted_iota(i32, (n_units, LANES), 1)).astype(bf16)
    same = jnp.concatenate([tcol] * (n_units // LANES), axis=1) == tabrow
    su = lax.broadcasted_iota(i32, (n_units, n_units), 0)
    lu = lax.broadcasted_iota(i32, (n_units, n_units), 1)
    valid = tabrow >= 0
    copy_rank = jnp.where(valid, jnp.sum(jnp.where(same & (su < lu), 1.0, 0.0), axis=0, keepdims=True).astype(i32), -1)
    before = ((su < lu) & (lax.shift_right_logical(su, 5) == lax.shift_right_logical(lu, 5))).astype(bf16)
    copies = jnp.dot(jnp.ones((SUB, n_units), bf16), unit_exp, preferred_element_type=f32)[0:1]
    dev8 = lax.broadcasted_iota(i32, (SUB, n_units), 0)
    dev_u = lax.shift_right_logical(lane_u, 5)
    where = [jnp.dot(((dev8 == dev_u) & (copy_rank == k)).astype(bf16), unit_exp, preferred_element_type=f32).astype(bf16) for k in range(n_copy)]

    for k in range(1, n_dev):
        src = lax.rem(me + n_dev - k, n_dev)
        pltpu.make_async_remote_copy(src_ref=hsend, dst_ref=hall.at[src], send_sem=ssem.at[k], recv_sem=rsem.at[k], device_id={'ep': src}, device_id_type=MESH).wait_recv()
    every = jnp.concatenate([hall[p, 0:1, :] for p in range(n_dev)], axis=0).astype(f32)
    taken = level_copies(every, where, copies, float(bound))
    loads = jnp.zeros((n_dev, n_units), f32)
    cum = jnp.zeros((n_dev, LANES), f32)
    for k in range(n_copy):
        per_unit = lax.dot_general(taken[k].astype(bf16), unit_exp, nt, preferred_element_type=f32)
        loads = jnp.where(copy_rank == k, per_unit, loads)
        cums[k * n_dev:(k + 1) * n_dev, :] = cum
        cum = cum + taken[k]
    starts = jnp.dot(loads.astype(bf16), before, preferred_element_type=f32)
    meta[0:n_dev, :] = loads.astype(i32)
    meta[n_dev:2 * n_dev, :] = starts.astype(i32)

    block = lax.rem(dev_u + n_dev - me, n_dev)
    first = meta[pl.ds(n_dev + me, 1), :] + block * stride
    row8 = lax.broadcasted_iota(i32, (2 * n_copy, n_units), 0)
    half = jnp.where(row8 < n_copy, lax.shift_right_logical(first, 6), first & 63)
    half = jnp.where(copy_rank == (row8 & (n_copy - 1)), half, 0)
    place = jnp.dot(half.astype(bf16), unit_exp, preferred_element_type=f32).astype(i32)
    own = [cums[pl.ds(k * n_dev + me, 1), :].astype(i32) for k in range(n_copy)]
    offs = [place[k:k + 1] * 64 + place[n_copy + k:n_copy + k + 1] - own[k] + 256 for k in range(n_copy)]
    bar = [jnp.where(copies > k, own[k], 255) for k in range(1, n_copy)]
    rows = [lax.shift_right_logical(o, 6) for o in offs] + [o & 63 for o in offs] + bar + [jnp.zeros((1, LANES), i32)] * 5
    lookup = jnp.concatenate(rows, axis=0).astype(f32).astype(bf16)

    @pl.loop(0, n_rows // SUB)
    def _(g):
        base = pl.multiple_of(g * SUB, SUB)
        ids = idx[pl.ds(base, SUB), :]
        ranks = addr[pl.ds(base, SUB), :]
        parts = []
        for r in range(SUB):
            rank = ranks[r:r + 1, :]
            hot_b = (sub_e == ids[r:r + 1, :]).astype(bf16)
            got = jnp.dot(lookup, hot_b, preferred_element_type=f32).astype(i32)
            pos = got[0:1] * 64 + got[n_copy:n_copy + 1]
            for k in range(1, n_copy):
                pos = jnp.where(rank >= got[2 * n_copy + k - 1:2 * n_copy + k], got[k:k + 1] * 64 + got[n_copy + k:n_copy + k + 1], pos)
            pos = pos + rank - 256
            parts.append(pos + lax.shift_right_logical(pos, 3) * 40)
        addr[pl.ds(base, SUB), :] = jnp.concatenate(parts, axis=0)

    slot_id = lane_u & (USTRIDE - 1)
    lo_row = jnp.zeros((1, n_units), f32)
    hi_row = jnp.zeros((1, n_units), f32)
    for s in range(n_slot):
        lo_row = jnp.where(slot_id == s, float(low[s]), lo_row)
        hi_row = jnp.where(slot_id == s, float(high[s]), hi_row)
    ends = loads + starts
    bad = jnp.max(jnp.where(valid & ((ends < lo_row) | (ends > hi_row)), 1.0, 0.0))
    top = jnp.max(jnp.where(valid, ends, 0.0))
    tier = jnp.where(bad > 0.0, float(len(caps)), sum(jnp.where(top > float(c), 1.0, 0.0) for c in caps))
    flag[0, 0] = tier.astype(i32)
    for copy in sends:
        copy.wait_send()


def pack_kernel(cap, slow, addr, flag, tok_hbm, send, tok, wide, tmp, stage, tsem, ssem):
    n_rows, n_col = addr.shape
    n_dev, stride = stage.shape[0], stage.shape[1]
    d_tiles = tok.shape[1] // LANES
    step = SUB * d_tiles
    load = pltpu.make_async_copy(tok_hbm, tok, tsem)
    load.start()
    zero_rows = 4 * step

    @pl.loop(0, wide.shape[0] // zero_rows)
    def _(b):
        wide[pl.ds(pl.multiple_of(b * zero_rows, zero_rows), zero_rows), :] = jnp.zeros((zero_rows, LANES), jnp.float32)

    load.wait()

    @pl.loop(0, n_rows)
    def _(r):
        for c in range(n_col // PACK):
            at = c * 2 * step
            x = tok[pl.ds(pl.multiple_of(r * n_col + c * PACK, PACK), PACK), :].astype(jnp.float32)
            for h in range(PACK // SUB):
                for j in range(d_tiles):
                    tmp[at + h * step + j * SUB:at + h * step + (j + 1) * SUB, :] = x[h * SUB:(h + 1) * SUB, j * LANES:(j + 1) * LANES]
            for i in range(PACK):
                a = addr[r, c * PACK + i]
                wide[pl.ds(a, d_tiles, stride=SUB), :] = tmp[pl.ds(at + (i // SUB) * step + i % SUB, d_tiles, stride=SUB), :]

    def narrow(k, b):
        base = (k * (stride // PACK) + b) * (2 * step)
        rows = pl.ds(pl.multiple_of(b * PACK, PACK), PACK)
        for j in range(d_tiles):
            top = wide[pl.ds(base + j * SUB, SUB), :]
            bot = wide[pl.ds(base + step + j * SUB, SUB), :]
            stage[k, rows, j * LANES:(j + 1) * LANES] = jnp.concatenate([top, bot], axis=0).astype(jnp.bfloat16)

    def store(k, lo, hi):
        return pltpu.make_async_copy(stage.at[k, pl.ds(lo, hi - lo)], send.at[k, pl.ds(lo, hi - lo)], ssem.at[k])

    @pl.loop(0, n_dev)
    def _(k):
        @pl.loop(0, cap // PACK, unroll=4)
        def _(b):
            narrow(k, b)

        store(k, 0, cap).start()

    @pl.loop(0, n_dev)
    def _(k):
        store(k, 0, cap).wait()

    @pl.when(flag[0, 0] == slow)
    def _():
        @pl.loop(0, n_dev)
        def _(k):
            @pl.loop(cap // PACK, stride // PACK)
            def _(b):
                narrow(k, b)

            rest = store(k, cap, stride)
            rest.start()
            rest.wait()


def unpack_kernel(cap, slow, addr, flag, gate, back_hbm, out_hbm, back, wide, tmp, out, bsem, osem):
    n_rows, n_col = addr.shape
    n_dev, stride = back.shape[0], back.shape[1]
    d_tiles = out.shape[1] // LANES
    step = SUB * d_tiles

    def load(k, lo, hi):
        return pltpu.make_async_copy(back_hbm.at[k, pl.ds(lo, hi - lo)], back.at[k, pl.ds(lo, hi - lo)], bsem.at[k])

    def widen(k, b):
        base = (k * (stride // PACK) + b) * (2 * step)
        rows = pl.ds(pl.multiple_of(b * PACK, PACK), PACK)
        for j in range(d_tiles):
            x = back[k, rows, j * LANES:(j + 1) * LANES].astype(jnp.float32)
            wide[pl.ds(base + j * SUB, SUB), :] = x[:SUB]
            wide[pl.ds(base + step + j * SUB, SUB), :] = x[SUB:]

    @pl.loop(0, n_dev)
    def _(k):
        load(k, 0, cap).start()

    @pl.loop(0, n_dev)
    def _(k):
        load(k, 0, cap).wait()

        @pl.loop(0, cap // PACK, unroll=4)
        def _(b):
            widen(k, b)

    @pl.when(flag[0, 0] == slow)
    def _():
        @pl.loop(0, n_dev)
        def _(k):
            rest = load(k, cap, stride)
            rest.start()
            rest.wait()

            @pl.loop(cap // PACK, stride // PACK)
            def _(b):
                widen(k, b)

    def give(g):
        rows = pl.ds(pl.multiple_of(g * n_col, n_col), n_col)
        return pltpu.make_async_copy(out.at[rows], out_hbm.at[rows], osem)

    @pl.loop(0, n_rows)
    def _(r):
        for c in range(n_col // PACK):
            at = c * 2 * step
            for i in range(PACK):
                a = addr[r, c * PACK + i]
                g = gate[r, c * PACK + i]
                tmp[pl.ds(at + (i // SUB) * step + i % SUB, d_tiles, stride=SUB), :] = wide[pl.ds(a, d_tiles, stride=SUB), :] * g
            rows = pl.ds(pl.multiple_of(r * n_col + c * PACK, PACK), PACK)
            for j in range(d_tiles):
                top = tmp[at + j * SUB:at + (j + 1) * SUB, :]
                bot = tmp[at + step + j * SUB:at + step + (j + 1) * SUB, :]
                out[rows, j * LANES:(j + 1) * LANES] = jnp.concatenate([top, bot], axis=0).astype(jnp.bfloat16)
        give(r).start()

    @pl.loop(0, n_rows)
    def _(r):
        give(r).wait()


def gelu(x):
    return x * (0.5 * (1.0 + jnp.tanh(0.7978845608028654 * (x + 0.044715 * (x * x * x)))))


def expert_kernel(cfg, meta, send, up_hbm, down_hbm, back, recv, xbuf, ybuf, up, down, hid, xs, win, dsend, drecv, rsend, rrecv, wsem):
    n_dev, n_slot, part = cfg['n_dev'], cfg['n_slot'], cfg['part']
    m_rows = n_dev * part
    d_model, d_ff = up_hbm.shape[1], up_hbm.shape[2]
    first, last, disp, ret, ret_lo = cfg['first'], cfg['last'], cfg['disp'], cfg['ret'], cfg['ret_lo']
    f32, bf16, i32 = jnp.float32, jnp.bfloat16, jnp.int32
    me = lax.axis_index('ep')

    def fetch(s, b):
        return (pltpu.make_async_copy(up_hbm.at[s], up.at[b], wsem.at[0, b]), pltpu.make_async_copy(down_hbm.at[s], down.at[b], wsem.at[1, b]))

    group_barrier(n_dev, me)

    def dispatch(j, k, peer):
        rows = pl.ds(disp[j], disp[j + 1] - disp[j])
        return pltpu.make_async_remote_copy(src_ref=send.at[k, rows], dst_ref=recv.at[k, rows], send_sem=dsend.at[j, k], recv_sem=drecv.at[j, k], device_id={'ep': peer}, device_id_type=MESH)

    def dispatch_own(j):
        rows = pl.ds(disp[j], disp[j + 1] - disp[j])
        return pltpu.make_async_copy(send.at[0, rows], recv.at[0, rows], drecv.at[j, 0])

    order = sorted(range(1, n_dev), key=lambda k: (abs(k - n_dev // 2), k))
    for j in range(len(first)):
        for k in order:
            dispatch(j, k, lax.rem(me + k, n_dev)).start()
        dispatch_own(j).start()
        if j == 0:
            for s in range(2):
                for copy in fetch(s, s):
                    copy.start()

    @pl.loop(0, n_dev)
    def _(k):
        @pl.loop(0, xbuf.shape[1])
        def _(b):
            xbuf[k, b] = jnp.zeros((PACK, d_model), bf16)

    def ffn(s, b):
        unit = me * USTRIDE + s
        lane = lax.broadcasted_iota(i32, (1, n_dev * WIN), 1)
        which = lax.shift_right_logical(lane, 6)
        off = jnp.zeros((1, n_dev * WIN), i32)
        num = jnp.zeros((1, n_dev * WIN), i32)
        for k in range(n_dev):
            src = lax.rem(me + n_dev - k, n_dev)
            load, start = meta[src, unit], meta[n_dev + src, unit]
            blk = lax.shift_right_logical(start, 4)
            base = blk * PACK
            for q in range(WIN // PACK):
                win[k * WIN + q * PACK:k * WIN + (q + 1) * PACK, :] = xbuf[k, blk + q]
            off = jnp.where(which == k, base - start, off)
            num = jnp.where(which == k, load, num)
        nth = (lane & (WIN - 1)) + off
        target = jnp.where((nth >= 0) & (nth < num), nth + which * part, -1)
        pick = (lax.broadcasted_iota(i32, (m_rows, n_dev * WIN), 0) == target).astype(bf16)
        xs[...] = jnp.dot(pick, win[...], preferred_element_type=f32).astype(bf16)
        tile = 512
        for t in range(d_ff // tile):
            pre = jnp.dot(xs[...], up[b, :, t * tile:(t + 1) * tile], preferred_element_type=f32)
            hid[:, t * tile:(t + 1) * tile] = gelu(pre).astype(bf16)
        tile = 256
        for t in range(d_model // tile):
            o = jnp.dot(hid[...], down[b, :, t * tile:(t + 1) * tile], preferred_element_type=f32).astype(bf16)
            for k in range(n_dev):
                ybuf[k, pl.ds(pl.multiple_of(s * part, PACK), part), t * tile:(t + 1) * tile] = o[k * part:(k + 1) * part]

    def give_back(j, k):
        rows = pl.ds(ret[j], ret[j + 1] - ret[j])
        peer = lax.rem(me + n_dev - k, n_dev)
        return pltpu.make_async_remote_copy(src_ref=recv.at[k, rows], dst_ref=back.at[k, rows], send_sem=rsend.at[j, k], recv_sem=rrecv.at[j, k], device_id={'ep': peer}, device_id_type=MESH)

    def give_own(j):
        rows = pl.ds(ret[j], ret[j + 1] - ret[j])
        return pltpu.make_async_copy(recv.at[0, rows], back.at[0, rows], rrecv.at[j, 0])

    def combine(j):
        n_rows = ret[j + 1] - ret[j]
        n_win = last[j] + 1 - ret_lo[j]
        width = n_win * part

        @pl.loop(0, n_dev)
        def _(i):
            k = lax.rem(n_dev // 2 + 3 * i, n_dev)
            src = lax.rem(me + n_dev - k, n_dev)
            lane = lax.broadcasted_iota(i32, (1, width), 1)
            target = jnp.full((1, width), -1, i32)
            for w in range(n_win):
                unit = me * USTRIDE + ret_lo[j] + w
                load, start = meta[src, unit], meta[n_dev + src, unit]
                nth = lane - w * part
                target = jnp.where((nth >= 0) & (nth < load), nth + start, target)
            pick = (lax.broadcasted_iota(i32, (n_rows, width), 0) + ret[j] == target).astype(bf16)
            rows = ybuf[k, ret_lo[j] * part:(last[j] + 1) * part, :]
            recv[k, ret[j]:ret[j + 1], :] = jnp.dot(pick, rows, preferred_element_type=f32).astype(bf16)

            @pl.when(k == 0)
            def _():
                give_own(j).start()

            @pl.when(k != 0)
            def _():
                give_back(j, k).start()

    @pl.loop(0, n_slot)
    def _(s):
        for j in range(len(first)):
            @pl.when(s == first[j])
            def _():
                for k in range(1, n_dev):
                    dispatch(j, k, lax.rem(me + n_dev - k, n_dev)).wait_recv()
                dispatch_own(j).wait()

                @pl.loop(0, n_dev)
                def _(k):
                    @pl.loop(disp[j] // PACK, disp[j + 1] // PACK)
                    def _(b):
                        xbuf[k, b] = recv[k, pl.ds(pl.multiple_of(b * PACK, PACK), PACK), :]

        b = lax.rem(s, 2)
        for copy in fetch(s, b):
            copy.wait()
        ffn(s, b)

        @pl.when(s + 2 < n_slot)
        def _():
            for copy in fetch(s + 2, b):
                copy.start()

        for j in range(len(last)):
            @pl.when(s == last[j])
            def _():
                combine(j)

    for k in range(1, n_dev):
        for j in range(len(first)):
            dispatch(j, k, lax.rem(me + k, n_dev)).wait_send()
        for j in range(len(last)):
            give_back(j, k).wait_send()
            give_back(j, k).wait_recv()
    for j in range(len(last)):
        give_own(j).wait()


def plan(n_dev, n_slot, n_pairs, bound, z, cap, groups, returns):
    mean = n_pairs / (n_dev * n_slot)
    spread = 9.3 * mean / 30.1
    hi = [bound * (s + 1) for s in range(n_slot)]
    lo = [0] * n_slot
    if z is not None:
        hi = [min(hi[s], math.ceil(mean * (s + 1) + z * spread * math.sqrt(s + 1)), cap) for s in range(n_slot)]
        lo = [max(0, math.floor(mean * (s + 1) - z * spread * math.sqrt(s + 1))) for s in range(n_slot - 1)] + [0]
    disp = [0] + [min(cap, up_to(hi[s], PACK)) for s in groups[:-1]] + [cap]
    ret = [0] + [lo[s] // PACK * PACK for s in returns[:-1]] + [cap]
    ret_lo = [min(s for s in range(n_slot) if hi[s] > ret[j]) for j in range(len(returns))]
    first = [0] + [s + 1 for s in groups[:-1]]
    return dict(n_dev=n_dev, n_slot=n_slot, cap=cap, lo=lo, hi=hi, first=first, last=list(returns), disp=disp, ret=ret, ret_lo=ret_lo, part=up_to(bound, PACK))


def solution(mesh):
    n_dev = mesh.shape['ep']

    def group_layer(tokens, topk_idx, topk_w, w_up, w_down, slot_expert):
        n_tok, d_model = tokens.shape
        n_slot = slot_expert.shape[1]
        d_ff = w_up.shape[3]
        n_pairs = n_tok * topk_idx.shape[1]
        base_load = n_pairs // (n_dev * n_slot)
        bound = base_load + base_load // 2 + 1
        mean = n_pairs // n_dev
        stride = up_to(n_slot * bound, PACK)
        caps = [min(stride, up_to(math.ceil(mean * f), PACK)) for f in TIERS]
        cuts = [n_slot * c // 17 - 1 for c in (4, 8, 12, 15, 17)]
        plans = [plan(n_dev, n_slot, n_pairs, bound, 4.0, c, cuts[:3] + cuts[4:], cuts) for c in caps]
        plans.append(plan(n_dev, n_slot, n_pairs, bound, None, stride, [n_slot - 1], [n_slot - 1]))
        wide_bounds = plan(n_dev, n_slot, n_pairs, bound, 4.0, stride, cuts, cuts)
        n_rows = n_pairs // LANES
        n_units = n_dev * USTRIDE
        f32, bf16, i32 = jnp.float32, jnp.bfloat16, jnp.int32
        vmem = pl.BlockSpec(memory_space=pltpu.VMEM)
        smem = pl.BlockSpec(memory_space=pltpu.SMEM)
        hbm = pl.BlockSpec(memory_space=pl.ANY)
        big = 63 * 1024 * 1024

        addr, meta, flag = pl.pallas_call(
            functools.partial(route_kernel, n_dev, n_slot, stride, bound, wide_bounds['lo'], wide_bounds['hi'], caps),
            out_shape=[jax.ShapeDtypeStruct((n_rows, LANES), i32), jax.ShapeDtypeStruct((2 * n_dev, n_units), i32), jax.ShapeDtypeStruct((1, 1), i32)],
            in_specs=[vmem, smem],
            out_specs=[vmem, vmem, smem],
            scratch_shapes=[pltpu.VMEM((SUB, LANES), i32), pltpu.VMEM((n_dev, SUB, LANES), i32), pltpu.VMEM((n_rows, LANES), f32), pltpu.VMEM((n_units, LANES), i32), pltpu.VMEM((4 * n_dev, LANES), f32), pltpu.SemaphoreType.DMA((n_dev,)), pltpu.SemaphoreType.DMA((n_dev,))],
            compiler_params=pltpu.CompilerParams(collective_id=0, has_side_effects=True),
            name='route',
        )(topk_idx.reshape(n_rows, LANES), slot_expert)

        d_tiles = d_model // LANES
        wide = pltpu.VMEM((n_dev * stride * d_tiles, LANES), f32)
        tmp = pltpu.VMEM((LANES * d_tiles, LANES), f32)
        block = pltpu.VMEM((n_dev, stride, d_model), bf16)
        rows_vmem = pltpu.VMEM((n_tok, d_model), bf16)
        sem, sems = pltpu.SemaphoreType.DMA, pltpu.SemaphoreType.DMA((n_dev,))
        send = pl.pallas_call(
            functools.partial(pack_kernel, caps[-1], len(caps)),
            out_shape=jax.ShapeDtypeStruct((n_dev, stride, d_model), bf16),
            in_specs=[smem, smem, hbm],
            out_specs=hbm,
            scratch_shapes=[rows_vmem, wide, tmp, block, sem, sems],
            compiler_params=pltpu.CompilerParams(vmem_limit_bytes=big),
            name='pack',
        )(addr, flag, tokens)

        def run(cfg, meta, send, w_up, w_down):
            part, cap = cfg['part'], cfg['cap']
            m_rows = n_dev * part
            sent = pltpu.SemaphoreType.DMA((len(cfg['first']), n_dev))
            given = pltpu.SemaphoreType.DMA((len(cfg['last']), n_dev))
            return pl.pallas_call(
                functools.partial(expert_kernel, cfg),
                out_shape=jax.ShapeDtypeStruct((n_dev, stride, d_model), bf16),
                in_specs=[smem, hbm, hbm, hbm],
                out_specs=hbm,
                scratch_shapes=[
                    pltpu.VMEM((n_dev, cap, d_model), bf16),
                    pltpu.VMEM((n_dev, (cap + WIN) // PACK, PACK, d_model), bf16),
                    pltpu.VMEM((n_dev, n_slot * part, d_model), bf16),
                    pltpu.VMEM((2, d_model, d_ff), bf16),
                    pltpu.VMEM((2, d_ff, d_model), bf16),
                    pltpu.VMEM((m_rows, d_ff), bf16),
                    pltpu.VMEM((m_rows, d_model), bf16),
                    pltpu.VMEM((n_dev * WIN, d_model), bf16),
                    sent, sent, given, given,
                    pltpu.SemaphoreType.DMA((2, 2)),
                ],
                compiler_params=pltpu.CompilerParams(collective_id=1, has_side_effects=True, vmem_limit_bytes=big),
                name='experts',
            )(meta, send, w_up, w_down)

        back = lax.switch(flag[0, 0], [functools.partial(run, p) for p in plans], meta, send, w_up[0], w_down[0])

        return pl.pallas_call(
            functools.partial(unpack_kernel, caps[-1], len(caps)),
            out_shape=jax.ShapeDtypeStruct((n_tok, d_model), bf16),
            in_specs=[smem, smem, smem, hbm],
            out_specs=hbm,
            scratch_shapes=[block, wide, tmp, rows_vmem, sems, sem],
            compiler_params=pltpu.CompilerParams(vmem_limit_bytes=big),
            name='unpack',
        )(addr, flag, topk_w.reshape(n_rows, LANES), back)

    row_spec = P(('dp', 'ep'), None)
    weight_spec = P('ep', None, None, None)
    return jax.shard_map(group_layer, mesh=mesh, in_specs=(row_spec, row_spec, row_spec, weight_spec, weight_spec, P(None, None)), out_specs=row_spec, check_vma=False)
```

```python
import functools
import math

import jax
import jax.numpy as jnp
from jax import lax
from jax.experimental import pallas as pl
from jax.experimental.pallas import tpu as pltpu
from jax.sharding import PartitionSpec as P

MESH = pl.DeviceIdType.MESH
LANES = 128
SUB = 8
PACK = 16
USTRIDE = 32
WIN = 64
STEP = 32
CHUNK = 128
TIERS = (1.125, 1.156, 1.21875)


def up_to(x, m):
    return -(-x // m) * m


def group_barrier(n_dev, me):
    barrier = pltpu.get_barrier_semaphore()
    for k in range(1, n_dev):
        pl.semaphore_signal(barrier, inc=1, device_id={'ep': lax.rem(me + k, n_dev)}, device_id_type=MESH)
    pl.semaphore_wait(barrier, n_dev - 1)


def level_copies(loads, where, copies, bound):
    n_copy = len(where)
    f32, bf16 = jnp.float32, jnp.bfloat16
    share = [jnp.where(k < copies, loads / jnp.maximum(copies, 1.0), 0.0) for k in range(n_copy)]
    for _ in range(2):
        block = sum(lax.dot_general(share[k].astype(bf16), where[k], (((1,), (1,)), ((), ())), preferred_element_type=f32) for k in range(n_copy))
        there = [jnp.where(k < copies, jnp.dot(block.astype(bf16), where[k], preferred_element_type=f32), 0.0) for k in range(n_copy)]
        mean = sum(there) / jnp.maximum(copies, 1.0)
        share = [jnp.where(k < copies, jnp.clip(share[k] + 0.5 * (mean - there[k]), 0.0, bound), 0.0) for k in range(n_copy)]
    left, taken = loads, []
    for k in range(n_copy):
        after = jnp.maximum(copies - (k + 1), 0.0)
        want = jnp.floor(share[k] + 0.5)
        got = jnp.minimum(jnp.maximum(want, jnp.maximum(left - bound * after, 0.0)), jnp.minimum(left, bound))
        got = jnp.where(k < copies, got, 0.0)
        taken.append(got)
        left = left - got
    return taken


def route_kernel(n_dev, n_slot, stride, bound, low, high, caps, idx, table, addr, meta, flag, hsend, hall, hrow, tabcol, cums, ssem, rsem):
    me = lax.axis_index('ep')
    f32, bf16, i32 = jnp.float32, jnp.bfloat16, jnp.int32
    n_rows = idx.shape[0]
    n_units = n_dev * USTRIDE
    n_copy = 4
    nt = (((1,), (1,)), ((), ()))
    group_barrier(n_dev, me)
    sub_e = lax.broadcasted_iota(i32, (LANES, LANES), 0)
    lane_e = lax.broadcasted_iota(i32, (LANES, LANES), 1)
    ones = jnp.ones((SUB, LANES), bf16)

    @pl.loop(0, n_rows // SUB)
    def _(g):
        base = pl.multiple_of(g * SUB, SUB)
        rows = idx[pl.ds(base, SUB), :]
        parts = []
        for r in range(SUB):
            hot = (sub_e == rows[r:r + 1, :]).astype(bf16)
            parts.append(lax.dot_general(ones, hot, nt, preferred_element_type=f32)[0:1])
        hrow[pl.ds(base, SUB), :] = jnp.concatenate(parts, axis=0)

    hrows = hrow[...]
    hist = jnp.broadcast_to(jnp.sum(hrows, axis=0, keepdims=True), (SUB, LANES)).astype(i32)
    hsend[...] = hist
    hall[me] = hist
    sends = []
    for k in range(1, n_dev):
        copy = pltpu.make_async_remote_copy(src_ref=hsend, dst_ref=hall.at[me], send_sem=ssem.at[k], recv_sem=rsem.at[k], device_id={'ep': lax.rem(me + k, n_dev)}, device_id_type=MESH)
        copy.start()
        sends.append(copy)

    rr = lax.broadcasted_iota(i32, (n_rows, n_rows), 0)
    cc = lax.broadcasted_iota(i32, (n_rows, n_rows), 1)
    hrow[...] = jnp.dot((cc < rr).astype(bf16), hrows.astype(bf16), preferred_element_type=f32)
    tri = (sub_e < lane_e).astype(bf16)

    @pl.loop(0, n_rows // SUB)
    def _(g):
        base = pl.multiple_of(g * SUB, SUB)
        rows = idx[pl.ds(base, SUB), :]
        runs = hrow[pl.ds(base, SUB), :].astype(bf16)
        parts = []
        for r in range(SUB):
            hot = sub_e == rows[r:r + 1, :]
            hot_b = hot.astype(bf16)
            prefix = jnp.dot(hot_b, tri, preferred_element_type=f32)
            run = jnp.dot(runs, hot_b, preferred_element_type=f32)[r:r + 1]
            parts.append(jnp.sum(jnp.where(hot, prefix, 0.0), axis=0, keepdims=True) + run)
        addr[pl.ds(base, SUB), :] = jnp.concatenate(parts, axis=0).astype(i32)

    lane_u = lax.broadcasted_iota(i32, (1, n_units), 1)
    tabrow = jnp.full((1, n_units), -1, i32)
    tabcol[...] = jnp.full(tabcol.shape, -1, i32)
    for d in range(n_dev):
        for s in range(n_slot):
            u = d * USTRIDE + s
            tabrow = jnp.where(lane_u == u, table[d, s], tabrow)
            tabcol[u:u + 1, :] = jnp.full((1, LANES), table[d, s], i32)
    tcol = tabcol[...]
    unit_exp = (tcol == lax.broadcasted_iota(i32, (n_units, LANES), 1)).astype(bf16)
    same = jnp.concatenate([tcol] * (n_units // LANES), axis=1) == tabrow
    su = lax.broadcasted_iota(i32, (n_units, n_units), 0)
    lu = lax.broadcasted_iota(i32, (n_units, n_units), 1)
    valid = tabrow >= 0
    copy_rank = jnp.where(valid, jnp.sum(jnp.where(same & (su < lu), 1.0, 0.0), axis=0, keepdims=True).astype(i32), -1)
    before = ((su < lu) & (lax.shift_right_logical(su, 5) == lax.shift_right_logical(lu, 5))).astype(bf16)
    copies = jnp.dot(jnp.ones((SUB, n_units), bf16), unit_exp, preferred_element_type=f32)[0:1]
    dev8 = lax.broadcasted_iota(i32, (SUB, n_units), 0)
    dev_u = lax.shift_right_logical(lane_u, 5)
    where = [jnp.dot(((dev8 == dev_u) & (copy_rank == k)).astype(bf16), unit_exp, preferred_element_type=f32).astype(bf16) for k in range(n_copy)]

    for k in range(1, n_dev):
        src = lax.rem(me + n_dev - k, n_dev)
        pltpu.make_async_remote_copy(src_ref=hsend, dst_ref=hall.at[src], send_sem=ssem.at[k], recv_sem=rsem.at[k], device_id={'ep': src}, device_id_type=MESH).wait_recv()
    every = jnp.concatenate([hall[p, 0:1, :] for p in range(n_dev)], axis=0).astype(f32)
    taken = level_copies(every, where, copies, float(bound))
    loads = jnp.zeros((n_dev, n_units), f32)
    cum = jnp.zeros((n_dev, LANES), f32)
    for k in range(n_copy):
        per_unit = lax.dot_general(taken[k].astype(bf16), unit_exp, nt, preferred_element_type=f32)
        loads = jnp.where(copy_rank == k, per_unit, loads)
        cums[k * n_dev:(k + 1) * n_dev, :] = cum
        cum = cum + taken[k]
    starts = jnp.dot(loads.astype(bf16), before, preferred_element_type=f32)
    meta[0:n_dev, :] = loads.astype(i32)
    meta[n_dev:2 * n_dev, :] = starts.astype(i32)

    block = lax.rem(dev_u + n_dev - me, n_dev)
    first = meta[pl.ds(n_dev + me, 1), :] + block * stride
    row8 = lax.broadcasted_iota(i32, (2 * n_copy, n_units), 0)
    half = jnp.where(row8 < n_copy, lax.shift_right_logical(first, 6), first & 63)
    half = jnp.where(copy_rank == (row8 & (n_copy - 1)), half, 0)
    place = jnp.dot(half.astype(bf16), unit_exp, preferred_element_type=f32).astype(i32)
    own = [cums[pl.ds(k * n_dev + me, 1), :].astype(i32) for k in range(n_copy)]
    offs = [place[k:k + 1] * 64 + place[n_copy + k:n_copy + k + 1] - own[k] + 256 for k in range(n_copy)]
    bar = [jnp.where(copies > k, own[k], 255) for k in range(1, n_copy)]
    rows = [lax.shift_right_logical(o, 6) for o in offs] + [o & 63 for o in offs] + bar + [jnp.zeros((1, LANES), i32)] * 5
    lookup = jnp.concatenate(rows, axis=0).astype(f32).astype(bf16)

    @pl.loop(0, n_rows // SUB)
    def _(g):
        base = pl.multiple_of(g * SUB, SUB)
        ids = idx[pl.ds(base, SUB), :]
        ranks = addr[pl.ds(base, SUB), :]
        parts = []
        for r in range(SUB):
            rank = ranks[r:r + 1, :]
            hot_b = (sub_e == ids[r:r + 1, :]).astype(bf16)
            got = jnp.dot(lookup, hot_b, preferred_element_type=f32).astype(i32)
            pos = got[0:1] * 64 + got[n_copy:n_copy + 1]
            for k in range(1, n_copy):
                pos = jnp.where(rank >= got[2 * n_copy + k - 1:2 * n_copy + k], got[k:k + 1] * 64 + got[n_copy + k:n_copy + k + 1], pos)
            pos = pos + rank - 256
            parts.append(pos + lax.shift_right_logical(pos, 3) * 40)
        addr[pl.ds(base, SUB), :] = jnp.concatenate(parts, axis=0)

    slot_id = lane_u & (USTRIDE - 1)
    lo_row = jnp.zeros((1, n_units), f32)
    hi_row = jnp.zeros((1, n_units), f32)
    for s in range(n_slot):
        lo_row = jnp.where(slot_id == s, float(low[s]), lo_row)
        hi_row = jnp.where(slot_id == s, float(high[s]), hi_row)
    ends = loads + starts
    bad = jnp.max(jnp.where(valid & ((ends < lo_row) | (ends > hi_row)), 1.0, 0.0))
    top = jnp.max(jnp.where(valid, ends, 0.0))
    tier = jnp.where(bad > 0.0, float(len(caps)), sum(jnp.where(top > float(c), 1.0, 0.0) for c in caps))
    flag[0, 0] = tier.astype(i32)
    for copy in sends:
        copy.wait_send()


def unpack_kernel(cap, slow, addr, flag, gate, back_hbm, out_hbm, back, wide, tmp, out, bsem, osem):
    n_rows, n_col = addr.shape
    n_dev, stride = back.shape[0], back.shape[1] * PACK
    d_tiles = out.shape[1] // LANES
    step = SUB * d_tiles

    def load(k, lo, hi):
        rows = pl.ds(lo // PACK, (hi - lo) // PACK)
        return pltpu.make_async_copy(back_hbm.at[k, rows], back.at[k, rows], bsem.at[k])

    def widen(k, b):
        base = (k * (stride // PACK) + b) * (2 * step)
        for j in range(d_tiles):
            x = back[k, b, :, j * LANES:(j + 1) * LANES].astype(jnp.float32)
            wide[pl.ds(base + j * SUB, SUB), :] = x[:SUB]
            wide[pl.ds(base + step + j * SUB, SUB), :] = x[SUB:]

    @pl.loop(0, n_dev)
    def _(k):
        load(k, 0, cap).start()

    @pl.loop(0, n_dev)
    def _(k):
        load(k, 0, cap).wait()

        @pl.loop(0, cap // PACK, unroll=4)
        def _(b):
            widen(k, b)

    @pl.when(flag[0, 0] == slow)
    def _():
        @pl.loop(0, n_dev)
        def _(k):
            rest = load(k, cap, stride)
            rest.start()
            rest.wait()

            @pl.loop(cap // PACK, stride // PACK)
            def _(b):
                widen(k, b)

    def give(g):
        rows = pl.ds(pl.multiple_of(g * n_col, n_col), n_col)
        return pltpu.make_async_copy(out.at[rows], out_hbm.at[rows], osem)

    @pl.loop(0, n_rows)
    def _(r):
        for c in range(n_col // PACK):
            at = c * 2 * step
            for i in range(PACK):
                a = addr[r, c * PACK + i]
                g = gate[r, c * PACK + i]
                tmp[pl.ds(at + (i // SUB) * step + i % SUB, d_tiles, stride=SUB), :] = wide[pl.ds(a, d_tiles, stride=SUB), :] * g
            rows = pl.ds(pl.multiple_of(r * n_col + c * PACK, PACK), PACK)
            for j in range(d_tiles):
                top = tmp[at + j * SUB:at + (j + 1) * SUB, :]
                bot = tmp[at + step + j * SUB:at + step + (j + 1) * SUB, :]
                out[rows, j * LANES:(j + 1) * LANES] = jnp.concatenate([top, bot], axis=0).astype(jnp.bfloat16)
        give(r).start()

    @pl.loop(0, n_rows)
    def _(r):
        give(r).wait()


def gelu(x):
    return x * (0.5 * (1.0 + jnp.tanh(0.7978845608028654 * (x + 0.044715 * (x * x * x)))))


def expert_kernel(cfg, meta, addr, tok_hbm, up_hbm, down_hbm, back, tok, recv, xbuf, ybuf, up, down, mix, xs, win, dsend, drecv, rsend, rrecv, wsem, tsem):
    n_dev, n_slot, part, stride = cfg['n_dev'], cfg['n_slot'], cfg['part'], cfg['stride']
    m_rows = n_dev * part
    n_tok, d_model, d_ff = tok.shape[0], up_hbm.shape[1], up_hbm.shape[2]
    first, last, disp, ret, ret_lo = cfg['first'], cfg['last'], cfg['disp'], cfg['ret'], cfg['ret_lo']
    n_step = -(-disp[-1] // STEP)
    f32, bf16, i32 = jnp.float32, jnp.bfloat16, jnp.int32
    me = lax.axis_index('ep')

    def fetch(s, b):
        return (pltpu.make_async_copy(up_hbm.at[s], up.at[b], wsem.at[0, b]), pltpu.make_async_copy(down_hbm.at[s], down.at[b], wsem.at[1, b]))

    load_tok = pltpu.make_async_copy(tok_hbm, tok, tsem)
    load_tok.start()
    group_barrier(n_dev, me)
    tail = n_step * (STEP // PACK)

    @pl.loop(0, n_dev)
    def _(k):
        xbuf[k, tail:] = jnp.zeros((xbuf.shape[1] - tail, PACK, d_model), bf16)

    def dispatch(j, k, peer, lo, num):
        return pltpu.make_async_remote_copy(src_ref=xbuf.at[k, pl.ds(lo, num)], dst_ref=recv.at[k, pl.ds(lo, num)], send_sem=dsend.at[j, k], recv_sem=drecv.at[j, k], device_id={'ep': peer}, device_id_type=MESH)

    def dispatched(j, k, peer):
        return dispatch(j, k, peer, disp[j] // PACK, (disp[j + 1] - disp[j]) // PACK)

    order = sorted(range(1, n_dev), key=lambda k: (abs(k - n_dev // 2), k))
    whole = disp[-1] // STEP
    load_tok.wait()

    @pl.loop(0, n_step)
    def _(u):
        row = lax.broadcasted_iota(i32, (n_dev * STEP, LANES), 0)
        pos = lax.shift_right_logical(row, 5) * stride + (row & (STEP - 1)) + u * STEP
        want = pos + lax.shift_right_logical(pos, 3) * 40
        for q in range(n_tok // LANES):
            mix[:n_dev * STEP, q * LANES:(q + 1) * LANES] = (want == addr[q:q + 1, :]).astype(bf16)
        rows = jnp.dot(mix[:n_dev * STEP, :n_tok], tok[...], preferred_element_type=f32).astype(bf16)
        for k in range(n_dev):
            for h in range(STEP // PACK):
                at = k * STEP + h * PACK
                xbuf[k, u * (STEP // PACK) + h] = rows[at:at + PACK]
        j = u // (CHUNK // STEP) if len(first) > 1 else 0

        @pl.when(u < whole)
        def _():
            for k in order:
                dispatch(j, k, lax.rem(me + k, n_dev), u * (STEP // PACK), STEP // PACK).start()

        if whole < n_step:
            @pl.when(u == whole)
            def _():
                for k in order:
                    dispatch(j, k, lax.rem(me + k, n_dev), u * (STEP // PACK), (disp[-1] - whole * STEP) // PACK).start()

        @pl.when(u == 0)
        def _():
            for s in range(2):
                for copy in fetch(s, s):
                    copy.start()

    def ffn(s, b):
        unit = me * USTRIDE + s
        lane = lax.broadcasted_iota(i32, (1, n_dev * WIN), 1)
        which = lax.shift_right_logical(lane, 6)
        off = jnp.zeros((1, n_dev * WIN), i32)
        num = jnp.zeros((1, n_dev * WIN), i32)
        for k in range(n_dev):
            src = lax.rem(me + n_dev - k, n_dev)
            load, start = meta[src, unit], meta[n_dev + src, unit]
            blk = lax.shift_right_logical(start, 4)
            base = blk * PACK
            for q in range(WIN // PACK):
                win[k * WIN + q * PACK:k * WIN + (q + 1) * PACK, :] = xbuf[k, blk + q]
            off = jnp.where(which == k, base - start, off)
            num = jnp.where(which == k, load, num)
        nth = (lane & (WIN - 1)) + off
        target = jnp.where((nth >= 0) & (nth < num), nth + which * part, -1)
        pick = (lax.broadcasted_iota(i32, (m_rows, n_dev * WIN), 0) == target).astype(bf16)
        xs[...] = jnp.dot(pick, win[...], preferred_element_type=f32).astype(bf16)
        tile = 512
        for t in range(d_ff // tile):
            pre = jnp.dot(xs[...], up[b, :, t * tile:(t + 1) * tile], preferred_element_type=f32)
            mix[:, t * tile:(t + 1) * tile] = gelu(pre).astype(bf16)
        tile = 256
        for t in range(d_model // tile):
            o = jnp.dot(mix[:, :d_ff], down[b, :, t * tile:(t + 1) * tile], preferred_element_type=f32).astype(bf16)
            for k in range(n_dev):
                ybuf[k, pl.ds(pl.multiple_of(s * part, PACK), part), t * tile:(t + 1) * tile] = o[k * part:(k + 1) * part]

    def give_back(j, k):
        rows = pl.ds(ret[j] // PACK, (ret[j + 1] - ret[j]) // PACK)
        peer = lax.rem(me + n_dev - k, n_dev)
        return pltpu.make_async_remote_copy(src_ref=recv.at[k, rows], dst_ref=back.at[k, rows], send_sem=rsend.at[j, k], recv_sem=rrecv.at[j, k], device_id={'ep': peer}, device_id_type=MESH)

    def give_own(j):
        rows = pl.ds(ret[j] // PACK, (ret[j + 1] - ret[j]) // PACK)
        return pltpu.make_async_copy(recv.at[0, rows], back.at[0, rows], rrecv.at[j, 0])

    def combine(j):
        n_rows = ret[j + 1] - ret[j]
        n_win = last[j] + 1 - ret_lo[j]
        width = n_win * part

        @pl.loop(0, n_dev)
        def _(i):
            k = lax.rem(n_dev // 2 + 3 * i, n_dev)
            src = lax.rem(me + n_dev - k, n_dev)
            lane = lax.broadcasted_iota(i32, (1, width), 1)
            target = jnp.full((1, width), -1, i32)
            for w in range(n_win):
                unit = me * USTRIDE + ret_lo[j] + w
                load, start = meta[src, unit], meta[n_dev + src, unit]
                nth = lane - w * part
                target = jnp.where((nth >= 0) & (nth < load), nth + start, target)
            pick = (lax.broadcasted_iota(i32, (n_rows, width), 0) + ret[j] == target).astype(bf16)
            rows = ybuf[k, ret_lo[j] * part:(last[j] + 1) * part, :]
            mixed = jnp.dot(pick, rows, preferred_element_type=f32).astype(bf16)
            recv[k, ret[j] // PACK:ret[j + 1] // PACK] = mixed.reshape(n_rows // PACK, PACK, d_model)

            @pl.when(k == 0)
            def _():
                give_own(j).start()

            @pl.when(k != 0)
            def _():
                give_back(j, k).start()

    @pl.loop(0, n_slot)
    def _(s):
        for j in range(len(first)):
            @pl.when(s == first[j])
            def _():
                for k in range(1, n_dev):
                    dispatched(j, k, lax.rem(me + n_dev - k, n_dev)).wait_recv()
                    dispatched(j, k, lax.rem(me + k, n_dev)).wait_send()

                @pl.loop(1, n_dev)
                def _(k):
                    @pl.loop(disp[j] // PACK, disp[j + 1] // PACK)
                    def _(b):
                        xbuf[k, b] = recv[k, b]

        b = lax.rem(s, 2)
        for copy in fetch(s, b):
            copy.wait()
        ffn(s, b)

        @pl.when(s + 2 < n_slot)
        def _():
            for copy in fetch(s + 2, b):
                copy.start()

        for j in range(len(last)):
            @pl.when(s == last[j])
            def _():
                combine(j)

    for k in range(1, n_dev):
        for j in range(len(last)):
            give_back(j, k).wait_send()
            give_back(j, k).wait_recv()
    for j in range(len(last)):
        give_own(j).wait()


def plan(n_dev, n_slot, n_pairs, bound, stride, z, cap, returns):
    mean = n_pairs / (n_dev * n_slot)
    spread = 9.3 * mean / 30.1
    hi = [bound * (s + 1) for s in range(n_slot)]
    lo = [0] * n_slot
    if z is not None:
        hi = [min(hi[s], math.ceil(mean * (s + 1) + z * spread * math.sqrt(s + 1)), cap) for s in range(n_slot)]
        lo = [max(0, math.floor(mean * (s + 1) - z * spread * math.sqrt(s + 1))) for s in range(n_slot - 1)] + [0]
    disp = [0, cap] if z is None else list(range(0, cap, CHUNK)) + [cap]
    ret = [0] + [lo[s] // PACK * PACK for s in returns[:-1]] + [cap]
    ret_lo = [min(s for s in range(n_slot) if hi[s] > ret[j]) for j in range(len(returns))]
    first = [min((s for s in range(n_slot) if hi[s] > d), default=n_slot - 1) for d in disp[:-1]]
    return dict(n_dev=n_dev, n_slot=n_slot, cap=cap, stride=stride, lo=lo, hi=hi, first=first, last=list(returns), disp=disp, ret=ret, ret_lo=ret_lo, part=up_to(bound, PACK))


def solution(mesh):
    n_dev = mesh.shape['ep']

    def group_layer(tokens, topk_idx, topk_w, w_up, w_down, slot_expert):
        n_tok, d_model = tokens.shape
        n_slot = slot_expert.shape[1]
        d_ff = w_up.shape[3]
        n_pairs = n_tok * topk_idx.shape[1]
        base_load = n_pairs // (n_dev * n_slot)
        bound = base_load + base_load // 2 + 1
        mean = n_pairs // n_dev
        stride = up_to(n_slot * bound, PACK)
        caps = [min(stride, up_to(math.ceil(mean * f), PACK)) for f in TIERS]
        cuts = [n_slot * c // 17 - 1 for c in (5, 9, 12, 15, 17)]
        plans = [plan(n_dev, n_slot, n_pairs, bound, stride, 4.0, c, cuts) for c in caps]
        plans.append(plan(n_dev, n_slot, n_pairs, bound, stride, None, stride, [n_slot - 1]))
        wide_bounds = plan(n_dev, n_slot, n_pairs, bound, stride, 4.0, stride, cuts)
        n_rows = n_pairs // LANES
        n_units = n_dev * USTRIDE
        f32, bf16, i32 = jnp.float32, jnp.bfloat16, jnp.int32
        vmem = pl.BlockSpec(memory_space=pltpu.VMEM)
        smem = pl.BlockSpec(memory_space=pltpu.SMEM)
        hbm = pl.BlockSpec(memory_space=pl.ANY)
        big = 63 * 1024 * 1024

        addr, meta, flag = pl.pallas_call(
            functools.partial(route_kernel, n_dev, n_slot, stride, bound, wide_bounds['lo'], wide_bounds['hi'], caps),
            out_shape=[jax.ShapeDtypeStruct((n_rows, LANES), i32), jax.ShapeDtypeStruct((2 * n_dev, n_units), i32), jax.ShapeDtypeStruct((1, 1), i32)],
            in_specs=[vmem, smem],
            out_specs=[vmem, vmem, smem],
            scratch_shapes=[pltpu.VMEM((SUB, LANES), i32), pltpu.VMEM((n_dev, SUB, LANES), i32), pltpu.VMEM((n_rows, LANES), f32), pltpu.VMEM((n_units, LANES), i32), pltpu.VMEM((4 * n_dev, LANES), f32), pltpu.SemaphoreType.DMA((n_dev,)), pltpu.SemaphoreType.DMA((n_dev,))],
            compiler_params=pltpu.CompilerParams(collective_id=0, has_side_effects=True),
            name='route',
        )(topk_idx.reshape(n_rows, LANES), slot_expert)

        d_tiles = d_model // LANES
        wide = pltpu.VMEM((n_dev * stride * d_tiles, LANES), f32)
        tmp = pltpu.VMEM((LANES * d_tiles, LANES), f32)
        block = pltpu.VMEM((n_dev, stride // PACK, PACK, d_model), bf16)
        rows_vmem = pltpu.VMEM((n_tok, d_model), bf16)
        sem, sems = pltpu.SemaphoreType.DMA, pltpu.SemaphoreType.DMA((n_dev,))
        def run(cfg, meta, addr, tokens, w_up, w_down):
            part, cap = cfg['part'], cfg['cap']
            m_rows = n_dev * part
            sent = pltpu.SemaphoreType.DMA((len(cfg['first']), n_dev))
            given = pltpu.SemaphoreType.DMA((len(cfg['last']), n_dev))
            return pl.pallas_call(
                functools.partial(expert_kernel, cfg),
                out_shape=jax.ShapeDtypeStruct((n_dev, stride // PACK, PACK, d_model), bf16),
                in_specs=[smem, vmem, hbm, hbm, hbm],
                out_specs=hbm,
                scratch_shapes=[
                    rows_vmem,
                    pltpu.VMEM((n_dev, cap // PACK, PACK, d_model), bf16),
                    pltpu.VMEM((n_dev, (up_to(cap, STEP) + WIN) // PACK, PACK, d_model), bf16),
                    pltpu.VMEM((n_dev, n_slot * part, d_model), bf16),
                    pltpu.VMEM((2, d_model, d_ff), bf16),
                    pltpu.VMEM((2, d_ff, d_model), bf16),
                    pltpu.VMEM((m_rows, max(d_ff, n_tok)), bf16),
                    pltpu.VMEM((m_rows, d_model), bf16),
                    pltpu.VMEM((n_dev * WIN, d_model), bf16),
                    sent, sent, given, given,
                    pltpu.SemaphoreType.DMA((2, 2)),
                    sem,
                ],
                compiler_params=pltpu.CompilerParams(collective_id=1, has_side_effects=True, vmem_limit_bytes=big),
                name='experts',
            )(meta, addr, tokens, w_up, w_down)

        back = lax.switch(flag[0, 0], [functools.partial(run, p) for p in plans], meta, addr, tokens, w_up[0], w_down[0])

        return pl.pallas_call(
            functools.partial(unpack_kernel, caps[-1], len(caps)),
            out_shape=jax.ShapeDtypeStruct((n_tok, d_model), bf16),
            in_specs=[smem, smem, smem, hbm],
            out_specs=hbm,
            scratch_shapes=[block, wide, tmp, rows_vmem, sems, sem],
            compiler_params=pltpu.CompilerParams(vmem_limit_bytes=big),
            name='unpack',
        )(addr, flag, topk_w.reshape(n_rows, LANES), back)

    row_spec = P(('dp', 'ep'), None)
    weight_spec = P('ep', None, None, None)
    return jax.shard_map(group_layer, mesh=mesh, in_specs=(row_spec, row_spec, row_spec, weight_spec, weight_spec, P(None, None)), out_specs=row_spec, check_vma=False)
```

```python
import functools
import math

import jax
import jax.numpy as jnp
from jax import lax
from jax.experimental import pallas as pl
from jax.experimental.pallas import tpu as pltpu
from jax.sharding import PartitionSpec as P

MESH = pl.DeviceIdType.MESH
LANES = 128
SUB = 8
PACK = 16
USTRIDE = 32
WIN = 64
STEP = 32
CHUNK = 128
TIERS = (1.125, 1.156, 1.21875)


def up_to(x, m):
    return -(-x // m) * m


def group_barrier(n_dev, me):
    barrier = pltpu.get_barrier_semaphore()
    for k in range(1, n_dev):
        pl.semaphore_signal(barrier, inc=1, device_id={'ep': lax.rem(me + k, n_dev)}, device_id_type=MESH)
    pl.semaphore_wait(barrier, n_dev - 1)


def level_copies(loads, where, copies, bound):
    n_copy = len(where)
    f32, bf16 = jnp.float32, jnp.bfloat16
    share = [jnp.where(k < copies, loads / jnp.maximum(copies, 1.0), 0.0) for k in range(n_copy)]
    for _ in range(2):
        block = sum(lax.dot_general(share[k].astype(bf16), where[k], (((1,), (1,)), ((), ())), preferred_element_type=f32) for k in range(n_copy))
        there = [jnp.where(k < copies, jnp.dot(block.astype(bf16), where[k], preferred_element_type=f32), 0.0) for k in range(n_copy)]
        mean = sum(there) / jnp.maximum(copies, 1.0)
        share = [jnp.where(k < copies, jnp.clip(share[k] + 0.5 * (mean - there[k]), 0.0, bound), 0.0) for k in range(n_copy)]
    left, taken = loads, []
    for k in range(n_copy):
        after = jnp.maximum(copies - (k + 1), 0.0)
        want = jnp.floor(share[k] + 0.5)
        got = jnp.minimum(jnp.maximum(want, jnp.maximum(left - bound * after, 0.0)), jnp.minimum(left, bound))
        got = jnp.where(k < copies, got, 0.0)
        taken.append(got)
        left = left - got
    return taken


def route_kernel(n_dev, n_slot, stride, bound, low, high, caps, idx, table, addr, meta, flag, hsend, hall, hrow, tabcol, cums, ssem, rsem):
    me = lax.axis_index('ep')
    f32, bf16, i32 = jnp.float32, jnp.bfloat16, jnp.int32
    n_rows = idx.shape[0]
    n_units = n_dev * USTRIDE
    n_copy = 4
    nt = (((1,), (1,)), ((), ()))
    group_barrier(n_dev, me)
    sub_e = lax.broadcasted_iota(i32, (LANES, LANES), 0)
    lane_e = lax.broadcasted_iota(i32, (LANES, LANES), 1)
    ones = jnp.ones((SUB, LANES), bf16)

    @pl.loop(0, n_rows // SUB)
    def _(g):
        base = pl.multiple_of(g * SUB, SUB)
        rows = idx[pl.ds(base, SUB), :]
        parts = []
        for r in range(SUB):
            hot = (sub_e == rows[r:r + 1, :]).astype(bf16)
            parts.append(lax.dot_general(ones, hot, nt, preferred_element_type=f32)[0:1])
        hrow[pl.ds(base, SUB), :] = jnp.concatenate(parts, axis=0)

    hrows = hrow[...]
    hist = jnp.broadcast_to(jnp.sum(hrows, axis=0, keepdims=True), (SUB, LANES)).astype(i32)
    hsend[...] = hist
    hall[me] = hist
    sends = []
    for k in range(1, n_dev):
        copy = pltpu.make_async_remote_copy(src_ref=hsend, dst_ref=hall.at[me], send_sem=ssem.at[k], recv_sem=rsem.at[k], device_id={'ep': lax.rem(me + k, n_dev)}, device_id_type=MESH)
        copy.start()
        sends.append(copy)

    rr = lax.broadcasted_iota(i32, (n_rows, n_rows), 0)
    cc = lax.broadcasted_iota(i32, (n_rows, n_rows), 1)
    hrow[...] = jnp.dot((cc < rr).astype(bf16), hrows.astype(bf16), preferred_element_type=f32)
    tri = (sub_e < lane_e).astype(bf16)

    @pl.loop(0, n_rows // SUB)
    def _(g):
        base = pl.multiple_of(g * SUB, SUB)
        rows = idx[pl.ds(base, SUB), :]
        runs = hrow[pl.ds(base, SUB), :].astype(bf16)
        parts = []
        for r in range(SUB):
            hot = sub_e == rows[r:r + 1, :]
            hot_b = hot.astype(bf16)
            prefix = jnp.dot(hot_b, tri, preferred_element_type=f32)
            run = jnp.dot(runs, hot_b, preferred_element_type=f32)[r:r + 1]
            parts.append(jnp.sum(jnp.where(hot, prefix, 0.0), axis=0, keepdims=True) + run)
        addr[pl.ds(base, SUB), :] = jnp.concatenate(parts, axis=0).astype(i32)

    lane_u = lax.broadcasted_iota(i32, (1, n_units), 1)
    tabrow = jnp.full((1, n_units), -1, i32)
    tabcol[...] = jnp.full(tabcol.shape, -1, i32)
    for d in range(n_dev):
        for s in range(n_slot):
            u = d * USTRIDE + s
            tabrow = jnp.where(lane_u == u, table[d, s], tabrow)
            tabcol[u:u + 1, :] = jnp.full((1, LANES), table[d, s], i32)
    tcol = tabcol[...]
    unit_exp = (tcol == lax.broadcasted_iota(i32, (n_units, LANES), 1)).astype(bf16)
    same = jnp.concatenate([tcol] * (n_units // LANES), axis=1) == tabrow
    su = lax.broadcasted_iota(i32, (n_units, n_units), 0)
    lu = lax.broadcasted_iota(i32, (n_units, n_units), 1)
    valid = tabrow >= 0
    copy_rank = jnp.where(valid, jnp.sum(jnp.where(same & (su < lu), 1.0, 0.0), axis=0, keepdims=True).astype(i32), -1)
    before = ((su < lu) & (lax.shift_right_logical(su, 5) == lax.shift_right_logical(lu, 5))).astype(bf16)
    copies = jnp.dot(jnp.ones((SUB, n_units), bf16), unit_exp, preferred_element_type=f32)[0:1]
    dev8 = lax.broadcasted_iota(i32, (SUB, n_units), 0)
    dev_u = lax.shift_right_logical(lane_u, 5)
    where = [jnp.dot(((dev8 == dev_u) & (copy_rank == k)).astype(bf16), unit_exp, preferred_element_type=f32).astype(bf16) for k in range(n_copy)]

    for k in range(1, n_dev):
        src = lax.rem(me + n_dev - k, n_dev)
        pltpu.make_async_remote_copy(src_ref=hsend, dst_ref=hall.at[src], send_sem=ssem.at[k], recv_sem=rsem.at[k], device_id={'ep': src}, device_id_type=MESH).wait_recv()
    every = jnp.concatenate([hall[p, 0:1, :] for p in range(n_dev)], axis=0).astype(f32)
    taken = level_copies(every, where, copies, float(bound))
    loads = jnp.zeros((n_dev, n_units), f32)
    cum = jnp.zeros((n_dev, LANES), f32)
    for k in range(n_copy):
        per_unit = lax.dot_general(taken[k].astype(bf16), unit_exp, nt, preferred_element_type=f32)
        loads = jnp.where(copy_rank == k, per_unit, loads)
        cums[k * n_dev:(k + 1) * n_dev, :] = cum
        cum = cum + taken[k]
    starts = jnp.dot(loads.astype(bf16), before, preferred_element_type=f32)
    meta[0:n_dev, :] = loads.astype(i32)
    meta[n_dev:2 * n_dev, :] = starts.astype(i32)

    block = lax.rem(dev_u + n_dev - me, n_dev)
    first = meta[pl.ds(n_dev + me, 1), :] + block * stride
    row8 = lax.broadcasted_iota(i32, (2 * n_copy, n_units), 0)
    half = jnp.where(row8 < n_copy, lax.shift_right_logical(first, 6), first & 63)
    half = jnp.where(copy_rank == (row8 & (n_copy - 1)), half, 0)
    place = jnp.dot(half.astype(bf16), unit_exp, preferred_element_type=f32).astype(i32)
    own = [cums[pl.ds(k * n_dev + me, 1), :].astype(i32) for k in range(n_copy)]
    offs = [place[k:k + 1] * 64 + place[n_copy + k:n_copy + k + 1] - own[k] + 256 for k in range(n_copy)]
    bar = [jnp.where(copies > k, own[k], 255) for k in range(1, n_copy)]
    rows = [lax.shift_right_logical(o, 6) for o in offs] + [o & 63 for o in offs] + bar + [jnp.zeros((1, LANES), i32)] * 5
    lookup = jnp.concatenate(rows, axis=0).astype(f32).astype(bf16)

    @pl.loop(0, n_rows // SUB)
    def _(g):
        base = pl.multiple_of(g * SUB, SUB)
        ids = idx[pl.ds(base, SUB), :]
        ranks = addr[pl.ds(base, SUB), :]
        parts = []
        for r in range(SUB):
            rank = ranks[r:r + 1, :]
            hot_b = (sub_e == ids[r:r + 1, :]).astype(bf16)
            got = jnp.dot(lookup, hot_b, preferred_element_type=f32).astype(i32)
            pos = got[0:1] * 64 + got[n_copy:n_copy + 1]
            for k in range(1, n_copy):
                pos = jnp.where(rank >= got[2 * n_copy + k - 1:2 * n_copy + k], got[k:k + 1] * 64 + got[n_copy + k:n_copy + k + 1], pos)
            pos = pos + rank - 256
            parts.append(pos + lax.shift_right_logical(pos, 3) * 40)
        addr[pl.ds(base, SUB), :] = jnp.concatenate(parts, axis=0)

    slot_id = lane_u & (USTRIDE - 1)
    lo_row = jnp.zeros((1, n_units), f32)
    hi_row = jnp.zeros((1, n_units), f32)
    for s in range(n_slot):
        lo_row = jnp.where(slot_id == s, float(low[s]), lo_row)
        hi_row = jnp.where(slot_id == s, float(high[s]), hi_row)
    ends = loads + starts
    bad = jnp.max(jnp.where(valid & ((ends < lo_row) | (ends > hi_row)), 1.0, 0.0))
    top = jnp.max(jnp.where(valid, ends, 0.0))
    tier = jnp.where(bad > 0.0, float(len(caps)), sum(jnp.where(top > float(c), 1.0, 0.0) for c in caps))
    flag[0, 0] = tier.astype(i32)
    for copy in sends:
        copy.wait_send()


def unpack_kernel(cap, slow, addr, flag, gate, back_hbm, out_hbm, back, wide, tmp, out, bsem, osem):
    n_rows, n_col = addr.shape
    n_dev, stride = back.shape[0], back.shape[1] * PACK
    d_tiles = out.shape[1] // LANES
    step = SUB * d_tiles

    def load(k, lo, hi):
        rows = pl.ds(lo // PACK, (hi - lo) // PACK)
        return pltpu.make_async_copy(back_hbm.at[k, rows], back.at[k, rows], bsem.at[k])

    def widen(k, b):
        base = (k * (stride // PACK) + b) * (2 * step)
        for j in range(d_tiles):
            x = back[k, b, :, j * LANES:(j + 1) * LANES].astype(jnp.float32)
            wide[pl.ds(base + j * SUB, SUB), :] = x[:SUB]
            wide[pl.ds(base + step + j * SUB, SUB), :] = x[SUB:]

    @pl.loop(0, n_dev)
    def _(k):
        load(k, 0, cap).start()

    @pl.loop(0, n_dev)
    def _(k):
        load(k, 0, cap).wait()

        @pl.loop(0, cap // PACK, unroll=4)
        def _(b):
            widen(k, b)

    @pl.when(flag[0, 0] == slow)
    def _():
        @pl.loop(0, n_dev)
        def _(k):
            rest = load(k, cap, stride)
            rest.start()
            rest.wait()

            @pl.loop(cap // PACK, stride // PACK)
            def _(b):
                widen(k, b)

    def give(g):
        rows = pl.ds(pl.multiple_of(g * n_col, n_col), n_col)
        return pltpu.make_async_copy(out.at[rows], out_hbm.at[rows], osem)

    @pl.loop(0, n_rows)
    def _(r):
        for c in range(n_col // PACK):
            at = c * 2 * step
            for i in range(PACK):
                a = addr[r, c * PACK + i]
                g = gate[r, c * PACK + i]
                tmp[pl.ds(at + (i // SUB) * step + i % SUB, d_tiles, stride=SUB), :] = wide[pl.ds(a, d_tiles, stride=SUB), :] * g
            rows = pl.ds(pl.multiple_of(r * n_col + c * PACK, PACK), PACK)
            for j in range(d_tiles):
                top = tmp[at + j * SUB:at + (j + 1) * SUB, :]
                bot = tmp[at + step + j * SUB:at + step + (j + 1) * SUB, :]
                out[rows, j * LANES:(j + 1) * LANES] = jnp.concatenate([top, bot], axis=0).astype(jnp.bfloat16)
        give(r).start()

    @pl.loop(0, n_rows)
    def _(r):
        give(r).wait()


def gelu(x):
    return x * (0.5 * (1.0 + jnp.tanh(0.7978845608028654 * (x + 0.044715 * (x * x * x)))))


def expert_kernel(cfg, meta, addr, tok_hbm, up_hbm, down_hbm, back, tok, recv, xbuf, ybuf, up, down, mix, xs, win, dsend, drecv, rsend, rrecv, wsem, tsem):
    n_dev, n_slot, part, stride = cfg['n_dev'], cfg['n_slot'], cfg['part'], cfg['stride']
    m_rows = n_dev * part
    n_tok, d_model, d_ff = tok.shape[0], up_hbm.shape[1], up_hbm.shape[2]
    first, last, disp, ret, ret_lo = cfg['first'], cfg['last'], cfg['disp'], cfg['ret'], cfg['ret_lo']
    n_step = -(-disp[-1] // STEP)
    f32, bf16, i32 = jnp.float32, jnp.bfloat16, jnp.int32
    me = lax.axis_index('ep')

    def fetch(s, b):
        return (pltpu.make_async_copy(up_hbm.at[s], up.at[b], wsem.at[0, b]), pltpu.make_async_copy(down_hbm.at[s], down.at[b], wsem.at[1, b]))

    load_tok = pltpu.make_async_copy(tok_hbm, tok, tsem)
    load_tok.start()
    group_barrier(n_dev, me)
    tail = n_step * (STEP // PACK)

    @pl.loop(0, n_dev)
    def _(k):
        xbuf[k, tail:] = jnp.zeros((xbuf.shape[1] - tail, PACK, d_model), bf16)

    def dispatch(j, k, peer, lo, num):
        return pltpu.make_async_remote_copy(src_ref=xbuf.at[k, pl.ds(lo, num)], dst_ref=recv.at[k, pl.ds(lo, num)], send_sem=dsend.at[j, k], recv_sem=drecv.at[j, k], device_id={'ep': peer}, device_id_type=MESH)

    def dispatched(j, k, peer):
        return dispatch(j, k, peer, disp[j] // PACK, (disp[j + 1] - disp[j]) // PACK)

    order = sorted(range(1, n_dev), key=lambda k: (abs(k - n_dev // 2), k))
    load_tok.wait()

    @pl.loop(0, n_step)
    def _(u):
        row = lax.broadcasted_iota(i32, (n_dev * STEP, LANES), 0)
        pos = lax.shift_right_logical(row, 5) * stride + (row & (STEP - 1)) + u * STEP
        want = pos + lax.shift_right_logical(pos, 3) * 40
        for q in range(n_tok // LANES):
            mix[:n_dev * STEP, q * LANES:(q + 1) * LANES] = (want == addr[q:q + 1, :]).astype(bf16)
        rows = jnp.dot(mix[:n_dev * STEP, :n_tok], tok[...], preferred_element_type=f32).astype(bf16)
        for k in range(n_dev):
            for h in range(STEP // PACK):
                at = k * STEP + h * PACK
                xbuf[k, u * (STEP // PACK) + h] = rows[at:at + PACK]
        for lo, hi, j in cfg['pieces']:
            @pl.when(u == -(-hi // STEP) - 1)
            def _():
                for k in order:
                    dispatch(j, k, lax.rem(me + k, n_dev), lo // PACK, (hi - lo) // PACK).start()

        @pl.when(u == 0)
        def _():
            for s in range(2):
                for copy in fetch(s, s):
                    copy.start()

    def ffn(s, b):
        unit = me * USTRIDE + s
        lane = lax.broadcasted_iota(i32, (1, n_dev * WIN), 1)
        which = lax.shift_right_logical(lane, 6)
        off = jnp.zeros((1, n_dev * WIN), i32)
        num = jnp.zeros((1, n_dev * WIN), i32)
        for k in range(n_dev):
            src = lax.rem(me + n_dev - k, n_dev)
            load, start = meta[src, unit], meta[n_dev + src, unit]
            blk = lax.shift_right_logical(start, 4)
            base = blk * PACK
            for q in range(WIN // PACK):
                win[k * WIN + q * PACK:k * WIN + (q + 1) * PACK, :] = xbuf[k, blk + q]
            off = jnp.where(which == k, base - start, off)
            num = jnp.where(which == k, load, num)
        nth = (lane & (WIN - 1)) + off
        target = jnp.where((nth >= 0) & (nth < num), nth + which * part, -1)
        pick = (lax.broadcasted_iota(i32, (m_rows, n_dev * WIN), 0) == target).astype(bf16)
        xs[...] = jnp.dot(pick, win[...], preferred_element_type=f32).astype(bf16)
        tile = 512
        for t in range(d_ff // tile):
            pre = jnp.dot(xs[...], up[b, :, t * tile:(t + 1) * tile], preferred_element_type=f32)
            mix[:, t * tile:(t + 1) * tile] = gelu(pre).astype(bf16)
        tile = 256
        for t in range(d_model // tile):
            o = jnp.dot(mix[:, :d_ff], down[b, :, t * tile:(t + 1) * tile], preferred_element_type=f32).astype(bf16)
            for k in range(n_dev):
                ybuf[k, pl.ds(pl.multiple_of(s * part, PACK), part), t * tile:(t + 1) * tile] = o[k * part:(k + 1) * part]

    def give_back(j, k):
        rows = pl.ds(ret[j] // PACK, (ret[j + 1] - ret[j]) // PACK)
        peer = lax.rem(me + n_dev - k, n_dev)
        return pltpu.make_async_remote_copy(src_ref=recv.at[k, rows], dst_ref=back.at[k, rows], send_sem=rsend.at[j, k], recv_sem=rrecv.at[j, k], device_id={'ep': peer}, device_id_type=MESH)

    def give_own(j):
        rows = pl.ds(ret[j] // PACK, (ret[j + 1] - ret[j]) // PACK)
        return pltpu.make_async_copy(recv.at[0, rows], back.at[0, rows], rrecv.at[j, 0])

    def combine(j):
        n_rows = ret[j + 1] - ret[j]
        n_win = last[j] + 1 - ret_lo[j]
        width = n_win * part

        @pl.loop(0, n_dev)
        def _(i):
            k = lax.rem(n_dev // 2 + 3 * i, n_dev)
            src = lax.rem(me + n_dev - k, n_dev)
            lane = lax.broadcasted_iota(i32, (1, width), 1)
            target = jnp.full((1, width), -1, i32)
            for w in range(n_win):
                unit = me * USTRIDE + ret_lo[j] + w
                load, start = meta[src, unit], meta[n_dev + src, unit]
                nth = lane - w * part
                target = jnp.where((nth >= 0) & (nth < load), nth + start, target)
            pick = (lax.broadcasted_iota(i32, (n_rows, width), 0) + ret[j] == target).astype(bf16)
            rows = ybuf[k, ret_lo[j] * part:(last[j] + 1) * part, :]
            mixed = jnp.dot(pick, rows, preferred_element_type=f32).astype(bf16)
            recv[k, ret[j] // PACK:ret[j + 1] // PACK] = mixed.reshape(n_rows // PACK, PACK, d_model)

            @pl.when(k == 0)
            def _():
                give_own(j).start()

            @pl.when(k != 0)
            def _():
                give_back(j, k).start()

    @pl.loop(0, n_slot)
    def _(s):
        for j in range(len(first)):
            @pl.when(s == first[j])
            def _():
                for k in range(1, n_dev):
                    dispatched(j, k, lax.rem(me + n_dev - k, n_dev)).wait_recv()
                    dispatched(j, k, lax.rem(me + k, n_dev)).wait_send()

                @pl.loop(1, n_dev)
                def _(k):
                    @pl.loop(disp[j] // PACK, disp[j + 1] // PACK)
                    def _(b):
                        xbuf[k, b] = recv[k, b]

        b = lax.rem(s, 2)
        for copy in fetch(s, b):
            copy.wait()
        ffn(s, b)

        @pl.when(s + 2 < n_slot)
        def _():
            for copy in fetch(s + 2, b):
                copy.start()

        for j in range(len(last)):
            @pl.when(s == last[j])
            def _():
                combine(j)

    for k in range(1, n_dev):
        for j in range(len(last)):
            give_back(j, k).wait_send()
            give_back(j, k).wait_recv()
    for j in range(len(last)):
        give_own(j).wait()


def plan(n_dev, n_slot, n_pairs, bound, stride, z, cap, returns):
    mean = n_pairs / (n_dev * n_slot)
    spread = 9.3 * mean / 30.1
    hi = [bound * (s + 1) for s in range(n_slot)]
    lo = [0] * n_slot
    if z is not None:
        hi = [min(hi[s], math.ceil(mean * (s + 1) + z * spread * math.sqrt(s + 1)), cap) for s in range(n_slot)]
        lo = [max(0, math.floor(mean * (s + 1) - z * spread * math.sqrt(s + 1))) for s in range(n_slot - 1)] + [0]
    disp = [0, cap] if z is None else list(range(0, cap - CHUNK, CHUNK)) + [cap]
    pieces = [(0, STEP, 0), (STEP, 2 * STEP, 0), (2 * STEP, disp[1], 0)]
    pieces += [(disp[j], disp[j + 1], j) for j in range(1, len(disp) - 1)]
    ret = [0] + [lo[s] // PACK * PACK for s in returns[:-1]] + [cap]
    ret_lo = [min(s for s in range(n_slot) if hi[s] > ret[j]) for j in range(len(returns))]
    first = [min((s for s in range(n_slot) if hi[s] > d), default=n_slot - 1) for d in disp[:-1]]
    return dict(n_dev=n_dev, n_slot=n_slot, cap=cap, stride=stride, pieces=pieces, lo=lo, hi=hi, first=first, last=list(returns), disp=disp, ret=ret, ret_lo=ret_lo, part=up_to(bound, PACK))


def solution(mesh):
    n_dev = mesh.shape['ep']

    def group_layer(tokens, topk_idx, topk_w, w_up, w_down, slot_expert):
        n_tok, d_model = tokens.shape
        n_slot = slot_expert.shape[1]
        d_ff = w_up.shape[3]
        n_pairs = n_tok * topk_idx.shape[1]
        base_load = n_pairs // (n_dev * n_slot)
        bound = base_load + base_load // 2 + 1
        mean = n_pairs // n_dev
        stride = up_to(n_slot * bound, PACK)
        caps = [min(stride, up_to(math.ceil(mean * f), PACK)) for f in TIERS]
        cuts = [n_slot * c // 17 - 1 for c in (9, 12, 15, 17)]
        plans = [plan(n_dev, n_slot, n_pairs, bound, stride, 4.0, c, cuts) for c in caps]
        plans.append(plan(n_dev, n_slot, n_pairs, bound, stride, None, stride, [n_slot - 1]))
        wide_bounds = plan(n_dev, n_slot, n_pairs, bound, stride, 4.0, stride, cuts)
        n_rows = n_pairs // LANES
        n_units = n_dev * USTRIDE
        f32, bf16, i32 = jnp.float32, jnp.bfloat16, jnp.int32
        vmem = pl.BlockSpec(memory_space=pltpu.VMEM)
        smem = pl.BlockSpec(memory_space=pltpu.SMEM)
        hbm = pl.BlockSpec(memory_space=pl.ANY)
        big = 63 * 1024 * 1024

        addr, meta, flag = pl.pallas_call(
            functools.partial(route_kernel, n_dev, n_slot, stride, bound, wide_bounds['lo'], wide_bounds['hi'], caps),
            out_shape=[jax.ShapeDtypeStruct((n_rows, LANES), i32), jax.ShapeDtypeStruct((2 * n_dev, n_units), i32), jax.ShapeDtypeStruct((1, 1), i32)],
            in_specs=[vmem, smem],
            out_specs=[vmem, vmem, smem],
            scratch_shapes=[pltpu.VMEM((SUB, LANES), i32), pltpu.VMEM((n_dev, SUB, LANES), i32), pltpu.VMEM((n_rows, LANES), f32), pltpu.VMEM((n_units, LANES), i32), pltpu.VMEM((4 * n_dev, LANES), f32), pltpu.SemaphoreType.DMA((n_dev,)), pltpu.SemaphoreType.DMA((n_dev,))],
            compiler_params=pltpu.CompilerParams(collective_id=0, has_side_effects=True),
            name='route',
        )(topk_idx.reshape(n_rows, LANES), slot_expert)

        d_tiles = d_model // LANES
        wide = pltpu.VMEM((n_dev * stride * d_tiles, LANES), f32)
        tmp = pltpu.VMEM((LANES * d_tiles, LANES), f32)
        block = pltpu.VMEM((n_dev, stride // PACK, PACK, d_model), bf16)
        rows_vmem = pltpu.VMEM((n_tok, d_model), bf16)
        sem, sems = pltpu.SemaphoreType.DMA, pltpu.SemaphoreType.DMA((n_dev,))
        def run(cfg, meta, addr, tokens, w_up, w_down):
            part, cap = cfg['part'], cfg['cap']
            m_rows = n_dev * part
            sent = pltpu.SemaphoreType.DMA((len(cfg['first']), n_dev))
            given = pltpu.SemaphoreType.DMA((len(cfg['last']), n_dev))
            return pl.pallas_call(
                functools.partial(expert_kernel, cfg),
                out_shape=jax.ShapeDtypeStruct((n_dev, stride // PACK, PACK, d_model), bf16),
                in_specs=[smem, vmem, hbm, hbm, hbm],
                out_specs=hbm,
                scratch_shapes=[
                    rows_vmem,
                    pltpu.VMEM((n_dev, cap // PACK, PACK, d_model), bf16),
                    pltpu.VMEM((n_dev, (up_to(cap, STEP) + WIN) // PACK, PACK, d_model), bf16),
                    pltpu.VMEM((n_dev, n_slot * part, d_model), bf16),
                    pltpu.VMEM((2, d_model, d_ff), bf16),
                    pltpu.VMEM((2, d_ff, d_model), bf16),
                    pltpu.VMEM((m_rows, max(d_ff, n_tok)), bf16),
                    pltpu.VMEM((m_rows, d_model), bf16),
                    pltpu.VMEM((n_dev * WIN, d_model), bf16),
                    sent, sent, given, given,
                    pltpu.SemaphoreType.DMA((2, 2)),
                    sem,
                ],
                compiler_params=pltpu.CompilerParams(collective_id=1, has_side_effects=True, vmem_limit_bytes=big),
                name='experts',
            )(meta, addr, tokens, w_up, w_down)

        back = lax.switch(flag[0, 0], [functools.partial(run, p) for p in plans], meta, addr, tokens, w_up[0], w_down[0])

        return pl.pallas_call(
            functools.partial(unpack_kernel, caps[-1], len(caps)),
            out_shape=jax.ShapeDtypeStruct((n_tok, d_model), bf16),
            in_specs=[smem, smem, smem, hbm],
            out_specs=hbm,
            scratch_shapes=[block, wide, tmp, rows_vmem, sems, sem],
            compiler_params=pltpu.CompilerParams(vmem_limit_bytes=big),
            name='unpack',
        )(addr, flag, topk_w.reshape(n_rows, LANES), back)

    row_spec = P(('dp', 'ep'), None)
    weight_spec = P('ep', None, None, None)
    return jax.shard_map(group_layer, mesh=mesh, in_specs=(row_spec, row_spec, row_spec, weight_spec, weight_spec, P(None, None)), out_specs=row_spec, check_vma=False)
```

```python
import functools
import math

import jax
import jax.numpy as jnp
from jax import lax
from jax.experimental import pallas as pl
from jax.experimental.pallas import tpu as pltpu
from jax.sharding import PartitionSpec as P

MESH = pl.DeviceIdType.MESH
LANES = 128
SUB = 8
PACK = 16
USTRIDE = 32
WIN = 64
STEP = 32
CHUNK = 128
TIERS = (1.125, 1.156, 1.21875)


def up_to(x, m):
    return -(-x // m) * m


def group_barrier(n_dev, me):
    barrier = pltpu.get_barrier_semaphore()
    for k in range(1, n_dev):
        pl.semaphore_signal(barrier, inc=1, device_id={'ep': lax.rem(me + k, n_dev)}, device_id_type=MESH)
    pl.semaphore_wait(barrier, n_dev - 1)


def level_copies(loads, where, copies, bound):
    n_copy = len(where)
    f32, bf16 = jnp.float32, jnp.bfloat16
    share = [jnp.where(k < copies, loads / jnp.maximum(copies, 1.0), 0.0) for k in range(n_copy)]
    for _ in range(2):
        block = sum(lax.dot_general(share[k].astype(bf16), where[k], (((1,), (1,)), ((), ())), preferred_element_type=f32) for k in range(n_copy))
        there = [jnp.where(k < copies, jnp.dot(block.astype(bf16), where[k], preferred_element_type=f32), 0.0) for k in range(n_copy)]
        mean = sum(there) / jnp.maximum(copies, 1.0)
        share = [jnp.where(k < copies, jnp.clip(share[k] + 0.5 * (mean - there[k]), 0.0, bound), 0.0) for k in range(n_copy)]
    left, taken = loads, []
    for k in range(n_copy):
        after = jnp.maximum(copies - (k + 1), 0.0)
        want = jnp.floor(share[k] + 0.5)
        got = jnp.minimum(jnp.maximum(want, jnp.maximum(left - bound * after, 0.0)), jnp.minimum(left, bound))
        got = jnp.where(k < copies, got, 0.0)
        taken.append(got)
        left = left - got
    return taken


def route_kernel(n_dev, n_slot, stride, bound, low, high, caps, idx, table, addr, meta, flag, hsend, hall, hrow, tabcol, cums, ssem, rsem):
    me = lax.axis_index('ep')
    f32, bf16, i32 = jnp.float32, jnp.bfloat16, jnp.int32
    n_rows = idx.shape[0]
    n_units = n_dev * USTRIDE
    n_copy = 4
    nt = (((1,), (1,)), ((), ()))
    group_barrier(n_dev, me)
    sub_e = lax.broadcasted_iota(i32, (LANES, LANES), 0)
    lane_e = lax.broadcasted_iota(i32, (LANES, LANES), 1)
    ones = jnp.ones((SUB, LANES), bf16)

    @pl.loop(0, n_rows // SUB)
    def _(g):
        base = pl.multiple_of(g * SUB, SUB)
        rows = idx[pl.ds(base, SUB), :]
        parts = []
        for r in range(SUB):
            hot = (sub_e == rows[r:r + 1, :]).astype(bf16)
            parts.append(lax.dot_general(ones, hot, nt, preferred_element_type=f32)[0:1])
        hrow[pl.ds(base, SUB), :] = jnp.concatenate(parts, axis=0)

    hrows = hrow[...]
    hist = jnp.broadcast_to(jnp.sum(hrows, axis=0, keepdims=True), (SUB, LANES)).astype(i32)
    hsend[...] = hist
    hall[me] = hist
    sends = []
    for k in range(1, n_dev):
        copy = pltpu.make_async_remote_copy(src_ref=hsend, dst_ref=hall.at[me], send_sem=ssem.at[k], recv_sem=rsem.at[k], device_id={'ep': lax.rem(me + k, n_dev)}, device_id_type=MESH)
        copy.start()
        sends.append(copy)

    rr = lax.broadcasted_iota(i32, (n_rows, n_rows), 0)
    cc = lax.broadcasted_iota(i32, (n_rows, n_rows), 1)
    hrow[...] = jnp.dot((cc < rr).astype(bf16), hrows.astype(bf16), preferred_element_type=f32)
    tri = (sub_e < lane_e).astype(bf16)

    @pl.loop(0, n_rows // SUB)
    def _(g):
        base = pl.multiple_of(g * SUB, SUB)
        rows = idx[pl.ds(base, SUB), :]
        runs = hrow[pl.ds(base, SUB), :].astype(bf16)
        parts = []
        for r in range(SUB):
            hot = sub_e == rows[r:r + 1, :]
            hot_b = hot.astype(bf16)
            prefix = jnp.dot(hot_b, tri, preferred_element_type=f32)
            run = jnp.dot(runs, hot_b, preferred_element_type=f32)[r:r + 1]
            parts.append(jnp.sum(jnp.where(hot, prefix, 0.0), axis=0, keepdims=True) + run)
        addr[pl.ds(base, SUB), :] = jnp.concatenate(parts, axis=0).astype(i32)

    lane_u = lax.broadcasted_iota(i32, (1, n_units), 1)
    tabrow = jnp.full((1, n_units), -1, i32)
    tabcol[...] = jnp.full(tabcol.shape, -1, i32)
    for d in range(n_dev):
        for s in range(n_slot):
            u = d * USTRIDE + s
            tabrow = jnp.where(lane_u == u, table[d, s], tabrow)
            tabcol[u:u + 1, :] = jnp.full((1, LANES), table[d, s], i32)
    tcol = tabcol[...]
    unit_exp = (tcol == lax.broadcasted_iota(i32, (n_units, LANES), 1)).astype(bf16)
    same = jnp.concatenate([tcol] * (n_units // LANES), axis=1) == tabrow
    su = lax.broadcasted_iota(i32, (n_units, n_units), 0)
    lu = lax.broadcasted_iota(i32, (n_units, n_units), 1)
    valid = tabrow >= 0
    copy_rank = jnp.where(valid, jnp.sum(jnp.where(same & (su < lu), 1.0, 0.0), axis=0, keepdims=True).astype(i32), -1)
    before = ((su < lu) & (lax.shift_right_logical(su, 5) == lax.shift_right_logical(lu, 5))).astype(bf16)
    copies = jnp.dot(jnp.ones((SUB, n_units), bf16), unit_exp, preferred_element_type=f32)[0:1]
    dev8 = lax.broadcasted_iota(i32, (SUB, n_units), 0)
    dev_u = lax.shift_right_logical(lane_u, 5)
    where = [jnp.dot(((dev8 == dev_u) & (copy_rank == k)).astype(bf16), unit_exp, preferred_element_type=f32).astype(bf16) for k in range(n_copy)]

    for k in range(1, n_dev):
        src = lax.rem(me + n_dev - k, n_dev)
        pltpu.make_async_remote_copy(src_ref=hsend, dst_ref=hall.at[src], send_sem=ssem.at[k], recv_sem=rsem.at[k], device_id={'ep': src}, device_id_type=MESH).wait_recv()
    every = jnp.concatenate([hall[p, 0:1, :] for p in range(n_dev)], axis=0).astype(f32)
    taken = level_copies(every, where, copies, float(bound))
    loads = jnp.zeros((n_dev, n_units), f32)
    cum = jnp.zeros((n_dev, LANES), f32)
    for k in range(n_copy):
        per_unit = lax.dot_general(taken[k].astype(bf16), unit_exp, nt, preferred_element_type=f32)
        loads = jnp.where(copy_rank == k, per_unit, loads)
        cums[k * n_dev:(k + 1) * n_dev, :] = cum
        cum = cum + taken[k]
    starts = jnp.dot(loads.astype(bf16), before, preferred_element_type=f32)
    meta[0:n_dev, :] = loads.astype(i32)
    meta[n_dev:2 * n_dev, :] = starts.astype(i32)

    block = lax.rem(dev_u + n_dev - me, n_dev)
    first = meta[pl.ds(n_dev + me, 1), :] + block * stride
    row8 = lax.broadcasted_iota(i32, (2 * n_copy, n_units), 0)
    half = jnp.where(row8 < n_copy, lax.shift_right_logical(first, 6), first & 63)
    half = jnp.where(copy_rank == (row8 & (n_copy - 1)), half, 0)
    place = jnp.dot(half.astype(bf16), unit_exp, preferred_element_type=f32).astype(i32)
    own = [cums[pl.ds(k * n_dev + me, 1), :].astype(i32) for k in range(n_copy)]
    offs = [place[k:k + 1] * 64 + place[n_copy + k:n_copy + k + 1] - own[k] + 256 for k in range(n_copy)]
    bar = [jnp.where(copies > k, own[k], 255) for k in range(1, n_copy)]
    rows = [lax.shift_right_logical(o, 6) for o in offs] + [o & 63 for o in offs] + bar + [jnp.zeros((1, LANES), i32)] * 5
    lookup = jnp.concatenate(rows, axis=0).astype(f32).astype(bf16)

    @pl.loop(0, n_rows // SUB)
    def _(g):
        base = pl.multiple_of(g * SUB, SUB)
        ids = idx[pl.ds(base, SUB), :]
        ranks = addr[pl.ds(base, SUB), :]
        parts = []
        for r in range(SUB):
            rank = ranks[r:r + 1, :]
            hot_b = (sub_e == ids[r:r + 1, :]).astype(bf16)
            got = jnp.dot(lookup, hot_b, preferred_element_type=f32).astype(i32)
            pos = got[0:1] * 64 + got[n_copy:n_copy + 1]
            for k in range(1, n_copy):
                pos = jnp.where(rank >= got[2 * n_copy + k - 1:2 * n_copy + k], got[k:k + 1] * 64 + got[n_copy + k:n_copy + k + 1], pos)
            pos = pos + rank - 256
            parts.append(pos + lax.shift_right_logical(pos, 3) * 40)
        addr[pl.ds(base, SUB), :] = jnp.concatenate(parts, axis=0)

    slot_id = lane_u & (USTRIDE - 1)
    lo_row = jnp.zeros((1, n_units), f32)
    hi_row = jnp.zeros((1, n_units), f32)
    for s in range(n_slot):
        lo_row = jnp.where(slot_id == s, float(low[s]), lo_row)
        hi_row = jnp.where(slot_id == s, float(high[s]), hi_row)
    ends = loads + starts
    bad = jnp.max(jnp.where(valid & ((ends < lo_row) | (ends > hi_row)), 1.0, 0.0))
    top = jnp.max(jnp.where(valid, ends, 0.0))
    tier = jnp.where(bad > 0.0, float(len(caps)), sum(jnp.where(top > float(c), 1.0, 0.0) for c in caps))
    flag[0, 0] = tier.astype(i32)
    for copy in sends:
        copy.wait_send()


def unpack_kernel(cap, slow, addr, flag, gate, back_hbm, out_hbm, back, wide, tmp, out, bsem, osem):
    n_rows, n_col = addr.shape
    n_dev, stride = back.shape[0], back.shape[1] * PACK
    d_tiles = out.shape[1] // LANES
    step = SUB * d_tiles

    def load(k, lo, hi):
        rows = pl.ds(lo // PACK, (hi - lo) // PACK)
        return pltpu.make_async_copy(back_hbm.at[k, rows], back.at[k, rows], bsem.at[k])

    def widen(k, b):
        base = (k * (stride // PACK) + b) * (2 * step)
        for j in range(d_tiles):
            x = back[k, b, :, j * LANES:(j + 1) * LANES].astype(jnp.float32)
            wide[pl.ds(base + j * SUB, SUB), :] = x[:SUB]
            wide[pl.ds(base + step + j * SUB, SUB), :] = x[SUB:]

    @pl.loop(0, n_dev)
    def _(k):
        load(k, 0, cap).start()

    @pl.loop(0, n_dev)
    def _(k):
        load(k, 0, cap).wait()

        @pl.loop(0, cap // PACK, unroll=4)
        def _(b):
            widen(k, b)

    @pl.when(flag[0, 0] == slow)
    def _():
        @pl.loop(0, n_dev)
        def _(k):
            rest = load(k, cap, stride)
            rest.start()
            rest.wait()

            @pl.loop(cap // PACK, stride // PACK)
            def _(b):
                widen(k, b)

    def give(g):
        rows = pl.ds(pl.multiple_of(g * n_col, n_col), n_col)
        return pltpu.make_async_copy(out.at[rows], out_hbm.at[rows], osem)

    @pl.loop(0, n_rows)
    def _(r):
        for c in range(n_col // PACK):
            at = c * 2 * step
            for i in range(PACK):
                a = addr[r, c * PACK + i]
                g = gate[r, c * PACK + i]
                tmp[pl.ds(at + (i // SUB) * step + i % SUB, d_tiles, stride=SUB), :] = wide[pl.ds(a, d_tiles, stride=SUB), :] * g
            rows = pl.ds(pl.multiple_of(r * n_col + c * PACK, PACK), PACK)
            for j in range(d_tiles):
                top = tmp[at + j * SUB:at + (j + 1) * SUB, :]
                bot = tmp[at + step + j * SUB:at + step + (j + 1) * SUB, :]
                out[rows, j * LANES:(j + 1) * LANES] = jnp.concatenate([top, bot], axis=0).astype(jnp.bfloat16)
        give(r).start()

    @pl.loop(0, n_rows)
    def _(r):
        give(r).wait()


def gelu(x):
    return x * (0.5 * (1.0 + jnp.tanh(0.7978845608028654 * (x + 0.044715 * (x * x * x)))))


def expert_kernel(cfg, meta, addr, tok_hbm, up_hbm, down_hbm, back, tok, recv, xbuf, ybuf, up, down, mix, xs, win, dsend, drecv, rsend, rrecv, wsem, tsem):
    n_dev, n_slot, part, stride = cfg['n_dev'], cfg['n_slot'], cfg['part'], cfg['stride']
    m_rows = n_dev * part
    n_tok, d_model, d_ff = tok.shape[0], up_hbm.shape[1], up_hbm.shape[2]
    first, last, disp, ret, ret_lo = cfg['first'], cfg['last'], cfg['disp'], cfg['ret'], cfg['ret_lo']
    n_step = -(-disp[-1] // STEP)
    f32, bf16, i32 = jnp.float32, jnp.bfloat16, jnp.int32
    me = lax.axis_index('ep')

    def fetch(s, b):
        return (pltpu.make_async_copy(up_hbm.at[s], up.at[b], wsem.at[0, b]), pltpu.make_async_copy(down_hbm.at[s], down.at[b], wsem.at[1, b]))

    load_tok = pltpu.make_async_copy(tok_hbm, tok, tsem)
    load_tok.start()
    group_barrier(n_dev, me)
    tail = n_step * (STEP // PACK)

    @pl.loop(0, n_dev)
    def _(k):
        xbuf[k, tail:] = jnp.zeros((xbuf.shape[1] - tail, PACK, d_model), bf16)

    def dispatch(j, k, peer, lo, num):
        return pltpu.make_async_remote_copy(src_ref=xbuf.at[k, pl.ds(lo, num)], dst_ref=recv.at[k, pl.ds(lo, num)], send_sem=dsend.at[j, k], recv_sem=drecv.at[j, k], device_id={'ep': peer}, device_id_type=MESH)

    def dispatched(j, k, peer):
        return dispatch(j, k, peer, disp[j] // PACK, (disp[j + 1] - disp[j]) // PACK)

    order = sorted(range(1, n_dev), key=lambda k: (abs(k - n_dev // 2), k))
    load_tok.wait()

    @pl.loop(0, n_step)
    def _(u):
        row = lax.broadcasted_iota(i32, (n_dev * STEP, LANES), 0)
        pos = lax.shift_right_logical(row, 5) * stride + (row & (STEP - 1)) + u * STEP
        want = pos + lax.shift_right_logical(pos, 3) * 40
        for q in range(n_tok // LANES):
            mix[:n_dev * STEP, q * LANES:(q + 1) * LANES] = (want == addr[q:q + 1, :]).astype(bf16)
        rows = jnp.dot(mix[:n_dev * STEP, :n_tok], tok[...], preferred_element_type=f32).astype(bf16)
        for k in range(n_dev):
            for h in range(STEP // PACK):
                at = k * STEP + h * PACK
                xbuf[k, u * (STEP // PACK) + h] = rows[at:at + PACK]
        for lo, hi, j in cfg['pieces']:
            @pl.when(u == -(-hi // STEP) - 1)
            def _():
                for k in order:
                    dispatch(j, k, lax.rem(me + k, n_dev), lo // PACK, (hi - lo) // PACK).start()

        @pl.when(u == 0)
        def _():
            for s in range(2):
                for copy in fetch(s, s):
                    copy.start()

    def ffn(s, b):
        unit = me * USTRIDE + s
        lane = lax.broadcasted_iota(i32, (1, n_dev * WIN), 1)
        which = lax.shift_right_logical(lane, 6)
        off = jnp.zeros((1, n_dev * WIN), i32)
        num = jnp.zeros((1, n_dev * WIN), i32)
        for k in range(n_dev):
            src = lax.rem(me + n_dev - k, n_dev)
            load, start = meta[src, unit], meta[n_dev + src, unit]
            blk = lax.shift_right_logical(start, 4)
            base = blk * PACK
            for q in range(WIN // PACK):
                win[k * WIN + q * PACK:k * WIN + (q + 1) * PACK, :] = xbuf[k, blk + q]
            off = jnp.where(which == k, base - start, off)
            num = jnp.where(which == k, load, num)
        nth = (lane & (WIN - 1)) + off
        target = jnp.where((nth >= 0) & (nth < num), nth + which * part, -1)
        pick = (lax.broadcasted_iota(i32, (m_rows, n_dev * WIN), 0) == target).astype(bf16)
        xs[...] = jnp.dot(pick, win[...], preferred_element_type=f32).astype(bf16)
        tile = 512
        for t in range(d_ff // tile):
            pre = jnp.dot(xs[...], up[b, :, t * tile:(t + 1) * tile], preferred_element_type=f32)
            mix[:, t * tile:(t + 1) * tile] = gelu(pre).astype(bf16)
        tile = 256
        for t in range(d_model // tile):
            o = jnp.dot(mix[:, :d_ff], down[b, :, t * tile:(t + 1) * tile], preferred_element_type=f32).astype(bf16)
            for k in range(n_dev):
                ybuf[k, pl.ds(pl.multiple_of(s * part, PACK), part), t * tile:(t + 1) * tile] = o[k * part:(k + 1) * part]

    def give_back(j, k):
        rows = pl.ds(ret[j] // PACK, (ret[j + 1] - ret[j]) // PACK)
        peer = lax.rem(me + n_dev - k, n_dev)
        return pltpu.make_async_remote_copy(src_ref=recv.at[k, rows], dst_ref=back.at[k, rows], send_sem=rsend.at[j, k], recv_sem=rrecv.at[j, k], device_id={'ep': peer}, device_id_type=MESH)

    def give_own(j):
        rows = pl.ds(ret[j] // PACK, (ret[j + 1] - ret[j]) // PACK)
        return pltpu.make_async_copy(recv.at[0, rows], back.at[0, rows], rrecv.at[j, 0])

    def combine(j):
        n_rows = ret[j + 1] - ret[j]
        n_win = last[j] + 1 - ret_lo[j]
        width = n_win * part

        @pl.loop(0, n_dev)
        def _(i):
            k = lax.rem(n_dev // 2 + 3 * i, n_dev)
            src = lax.rem(me + n_dev - k, n_dev)
            lane = lax.broadcasted_iota(i32, (1, width), 1)
            target = jnp.full((1, width), -1, i32)
            for w in range(n_win):
                unit = me * USTRIDE + ret_lo[j] + w
                load, start = meta[src, unit], meta[n_dev + src, unit]
                nth = lane - w * part
                target = jnp.where((nth >= 0) & (nth < load), nth + start, target)
            pick = (lax.broadcasted_iota(i32, (n_rows, width), 0) + ret[j] == target).astype(bf16)
            rows = ybuf[k, ret_lo[j] * part:(last[j] + 1) * part, :]
            mixed = jnp.dot(pick, rows, preferred_element_type=f32).astype(bf16)
            recv[k, ret[j] // PACK:ret[j + 1] // PACK] = mixed.reshape(n_rows // PACK, PACK, d_model)

            @pl.when(k == 0)
            def _():
                give_own(j).start()

            @pl.when(k != 0)
            def _():
                give_back(j, k).start()

    @pl.loop(0, n_slot)
    def _(s):
        for j in range(len(first)):
            @pl.when(s == first[j])
            def _():
                for k in range(1, n_dev):
                    dispatched(j, k, lax.rem(me + n_dev - k, n_dev)).wait_recv()
                    dispatched(j, k, lax.rem(me + k, n_dev)).wait_send()

                @pl.loop(1, n_dev)
                def _(k):
                    @pl.loop(disp[j] // PACK, disp[j + 1] // PACK)
                    def _(b):
                        xbuf[k, b] = recv[k, b]

        b = lax.rem(s, 2)
        for copy in fetch(s, b):
            copy.wait()
        ffn(s, b)

        @pl.when(s + 2 < n_slot)
        def _():
            for copy in fetch(s + 2, b):
                copy.start()

        for j in range(len(last)):
            @pl.when(s == last[j])
            def _():
                combine(j)

    for k in range(1, n_dev):
        for j in range(len(last)):
            give_back(j, k).wait_send()
            give_back(j, k).wait_recv()
    for j in range(len(last)):
        give_own(j).wait()


def plan(n_dev, n_slot, n_pairs, bound, stride, z, cap, returns):
    mean = n_pairs / (n_dev * n_slot)
    spread = 9.3 * mean / 30.1
    hi = [bound * (s + 1) for s in range(n_slot)]
    lo = [0] * n_slot
    if z is not None:
        hi = [min(hi[s], math.ceil(mean * (s + 1) + z * spread * math.sqrt(s + 1)), cap) for s in range(n_slot)]
        lo = [max(0, math.floor(mean * (s + 1) - z * spread * math.sqrt(s + 1))) for s in range(n_slot - 1)] + [0]
    disp = [0, cap] if z is None else list(range(0, cap - CHUNK // 4, CHUNK)) + [cap]
    pieces = [(0, STEP, 0), (STEP, 2 * STEP, 0), (2 * STEP, disp[1], 0)]
    pieces += [(disp[j], disp[j + 1], j) for j in range(1, len(disp) - 1)]
    ret = [0] + [lo[s] // PACK * PACK for s in returns[:-1]] + [cap]
    ret_lo = [min(s for s in range(n_slot) if hi[s] > ret[j]) for j in range(len(returns))]
    first = [min((s for s in range(n_slot) if hi[s] > d), default=n_slot - 1) for d in disp[:-1]]
    return dict(n_dev=n_dev, n_slot=n_slot, cap=cap, stride=stride, pieces=pieces, lo=lo, hi=hi, first=first, last=list(returns), disp=disp, ret=ret, ret_lo=ret_lo, part=up_to(bound, PACK))


def solution(mesh):
    n_dev = mesh.shape['ep']

    def group_layer(tokens, topk_idx, topk_w, w_up, w_down, slot_expert):
        n_tok, d_model = tokens.shape
        n_slot = slot_expert.shape[1]
        d_ff = w_up.shape[3]
        n_pairs = n_tok * topk_idx.shape[1]
        base_load = n_pairs // (n_dev * n_slot)
        bound = base_load + base_load // 2 + 1
        mean = n_pairs // n_dev
        stride = up_to(n_slot * bound, PACK)
        caps = [min(stride, up_to(math.ceil(mean * f), PACK)) for f in TIERS]
        cuts = [n_slot * c // 17 - 1 for c in (6, 9, 12, 15, 17)]
        plans = [plan(n_dev, n_slot, n_pairs, bound, stride, 4.0, c, cuts) for c in caps]
        plans.append(plan(n_dev, n_slot, n_pairs, bound, stride, None, stride, [n_slot - 1]))
        wide_bounds = plan(n_dev, n_slot, n_pairs, bound, stride, 4.0, stride, cuts)
        n_rows = n_pairs // LANES
        n_units = n_dev * USTRIDE
        f32, bf16, i32 = jnp.float32, jnp.bfloat16, jnp.int32
        vmem = pl.BlockSpec(memory_space=pltpu.VMEM)
        smem = pl.BlockSpec(memory_space=pltpu.SMEM)
        hbm = pl.BlockSpec(memory_space=pl.ANY)
        big = 63 * 1024 * 1024

        addr, meta, flag = pl.pallas_call(
            functools.partial(route_kernel, n_dev, n_slot, stride, bound, wide_bounds['lo'], wide_bounds['hi'], caps),
            out_shape=[jax.ShapeDtypeStruct((n_rows, LANES), i32), jax.ShapeDtypeStruct((2 * n_dev, n_units), i32), jax.ShapeDtypeStruct((1, 1), i32)],
            in_specs=[vmem, smem],
            out_specs=[vmem, vmem, smem],
            scratch_shapes=[pltpu.VMEM((SUB, LANES), i32), pltpu.VMEM((n_dev, SUB, LANES), i32), pltpu.VMEM((n_rows, LANES), f32), pltpu.VMEM((n_units, LANES), i32), pltpu.VMEM((4 * n_dev, LANES), f32), pltpu.SemaphoreType.DMA((n_dev,)), pltpu.SemaphoreType.DMA((n_dev,))],
            compiler_params=pltpu.CompilerParams(collective_id=0, has_side_effects=True),
            name='route',
        )(topk_idx.reshape(n_rows, LANES), slot_expert)

        d_tiles = d_model // LANES
        wide = pltpu.VMEM((n_dev * stride * d_tiles, LANES), f32)
        tmp = pltpu.VMEM((LANES * d_tiles, LANES), f32)
        block = pltpu.VMEM((n_dev, stride // PACK, PACK, d_model), bf16)
        rows_vmem = pltpu.VMEM((n_tok, d_model), bf16)
        sem, sems = pltpu.SemaphoreType.DMA, pltpu.SemaphoreType.DMA((n_dev,))
        def run(cfg, meta, addr, tokens, w_up, w_down):
            part, cap = cfg['part'], cfg['cap']
            m_rows = n_dev * part
            sent = pltpu.SemaphoreType.DMA((len(cfg['first']), n_dev))
            given = pltpu.SemaphoreType.DMA((len(cfg['last']), n_dev))
            return pl.pallas_call(
                functools.partial(expert_kernel, cfg),
                out_shape=jax.ShapeDtypeStruct((n_dev, stride // PACK, PACK, d_model), bf16),
                in_specs=[smem, vmem, hbm, hbm, hbm],
                out_specs=hbm,
                scratch_shapes=[
                    rows_vmem,
                    pltpu.VMEM((n_dev, cap // PACK, PACK, d_model), bf16),
                    pltpu.VMEM((n_dev, (up_to(cap, STEP) + WIN) // PACK, PACK, d_model), bf16),
                    pltpu.VMEM((n_dev, n_slot * part, d_model), bf16),
                    pltpu.VMEM((2, d_model, d_ff), bf16),
                    pltpu.VMEM((2, d_ff, d_model), bf16),
                    pltpu.VMEM((m_rows, max(d_ff, n_tok)), bf16),
                    pltpu.VMEM((m_rows, d_model), bf16),
                    pltpu.VMEM((n_dev * WIN, d_model), bf16),
                    sent, sent, given, given,
                    pltpu.SemaphoreType.DMA((2, 2)),
                    sem,
                ],
                compiler_params=pltpu.CompilerParams(collective_id=1, has_side_effects=True, vmem_limit_bytes=big),
                name='experts',
            )(meta, addr, tokens, w_up, w_down)

        back = lax.switch(flag[0, 0], [functools.partial(run, p) for p in plans], meta, addr, tokens, w_up[0], w_down[0])

        return pl.pallas_call(
            functools.partial(unpack_kernel, caps[-1], len(caps)),
            out_shape=jax.ShapeDtypeStruct((n_tok, d_model), bf16),
            in_specs=[smem, smem, smem, hbm],
            out_specs=hbm,
            scratch_shapes=[block, wide, tmp, rows_vmem, sems, sem],
            compiler_params=pltpu.CompilerParams(vmem_limit_bytes=big),
            name='unpack',
        )(addr, flag, topk_w.reshape(n_rows, LANES), back)

    row_spec = P(('dp', 'ep'), None)
    weight_spec = P('ep', None, None, None)
    return jax.shard_map(group_layer, mesh=mesh, in_specs=(row_spec, row_spec, row_spec, weight_spec, weight_spec, P(None, None)), out_specs=row_spec, check_vma=False)
```

```python
import functools
import math

import jax
import jax.numpy as jnp
from jax import lax
from jax.experimental import pallas as pl
from jax.experimental.pallas import tpu as pltpu
from jax.sharding import PartitionSpec as P

MESH = pl.DeviceIdType.MESH
LANES = 128
SUB = 8
PACK = 16
USTRIDE = 32
WIN = 64
STEP = 32
CHUNK = 128
TIERS = (1.125, 1.156, 1.21875)


def up_to(x, m):
    return -(-x // m) * m


def group_barrier(n_dev, me):
    barrier = pltpu.get_barrier_semaphore()
    for k in range(1, n_dev):
        pl.semaphore_signal(barrier, inc=1, device_id={'ep': lax.rem(me + k, n_dev)}, device_id_type=MESH)
    pl.semaphore_wait(barrier, n_dev - 1)


def level_copies(loads, where, copies, bound):
    n_copy = len(where)
    f32, bf16 = jnp.float32, jnp.bfloat16
    share = [jnp.where(k < copies, loads / jnp.maximum(copies, 1.0), 0.0) for k in range(n_copy)]
    for _ in range(2):
        block = sum(lax.dot_general(share[k].astype(bf16), where[k], (((1,), (1,)), ((), ())), preferred_element_type=f32) for k in range(n_copy))
        there = [jnp.where(k < copies, jnp.dot(block.astype(bf16), where[k], preferred_element_type=f32), 0.0) for k in range(n_copy)]
        mean = sum(there) / jnp.maximum(copies, 1.0)
        share = [jnp.where(k < copies, jnp.clip(share[k] + 0.5 * (mean - there[k]), 0.0, bound), 0.0) for k in range(n_copy)]
    left, taken = loads, []
    for k in range(n_copy):
        after = jnp.maximum(copies - (k + 1), 0.0)
        want = jnp.floor(share[k] + 0.5)
        got = jnp.minimum(jnp.maximum(want, jnp.maximum(left - bound * after, 0.0)), jnp.minimum(left, bound))
        got = jnp.where(k < copies, got, 0.0)
        taken.append(got)
        left = left - got
    return taken


def route_kernel(n_dev, n_slot, stride, bound, low, high, caps, idx, table, addr, meta, flag, hsend, hall, hrow, tabcol, cums, ssem, rsem):
    me = lax.axis_index('ep')
    f32, bf16, i32 = jnp.float32, jnp.bfloat16, jnp.int32
    n_rows = idx.shape[0]
    n_units = n_dev * USTRIDE
    n_copy = 4
    nt = (((1,), (1,)), ((), ()))
    group_barrier(n_dev, me)
    sub_e = lax.broadcasted_iota(i32, (LANES, LANES), 0)
    lane_e = lax.broadcasted_iota(i32, (LANES, LANES), 1)
    ones = jnp.ones((SUB, LANES), bf16)

    @pl.loop(0, n_rows // SUB)
    def _(g):
        base = pl.multiple_of(g * SUB, SUB)
        rows = idx[pl.ds(base, SUB), :]
        parts = []
        for r in range(SUB):
            hot = (sub_e == rows[r:r + 1, :]).astype(bf16)
            parts.append(lax.dot_general(ones, hot, nt, preferred_element_type=f32)[0:1])
        hrow[pl.ds(base, SUB), :] = jnp.concatenate(parts, axis=0)

    hrows = hrow[...]
    hist = jnp.broadcast_to(jnp.sum(hrows, axis=0, keepdims=True), (SUB, LANES)).astype(i32)
    hsend[...] = hist
    hall[me] = hist
    sends = []
    for k in range(1, n_dev):
        copy = pltpu.make_async_remote_copy(src_ref=hsend, dst_ref=hall.at[me], send_sem=ssem.at[k], recv_sem=rsem.at[k], device_id={'ep': lax.rem(me + k, n_dev)}, device_id_type=MESH)
        copy.start()
        sends.append(copy)

    rr = lax.broadcasted_iota(i32, (n_rows, n_rows), 0)
    cc = lax.broadcasted_iota(i32, (n_rows, n_rows), 1)
    hrow[...] = jnp.dot((cc < rr).astype(bf16), hrows.astype(bf16), preferred_element_type=f32)
    tri = (sub_e < lane_e).astype(bf16)

    @pl.loop(0, n_rows // SUB)
    def _(g):
        base = pl.multiple_of(g * SUB, SUB)
        rows = idx[pl.ds(base, SUB), :]
        runs = hrow[pl.ds(base, SUB), :].astype(bf16)
        parts = []
        for r in range(SUB):
            hot = sub_e == rows[r:r + 1, :]
            hot_b = hot.astype(bf16)
            prefix = jnp.dot(hot_b, tri, preferred_element_type=f32)
            run = jnp.dot(runs, hot_b, preferred_element_type=f32)[r:r + 1]
            parts.append(jnp.sum(jnp.where(hot, prefix, 0.0), axis=0, keepdims=True) + run)
        addr[pl.ds(base, SUB), :] = jnp.concatenate(parts, axis=0).astype(i32)

    lane_u = lax.broadcasted_iota(i32, (1, n_units), 1)
    tabrow = jnp.full((1, n_units), -1, i32)
    tabcol[...] = jnp.full(tabcol.shape, -1, i32)
    for d in range(n_dev):
        for s in range(n_slot):
            u = d * USTRIDE + s
            tabrow = jnp.where(lane_u == u, table[d, s], tabrow)
            tabcol[u:u + 1, :] = jnp.full((1, LANES), table[d, s], i32)
    tcol = tabcol[...]
    unit_exp = (tcol == lax.broadcasted_iota(i32, (n_units, LANES), 1)).astype(bf16)
    same = jnp.concatenate([tcol] * (n_units // LANES), axis=1) == tabrow
    su = lax.broadcasted_iota(i32, (n_units, n_units), 0)
    lu = lax.broadcasted_iota(i32, (n_units, n_units), 1)
    valid = tabrow >= 0
    copy_rank = jnp.where(valid, jnp.sum(jnp.where(same & (su < lu), 1.0, 0.0), axis=0, keepdims=True).astype(i32), -1)
    before = ((su < lu) & (lax.shift_right_logical(su, 5) == lax.shift_right_logical(lu, 5))).astype(bf16)
    copies = jnp.dot(jnp.ones((SUB, n_units), bf16), unit_exp, preferred_element_type=f32)[0:1]
    dev8 = lax.broadcasted_iota(i32, (SUB, n_units), 0)
    dev_u = lax.shift_right_logical(lane_u, 5)
    where = [jnp.dot(((dev8 == dev_u) & (copy_rank == k)).astype(bf16), unit_exp, preferred_element_type=f32).astype(bf16) for k in range(n_copy)]

    for k in range(1, n_dev):
        src = lax.rem(me + n_dev - k, n_dev)
        pltpu.make_async_remote_copy(src_ref=hsend, dst_ref=hall.at[src], send_sem=ssem.at[k], recv_sem=rsem.at[k], device_id={'ep': src}, device_id_type=MESH).wait_recv()
    every = jnp.concatenate([hall[p, 0:1, :] for p in range(n_dev)], axis=0).astype(f32)
    taken = level_copies(every, where, copies, float(bound))
    loads = jnp.zeros((n_dev, n_units), f32)
    cum = jnp.zeros((n_dev, LANES), f32)
    for k in range(n_copy):
        per_unit = lax.dot_general(taken[k].astype(bf16), unit_exp, nt, preferred_element_type=f32)
        loads = jnp.where(copy_rank == k, per_unit, loads)
        cums[k * n_dev:(k + 1) * n_dev, :] = cum
        cum = cum + taken[k]
    starts = jnp.dot(loads.astype(bf16), before, preferred_element_type=f32)
    meta[0:n_dev, :] = loads.astype(i32)
    meta[n_dev:2 * n_dev, :] = starts.astype(i32)

    block = lax.rem(dev_u + n_dev - me, n_dev)
    first = meta[pl.ds(n_dev + me, 1), :] + block * stride
    row8 = lax.broadcasted_iota(i32, (2 * n_copy, n_units), 0)
    half = jnp.where(row8 < n_copy, lax.shift_right_logical(first, 6), first & 63)
    half = jnp.where(copy_rank == (row8 & (n_copy - 1)), half, 0)
    place = jnp.dot(half.astype(bf16), unit_exp, preferred_element_type=f32).astype(i32)
    own = [cums[pl.ds(k * n_dev + me, 1), :].astype(i32) for k in range(n_copy)]
    offs = [place[k:k + 1] * 64 + place[n_copy + k:n_copy + k + 1] - own[k] + 256 for k in range(n_copy)]
    bar = [jnp.where(copies > k, own[k], 255) for k in range(1, n_copy)]
    rows = [lax.shift_right_logical(o, 6) for o in offs] + [o & 63 for o in offs] + bar + [jnp.zeros((1, LANES), i32)] * 5
    lookup = jnp.concatenate(rows, axis=0).astype(f32).astype(bf16)

    @pl.loop(0, n_rows // SUB)
    def _(g):
        base = pl.multiple_of(g * SUB, SUB)
        ids = idx[pl.ds(base, SUB), :]
        ranks = addr[pl.ds(base, SUB), :]
        parts = []
        for r in range(SUB):
            rank = ranks[r:r + 1, :]
            hot_b = (sub_e == ids[r:r + 1, :]).astype(bf16)
            got = jnp.dot(lookup, hot_b, preferred_element_type=f32).astype(i32)
            pos = got[0:1] * 64 + got[n_copy:n_copy + 1]
            for k in range(1, n_copy):
                pos = jnp.where(rank >= got[2 * n_copy + k - 1:2 * n_copy + k], got[k:k + 1] * 64 + got[n_copy + k:n_copy + k + 1], pos)
            pos = pos + rank - 256
            parts.append(pos + lax.shift_right_logical(pos, 3) * 40)
        addr[pl.ds(base, SUB), :] = jnp.concatenate(parts, axis=0)

    slot_id = lane_u & (USTRIDE - 1)
    lo_row = jnp.zeros((1, n_units), f32)
    hi_row = jnp.zeros((1, n_units), f32)
    for s in range(n_slot):
        lo_row = jnp.where(slot_id == s, float(low[s]), lo_row)
        hi_row = jnp.where(slot_id == s, float(high[s]), hi_row)
    ends = loads + starts
    bad = jnp.max(jnp.where(valid & ((ends < lo_row) | (ends > hi_row)), 1.0, 0.0))
    top = jnp.max(jnp.where(valid, ends, 0.0))
    tier = jnp.where(bad > 0.0, float(len(caps)), sum(jnp.where(top > float(c), 1.0, 0.0) for c in caps))
    flag[0, 0] = tier.astype(i32)
    for copy in sends:
        copy.wait_send()


def unpack_kernel(cap, slow, addr, flag, gate, back_hbm, out_hbm, back, wide, tmp, out, bsem, osem):
    n_rows, n_col = addr.shape
    n_dev, stride = back.shape[0], back.shape[1] * PACK
    d_tiles = out.shape[1] // LANES
    step = SUB * d_tiles

    def load(k, lo, hi):
        rows = pl.ds(lo // PACK, (hi - lo) // PACK)
        return pltpu.make_async_copy(back_hbm.at[k, rows], back.at[k, rows], bsem.at[k])

    def widen(k, b):
        base = (k * (stride // PACK) + b) * (2 * step)
        for j in range(d_tiles):
            x = back[k, b, :, j * LANES:(j + 1) * LANES].astype(jnp.float32)
            wide[pl.ds(base + j * SUB, SUB), :] = x[:SUB]
            wide[pl.ds(base + step + j * SUB, SUB), :] = x[SUB:]

    @pl.loop(0, n_dev)
    def _(k):
        load(k, 0, cap).start()

    @pl.loop(0, n_dev)
    def _(k):
        load(k, 0, cap).wait()

        @pl.loop(0, cap // PACK, unroll=4)
        def _(b):
            widen(k, b)

    @pl.when(flag[0, 0] == slow)
    def _():
        @pl.loop(0, n_dev)
        def _(k):
            rest = load(k, cap, stride)
            rest.start()
            rest.wait()

            @pl.loop(cap // PACK, stride // PACK)
            def _(b):
                widen(k, b)

    def give(g):
        rows = pl.ds(pl.multiple_of(g * n_col, n_col), n_col)
        return pltpu.make_async_copy(out.at[rows], out_hbm.at[rows], osem)

    @pl.loop(0, n_rows)
    def _(r):
        scale = jnp.broadcast_to(gate[pl.ds(r, 1), :], (LANES, n_col)).T
        for c in range(n_col // PACK):
            at = c * 2 * step
            for i in range(PACK):
                a = addr[r, c * PACK + i]
                tmp[pl.ds(at + (i // SUB) * step + i % SUB, d_tiles, stride=SUB), :] = wide[pl.ds(a, d_tiles, stride=SUB), :]
            rows = pl.ds(pl.multiple_of(r * n_col + c * PACK, PACK), PACK)
            for j in range(d_tiles):
                top = tmp[at + j * SUB:at + (j + 1) * SUB, :] * scale[c * PACK:c * PACK + SUB]
                bot = tmp[at + step + j * SUB:at + step + (j + 1) * SUB, :] * scale[c * PACK + SUB:(c + 1) * PACK]
                out[rows, j * LANES:(j + 1) * LANES] = jnp.concatenate([top, bot], axis=0).astype(jnp.bfloat16)
        give(r).start()

    @pl.loop(0, n_rows)
    def _(r):
        give(r).wait()


def gelu(x):
    return x * (0.5 * (1.0 + jnp.tanh(0.7978845608028654 * (x + 0.044715 * (x * x * x)))))


def expert_kernel(cfg, meta, addr, tok_hbm, up_hbm, down_hbm, back, tok, recv, xbuf, ybuf, up, down, mix, xs, win, dsend, drecv, rsend, rrecv, wsem, tsem):
    n_dev, n_slot, part, stride = cfg['n_dev'], cfg['n_slot'], cfg['part'], cfg['stride']
    m_rows = n_dev * part
    n_tok, d_model, d_ff = tok.shape[0], up_hbm.shape[1], up_hbm.shape[2]
    first, last, disp, ret, ret_lo = cfg['first'], cfg['last'], cfg['disp'], cfg['ret'], cfg['ret_lo']
    n_step = -(-disp[-1] // STEP)
    f32, bf16, i32 = jnp.float32, jnp.bfloat16, jnp.int32
    me = lax.axis_index('ep')

    def fetch(s, b):
        return (pltpu.make_async_copy(up_hbm.at[s], up.at[b], wsem.at[0, b]), pltpu.make_async_copy(down_hbm.at[s], down.at[b], wsem.at[1, b]))

    load_tok = pltpu.make_async_copy(tok_hbm, tok, tsem)
    load_tok.start()
    group_barrier(n_dev, me)
    tail = n_step * (STEP // PACK)

    @pl.loop(0, n_dev)
    def _(k):
        xbuf[k, tail:] = jnp.zeros((xbuf.shape[1] - tail, PACK, d_model), bf16)

    def dispatch(j, k, peer, lo, num):
        return pltpu.make_async_remote_copy(src_ref=xbuf.at[k, pl.ds(lo, num)], dst_ref=recv.at[k, pl.ds(lo, num)], send_sem=dsend.at[j, k], recv_sem=drecv.at[j, k], device_id={'ep': peer}, device_id_type=MESH)

    def dispatched(j, k, peer):
        return dispatch(j, k, peer, disp[j] // PACK, (disp[j + 1] - disp[j]) // PACK)

    order = sorted(range(1, n_dev), key=lambda k: (abs(k - n_dev // 2), k))
    load_tok.wait()

    @pl.loop(0, n_step)
    def _(u):
        row = lax.broadcasted_iota(i32, (n_dev * STEP, LANES), 0)
        pos = lax.shift_right_logical(row, 5) * stride + (row & (STEP - 1)) + u * STEP
        want = pos + lax.shift_right_logical(pos, 3) * 40
        for q in range(n_tok // LANES):
            mix[:n_dev * STEP, q * LANES:(q + 1) * LANES] = (want == addr[q:q + 1, :]).astype(bf16)
        rows = jnp.dot(mix[:n_dev * STEP, :n_tok], tok[...], preferred_element_type=f32).astype(bf16)
        for k in range(n_dev):
            for h in range(STEP // PACK):
                at = k * STEP + h * PACK
                xbuf[k, u * (STEP // PACK) + h] = rows[at:at + PACK]
        for lo, hi, j in cfg['pieces']:
            @pl.when(u == -(-hi // STEP) - 1)
            def _():
                for k in order:
                    dispatch(j, k, lax.rem(me + k, n_dev), lo // PACK, (hi - lo) // PACK).start()

        @pl.when(u == 0)
        def _():
            for s in range(2):
                for copy in fetch(s, s):
                    copy.start()

    def ffn(s, b):
        unit = me * USTRIDE + s
        lane = lax.broadcasted_iota(i32, (1, n_dev * WIN), 1)
        which = lax.shift_right_logical(lane, 6)
        off = jnp.zeros((1, n_dev * WIN), i32)
        num = jnp.zeros((1, n_dev * WIN), i32)
        for k in range(n_dev):
            src = lax.rem(me + n_dev - k, n_dev)
            load, start = meta[src, unit], meta[n_dev + src, unit]
            blk = lax.shift_right_logical(start, 4)
            base = blk * PACK
            for q in range(WIN // PACK):
                win[k * WIN + q * PACK:k * WIN + (q + 1) * PACK, :] = xbuf[k, blk + q]
            off = jnp.where(which == k, base - start, off)
            num = jnp.where(which == k, load, num)
        nth = (lane & (WIN - 1)) + off
        target = jnp.where((nth >= 0) & (nth < num), nth + which * part, -1)
        pick = (lax.broadcasted_iota(i32, (m_rows, n_dev * WIN), 0) == target).astype(bf16)
        xs[...] = jnp.dot(pick, win[...], preferred_element_type=f32).astype(bf16)
        tile = 512
        for t in range(d_ff // tile):
            pre = jnp.dot(xs[...], up[b, :, t * tile:(t + 1) * tile], preferred_element_type=f32)
            mix[:, t * tile:(t + 1) * tile] = gelu(pre).astype(bf16)
        tile = 256
        for t in range(d_model // tile):
            o = jnp.dot(mix[:, :d_ff], down[b, :, t * tile:(t + 1) * tile], preferred_element_type=f32).astype(bf16)
            for k in range(n_dev):
                ybuf[k, pl.ds(pl.multiple_of(s * part, PACK), part), t * tile:(t + 1) * tile] = o[k * part:(k + 1) * part]

    def give_back(j, k):
        rows = pl.ds(ret[j] // PACK, (ret[j + 1] - ret[j]) // PACK)
        peer = lax.rem(me + n_dev - k, n_dev)
        return pltpu.make_async_remote_copy(src_ref=recv.at[k, rows], dst_ref=back.at[k, rows], send_sem=rsend.at[j, k], recv_sem=rrecv.at[j, k], device_id={'ep': peer}, device_id_type=MESH)

    def give_own(j):
        rows = pl.ds(ret[j] // PACK, (ret[j + 1] - ret[j]) // PACK)
        return pltpu.make_async_copy(recv.at[0, rows], back.at[0, rows], rrecv.at[j, 0])

    def combine(j):
        n_rows = ret[j + 1] - ret[j]
        n_win = last[j] + 1 - ret_lo[j]
        width = n_win * part

        @pl.loop(0, n_dev)
        def _(i):
            k = lax.rem(n_dev // 2 + 3 * i, n_dev)
            src = lax.rem(me + n_dev - k, n_dev)
            lane = lax.broadcasted_iota(i32, (1, width), 1)
            target = jnp.full((1, width), -1, i32)
            for w in range(n_win):
                unit = me * USTRIDE + ret_lo[j] + w
                load, start = meta[src, unit], meta[n_dev + src, unit]
                nth = lane - w * part
                target = jnp.where((nth >= 0) & (nth < load), nth + start, target)
            pick = (lax.broadcasted_iota(i32, (n_rows, width), 0) + ret[j] == target).astype(bf16)
            rows = ybuf[k, ret_lo[j] * part:(last[j] + 1) * part, :]
            mixed = jnp.dot(pick, rows, preferred_element_type=f32).astype(bf16)
            recv[k, ret[j] // PACK:ret[j + 1] // PACK] = mixed.reshape(n_rows // PACK, PACK, d_model)

            @pl.when(k == 0)
            def _():
                give_own(j).start()

            @pl.when(k != 0)
            def _():
                give_back(j, k).start()

    @pl.loop(0, n_slot)
    def _(s):
        for j in range(len(first)):
            @pl.when(s == first[j])
            def _():
                for k in range(1, n_dev):
                    dispatched(j, k, lax.rem(me + n_dev - k, n_dev)).wait_recv()
                    dispatched(j, k, lax.rem(me + k, n_dev)).wait_send()

                @pl.loop(1, n_dev)
                def _(k):
                    @pl.loop(disp[j] // PACK, disp[j + 1] // PACK)
                    def _(b):
                        xbuf[k, b] = recv[k, b]

        b = lax.rem(s, 2)
        for copy in fetch(s, b):
            copy.wait()
        ffn(s, b)

        @pl.when(s + 2 < n_slot)
        def _():
            for copy in fetch(s + 2, b):
                copy.start()

        for j in range(len(last)):
            @pl.when(s == last[j])
            def _():
                combine(j)

    for k in range(1, n_dev):
        for j in range(len(last)):
            give_back(j, k).wait_send()
            give_back(j, k).wait_recv()
    for j in range(len(last)):
        give_own(j).wait()


def plan(n_dev, n_slot, n_pairs, bound, stride, z, cap, returns):
    mean = n_pairs / (n_dev * n_slot)
    spread = 9.3 * mean / 30.1
    hi = [bound * (s + 1) for s in range(n_slot)]
    lo = [0] * n_slot
    if z is not None:
        hi = [min(hi[s], math.ceil(mean * (s + 1) + z * spread * math.sqrt(s + 1)), cap) for s in range(n_slot)]
        lo = [max(0, math.floor(mean * (s + 1) - (z - 0.5) * spread * math.sqrt(s + 1))) if s in returns[:-1] else 0 for s in range(n_slot)]
    disp = [0, cap] if z is None else list(range(0, cap - CHUNK, CHUNK)) + [cap]
    pieces = [(0, STEP, 0), (STEP, 2 * STEP, 0), (2 * STEP, disp[1], 0)]
    pieces += [(disp[j], disp[j + 1], j) for j in range(1, len(disp) - 1)]
    ret = [0] + [lo[s] // PACK * PACK for s in returns[:-1]] + [cap]
    ret_lo = [min(s for s in range(n_slot) if hi[s] > ret[j]) for j in range(len(returns))]
    first = [min((s for s in range(n_slot) if hi[s] > d), default=n_slot - 1) for d in disp[:-1]]
    return dict(n_dev=n_dev, n_slot=n_slot, cap=cap, stride=stride, pieces=pieces, lo=lo, hi=hi, first=first, last=list(returns), disp=disp, ret=ret, ret_lo=ret_lo, part=up_to(bound, PACK))


def solution(mesh):
    n_dev = mesh.shape['ep']

    def group_layer(tokens, topk_idx, topk_w, w_up, w_down, slot_expert):
        n_tok, d_model = tokens.shape
        n_slot = slot_expert.shape[1]
        d_ff = w_up.shape[3]
        n_pairs = n_tok * topk_idx.shape[1]
        base_load = n_pairs // (n_dev * n_slot)
        bound = base_load + base_load // 2 + 1
        mean = n_pairs // n_dev
        stride = up_to(n_slot * bound, PACK)
        caps = [min(stride, up_to(math.ceil(mean * f), PACK)) for f in TIERS]
        cuts = [n_slot * c // 17 - 1 for c in (9, 12, 16, 17)]
        plans = [plan(n_dev, n_slot, n_pairs, bound, stride, 4.0, c, cuts) for c in caps]
        plans.append(plan(n_dev, n_slot, n_pairs, bound, stride, None, stride, [n_slot - 1]))
        wide_bounds = plan(n_dev, n_slot, n_pairs, bound, stride, 4.0, stride, cuts)
        n_rows = n_pairs // LANES
        n_units = n_dev * USTRIDE
        f32, bf16, i32 = jnp.float32, jnp.bfloat16, jnp.int32
        vmem = pl.BlockSpec(memory_space=pltpu.VMEM)
        smem = pl.BlockSpec(memory_space=pltpu.SMEM)
        hbm = pl.BlockSpec(memory_space=pl.ANY)
        big = 63 * 1024 * 1024

        addr, meta, flag = pl.pallas_call(
            functools.partial(route_kernel, n_dev, n_slot, stride, bound, wide_bounds['lo'], wide_bounds['hi'], caps),
            out_shape=[jax.ShapeDtypeStruct((n_rows, LANES), i32), jax.ShapeDtypeStruct((2 * n_dev, n_units), i32), jax.ShapeDtypeStruct((1, 1), i32)],
            in_specs=[vmem, smem],
            out_specs=[vmem, vmem, smem],
            scratch_shapes=[pltpu.VMEM((SUB, LANES), i32), pltpu.VMEM((n_dev, SUB, LANES), i32), pltpu.VMEM((n_rows, LANES), f32), pltpu.VMEM((n_units, LANES), i32), pltpu.VMEM((4 * n_dev, LANES), f32), pltpu.SemaphoreType.DMA((n_dev,)), pltpu.SemaphoreType.DMA((n_dev,))],
            compiler_params=pltpu.CompilerParams(collective_id=0, has_side_effects=True),
            name='route',
        )(topk_idx.reshape(n_rows, LANES), slot_expert)

        d_tiles = d_model // LANES
        wide = pltpu.VMEM((n_dev * stride * d_tiles, LANES), f32)
        tmp = pltpu.VMEM((LANES * d_tiles, LANES), f32)
        block = pltpu.VMEM((n_dev, stride // PACK, PACK, d_model), bf16)
        rows_vmem = pltpu.VMEM((n_tok, d_model), bf16)
        sem, sems = pltpu.SemaphoreType.DMA, pltpu.SemaphoreType.DMA((n_dev,))
        def run(cfg, meta, addr, tokens, w_up, w_down):
            part, cap = cfg['part'], cfg['cap']
            m_rows = n_dev * part
            sent = pltpu.SemaphoreType.DMA((len(cfg['first']), n_dev))
            given = pltpu.SemaphoreType.DMA((len(cfg['last']), n_dev))
            return pl.pallas_call(
                functools.partial(expert_kernel, cfg),
                out_shape=jax.ShapeDtypeStruct((n_dev, stride // PACK, PACK, d_model), bf16),
                in_specs=[smem, vmem, hbm, hbm, hbm],
                out_specs=hbm,
                scratch_shapes=[
                    rows_vmem,
                    pltpu.VMEM((n_dev, cap // PACK, PACK, d_model), bf16),
                    pltpu.VMEM((n_dev, (up_to(cap, STEP) + WIN) // PACK, PACK, d_model), bf16),
                    pltpu.VMEM((n_dev, n_slot * part, d_model), bf16),
                    pltpu.VMEM((2, d_model, d_ff), bf16),
                    pltpu.VMEM((2, d_ff, d_model), bf16),
                    pltpu.VMEM((m_rows, max(d_ff, n_tok)), bf16),
                    pltpu.VMEM((m_rows, d_model), bf16),
                    pltpu.VMEM((n_dev * WIN, d_model), bf16),
                    sent, sent, given, given,
                    pltpu.SemaphoreType.DMA((2, 2)),
                    sem,
                ],
                compiler_params=pltpu.CompilerParams(collective_id=1, has_side_effects=True, vmem_limit_bytes=big),
                name='experts',
            )(meta, addr, tokens, w_up, w_down)

        back = lax.switch(flag[0, 0], [functools.partial(run, p) for p in plans], meta, addr, tokens, w_up[0], w_down[0])

        return pl.pallas_call(
            functools.partial(unpack_kernel, caps[-1], len(caps)),
            out_shape=jax.ShapeDtypeStruct((n_tok, d_model), bf16),
            in_specs=[smem, smem, vmem, hbm],
            out_specs=hbm,
            scratch_shapes=[block, wide, tmp, rows_vmem, sems, sem],
            compiler_params=pltpu.CompilerParams(vmem_limit_bytes=big),
            name='unpack',
        )(addr, flag, topk_w.reshape(n_rows, LANES), back)

    row_spec = P(('dp', 'ep'), None)
    weight_spec = P('ep', None, None, None)
    return jax.shard_map(group_layer, mesh=mesh, in_specs=(row_spec, row_spec, row_spec, weight_spec, weight_spec, P(None, None)), out_specs=row_spec, check_vma=False)
```

```python
import functools
import math

import jax
import jax.numpy as jnp
from jax import lax
from jax.experimental import pallas as pl
from jax.experimental.pallas import tpu as pltpu
from jax.sharding import PartitionSpec as P

MESH = pl.DeviceIdType.MESH
LANES = 128
SUB = 8
PACK = 16
USTRIDE = 32
WIN = 64
STEP = 32
CHUNK = 128
TIERS = (1.125, 1.156, 1.21875)


def up_to(x, m):
    return -(-x // m) * m


def group_barrier(n_dev, me):
    barrier = pltpu.get_barrier_semaphore()
    for k in range(1, n_dev):
        pl.semaphore_signal(barrier, inc=1, device_id={'ep': lax.rem(me + k, n_dev)}, device_id_type=MESH)
    pl.semaphore_wait(barrier, n_dev - 1)


def level_copies(loads, where, copies, bound):
    n_copy = len(where)
    f32, bf16 = jnp.float32, jnp.bfloat16
    share = [jnp.where(k < copies, loads / jnp.maximum(copies, 1.0), 0.0) for k in range(n_copy)]
    for _ in range(2):
        block = sum(lax.dot_general(share[k].astype(bf16), where[k], (((1,), (1,)), ((), ())), preferred_element_type=f32) for k in range(n_copy))
        there = [jnp.where(k < copies, jnp.dot(block.astype(bf16), where[k], preferred_element_type=f32), 0.0) for k in range(n_copy)]
        mean = sum(there) / jnp.maximum(copies, 1.0)
        share = [jnp.where(k < copies, jnp.clip(share[k] + 0.5 * (mean - there[k]), 0.0, bound), 0.0) for k in range(n_copy)]
    left, taken = loads, []
    for k in range(n_copy):
        after = jnp.maximum(copies - (k + 1), 0.0)
        want = jnp.floor(share[k] + 0.5)
        got = jnp.minimum(jnp.maximum(want, jnp.maximum(left - bound * after, 0.0)), jnp.minimum(left, bound))
        got = jnp.where(k < copies, got, 0.0)
        taken.append(got)
        left = left - got
    return taken


def route_kernel(n_dev, n_slot, stride, bound, low, high, caps, idx, table, addr, meta, flag, hsend, hall, hrow, tabcol, cums, ssem, rsem):
    me = lax.axis_index('ep')
    f32, bf16, i32 = jnp.float32, jnp.bfloat16, jnp.int32
    n_rows = idx.shape[0]
    n_units = n_dev * USTRIDE
    n_copy = 4
    nt = (((1,), (1,)), ((), ()))
    group_barrier(n_dev, me)
    sub_e = lax.broadcasted_iota(i32, (LANES, LANES), 0)
    lane_e = lax.broadcasted_iota(i32, (LANES, LANES), 1)
    ones = jnp.ones((SUB, LANES), bf16)

    @pl.loop(0, n_rows // SUB)
    def _(g):
        base = pl.multiple_of(g * SUB, SUB)
        rows = idx[pl.ds(base, SUB), :]
        parts = []
        for r in range(SUB):
            hot = (sub_e == rows[r:r + 1, :]).astype(bf16)
            parts.append(lax.dot_general(ones, hot, nt, preferred_element_type=f32)[0:1])
        hrow[pl.ds(base, SUB), :] = jnp.concatenate(parts, axis=0)

    hrows = hrow[...]
    hist = jnp.broadcast_to(jnp.sum(hrows, axis=0, keepdims=True), (SUB, LANES)).astype(i32)
    hsend[...] = hist
    hall[me] = hist
    sends = []
    for k in range(1, n_dev):
        copy = pltpu.make_async_remote_copy(src_ref=hsend, dst_ref=hall.at[me], send_sem=ssem.at[k], recv_sem=rsem.at[k], device_id={'ep': lax.rem(me + k, n_dev)}, device_id_type=MESH)
        copy.start()
        sends.append(copy)

    rr = lax.broadcasted_iota(i32, (n_rows, n_rows), 0)
    cc = lax.broadcasted_iota(i32, (n_rows, n_rows), 1)
    hrow[...] = jnp.dot((cc < rr).astype(bf16), hrows.astype(bf16), preferred_element_type=f32)
    tri = (sub_e < lane_e).astype(bf16)

    @pl.loop(0, n_rows // SUB)
    def _(g):
        base = pl.multiple_of(g * SUB, SUB)
        rows = idx[pl.ds(base, SUB), :]
        runs = hrow[pl.ds(base, SUB), :].astype(bf16)
        parts = []
        for r in range(SUB):
            hot = sub_e == rows[r:r + 1, :]
            hot_b = hot.astype(bf16)
            prefix = jnp.dot(hot_b, tri, preferred_element_type=f32)
            run = jnp.dot(runs, hot_b, preferred_element_type=f32)[r:r + 1]
            parts.append(jnp.sum(jnp.where(hot, prefix, 0.0), axis=0, keepdims=True) + run)
        addr[pl.ds(base, SUB), :] = jnp.concatenate(parts, axis=0).astype(i32)

    lane_u = lax.broadcasted_iota(i32, (1, n_units), 1)
    tabrow = jnp.full((1, n_units), -1, i32)
    tabcol[...] = jnp.full(tabcol.shape, -1, i32)
    for d in range(n_dev):
        for s in range(n_slot):
            u = d * USTRIDE + s
            tabrow = jnp.where(lane_u == u, table[d, s], tabrow)
            tabcol[u:u + 1, :] = jnp.full((1, LANES), table[d, s], i32)
    tcol = tabcol[...]
    unit_exp = (tcol == lax.broadcasted_iota(i32, (n_units, LANES), 1)).astype(bf16)
    same = jnp.concatenate([tcol] * (n_units // LANES), axis=1) == tabrow
    su = lax.broadcasted_iota(i32, (n_units, n_units), 0)
    lu = lax.broadcasted_iota(i32, (n_units, n_units), 1)
    valid = tabrow >= 0
    copy_rank = jnp.where(valid, jnp.sum(jnp.where(same & (su < lu), 1.0, 0.0), axis=0, keepdims=True).astype(i32), -1)
    before = ((su < lu) & (lax.shift_right_logical(su, 5) == lax.shift_right_logical(lu, 5))).astype(bf16)
    copies = jnp.dot(jnp.ones((SUB, n_units), bf16), unit_exp, preferred_element_type=f32)[0:1]
    dev8 = lax.broadcasted_iota(i32, (SUB, n_units), 0)
    dev_u = lax.shift_right_logical(lane_u, 5)
    where = [jnp.dot(((dev8 == dev_u) & (copy_rank == k)).astype(bf16), unit_exp, preferred_element_type=f32).astype(bf16) for k in range(n_copy)]

    for k in range(1, n_dev):
        src = lax.rem(me + n_dev - k, n_dev)
        pltpu.make_async_remote_copy(src_ref=hsend, dst_ref=hall.at[src], send_sem=ssem.at[k], recv_sem=rsem.at[k], device_id={'ep': src}, device_id_type=MESH).wait_recv()
    every = jnp.concatenate([hall[p, 0:1, :] for p in range(n_dev)], axis=0).astype(f32)
    taken = level_copies(every, where, copies, float(bound))
    loads = jnp.zeros((n_dev, n_units), f32)
    cum = jnp.zeros((n_dev, LANES), f32)
    for k in range(n_copy):
        per_unit = lax.dot_general(taken[k].astype(bf16), unit_exp, nt, preferred_element_type=f32)
        loads = jnp.where(copy_rank == k, per_unit, loads)
        cums[k * n_dev:(k + 1) * n_dev, :] = cum
        cum = cum + taken[k]
    starts = jnp.dot(loads.astype(bf16), before, preferred_element_type=f32)
    meta[0:n_dev, :] = loads.astype(i32)
    meta[n_dev:2 * n_dev, :] = starts.astype(i32)

    block = lax.rem(dev_u + n_dev - me, n_dev)
    first = meta[pl.ds(n_dev + me, 1), :] + block * stride
    row8 = lax.broadcasted_iota(i32, (2 * n_copy, n_units), 0)
    half = jnp.where(row8 < n_copy, lax.shift_right_logical(first, 6), first & 63)
    half = jnp.where(copy_rank == (row8 & (n_copy - 1)), half, 0)
    place = jnp.dot(half.astype(bf16), unit_exp, preferred_element_type=f32).astype(i32)
    own = [cums[pl.ds(k * n_dev + me, 1), :].astype(i32) for k in range(n_copy)]
    offs = [place[k:k + 1] * 64 + place[n_copy + k:n_copy + k + 1] - own[k] + 256 for k in range(n_copy)]
    bar = [jnp.where(copies > k, own[k], 255) for k in range(1, n_copy)]
    rows = [lax.shift_right_logical(o, 6) for o in offs] + [o & 63 for o in offs] + bar + [jnp.zeros((1, LANES), i32)] * 5
    lookup = jnp.concatenate(rows, axis=0).astype(f32).astype(bf16)

    @pl.loop(0, n_rows // SUB)
    def _(g):
        base = pl.multiple_of(g * SUB, SUB)
        ids = idx[pl.ds(base, SUB), :]
        ranks = addr[pl.ds(base, SUB), :]
        parts = []
        for r in range(SUB):
            rank = ranks[r:r + 1, :]
            hot_b = (sub_e == ids[r:r + 1, :]).astype(bf16)
            got = jnp.dot(lookup, hot_b, preferred_element_type=f32).astype(i32)
            pos = got[0:1] * 64 + got[n_copy:n_copy + 1]
            for k in range(1, n_copy):
                pos = jnp.where(rank >= got[2 * n_copy + k - 1:2 * n_copy + k], got[k:k + 1] * 64 + got[n_copy + k:n_copy + k + 1], pos)
            pos = pos + rank - 256
            parts.append(pos + lax.shift_right_logical(pos, 3) * 40)
        addr[pl.ds(base, SUB), :] = jnp.concatenate(parts, axis=0)

    slot_id = lane_u & (USTRIDE - 1)
    lo_row = jnp.zeros((1, n_units), f32)
    hi_row = jnp.zeros((1, n_units), f32)
    for s in range(n_slot):
        lo_row = jnp.where(slot_id == s, float(low[s]), lo_row)
        hi_row = jnp.where(slot_id == s, float(high[s]), hi_row)
    ends = loads + starts
    bad = jnp.max(jnp.where(valid & ((ends < lo_row) | (ends > hi_row)), 1.0, 0.0))
    top = jnp.max(jnp.where(valid, ends, 0.0))
    tier = jnp.where(bad > 0.0, float(len(caps)), sum(jnp.where(top > float(c), 1.0, 0.0) for c in caps))
    flag[0, 0] = tier.astype(i32)
    for copy in sends:
        copy.wait_send()


def unpack_kernel(cap, slow, addr, flag, gate, back_hbm, out_hbm, back, wide, tmp, out, bsem, osem):
    n_rows, n_col = addr.shape
    n_dev, stride = back.shape[0], back.shape[1] * PACK
    d_tiles = out.shape[1] // LANES
    step = SUB * d_tiles

    def load(k, lo, hi):
        rows = pl.ds(lo // PACK, (hi - lo) // PACK)
        return pltpu.make_async_copy(back_hbm.at[k, rows], back.at[k, rows], bsem.at[k])

    def widen(k, b):
        base = (k * (stride // PACK) + b) * (2 * step)
        for j in range(d_tiles):
            x = back[k, b, :, j * LANES:(j + 1) * LANES].astype(jnp.float32)
            wide[pl.ds(base + j * SUB, SUB), :] = x[:SUB]
            wide[pl.ds(base + step + j * SUB, SUB), :] = x[SUB:]

    @pl.loop(0, n_dev)
    def _(k):
        load(k, 0, cap).start()

    @pl.loop(0, n_dev)
    def _(k):
        load(k, 0, cap).wait()

        @pl.loop(0, cap // PACK, unroll=4)
        def _(b):
            widen(k, b)

    @pl.when(flag[0, 0] == slow)
    def _():
        @pl.loop(0, n_dev)
        def _(k):
            rest = load(k, cap, stride)
            rest.start()
            rest.wait()

            @pl.loop(cap // PACK, stride // PACK)
            def _(b):
                widen(k, b)

    def give(g):
        rows = pl.ds(pl.multiple_of(g * n_col, n_col), n_col)
        return pltpu.make_async_copy(out.at[rows], out_hbm.at[rows], osem)

    @pl.loop(0, n_rows)
    def _(r):
        scale = jnp.broadcast_to(gate[pl.ds(r, 1), :], (LANES, n_col)).T
        for c in range(n_col // PACK):
            at = c * 2 * step
            for i in range(PACK):
                a = addr[r, c * PACK + i]
                tmp[pl.ds(at + (i // SUB) * step + i % SUB, d_tiles, stride=SUB), :] = wide[pl.ds(a, d_tiles, stride=SUB), :]
            rows = pl.ds(pl.multiple_of(r * n_col + c * PACK, PACK), PACK)
            for j in range(d_tiles):
                top = tmp[at + j * SUB:at + (j + 1) * SUB, :] * scale[c * PACK:c * PACK + SUB]
                bot = tmp[at + step + j * SUB:at + step + (j + 1) * SUB, :] * scale[c * PACK + SUB:(c + 1) * PACK]
                out[rows, j * LANES:(j + 1) * LANES] = jnp.concatenate([top, bot], axis=0).astype(jnp.bfloat16)
        give(r).start()

    @pl.loop(0, n_rows)
    def _(r):
        give(r).wait()


def gelu(x):
    return x * (0.5 * (1.0 + jnp.tanh(0.7978845608028654 * (x + 0.044715 * (x * x * x)))))


def expert_kernel(cfg, meta, addr, tok_hbm, up_hbm, down_hbm, back, tok, recv, xbuf, ybuf, up, down, mix, xs, win, dsend, drecv, rsend, rrecv, wsem, tsem):
    n_dev, n_slot, part, stride = cfg['n_dev'], cfg['n_slot'], cfg['part'], cfg['stride']
    m_rows = n_dev * part
    n_tok, d_model, d_ff = tok.shape[0], up_hbm.shape[1], up_hbm.shape[2]
    first, last, disp, ret, ret_lo = cfg['first'], cfg['last'], cfg['disp'], cfg['ret'], cfg['ret_lo']
    n_step = -(-disp[-1] // STEP)
    f32, bf16, i32 = jnp.float32, jnp.bfloat16, jnp.int32
    me = lax.axis_index('ep')

    def fetch(s, b):
        return (pltpu.make_async_copy(up_hbm.at[s], up.at[b], wsem.at[0, b]), pltpu.make_async_copy(down_hbm.at[s], down.at[b], wsem.at[1, b]))

    load_tok = pltpu.make_async_copy(tok_hbm, tok, tsem)
    load_tok.start()
    group_barrier(n_dev, me)
    tail = n_step * (STEP // PACK)

    @pl.loop(0, n_dev)
    def _(k):
        xbuf[k, tail:] = jnp.zeros((xbuf.shape[1] - tail, PACK, d_model), bf16)

    def dispatch(j, k, peer, lo, num):
        return pltpu.make_async_remote_copy(src_ref=xbuf.at[k, pl.ds(lo, num)], dst_ref=recv.at[k, pl.ds(lo, num)], send_sem=dsend.at[j, k], recv_sem=drecv.at[j, k], device_id={'ep': peer}, device_id_type=MESH)

    def dispatched(j, k, peer):
        return dispatch(j, k, peer, disp[j] // PACK, (disp[j + 1] - disp[j]) // PACK)

    order = sorted(range(1, n_dev), key=lambda k: (abs(k - n_dev // 2), k))
    load_tok.wait()

    @pl.loop(0, n_step)
    def _(u):
        row = lax.broadcasted_iota(i32, (n_dev * STEP, LANES), 0)
        pos = lax.shift_right_logical(row, 5) * stride + (row & (STEP - 1)) + u * STEP
        want = pos + lax.shift_right_logical(pos, 3) * 40
        for q in range(n_tok // LANES):
            mix[:n_dev * STEP, q * LANES:(q + 1) * LANES] = (want == addr[q:q + 1, :]).astype(bf16)
        rows = jnp.dot(mix[:n_dev * STEP, :n_tok], tok[...], preferred_element_type=f32).astype(bf16)
        for k in range(n_dev):
            for h in range(STEP // PACK):
                at = k * STEP + h * PACK
                xbuf[k, u * (STEP // PACK) + h] = rows[at:at + PACK]
        for lo, hi, j in cfg['pieces']:
            @pl.when(u == -(-hi // STEP) - 1)
            def _():
                for k in order:
                    dispatch(j, k, lax.rem(me + k, n_dev), lo // PACK, (hi - lo) // PACK).start()

        @pl.when(u == 0)
        def _():
            for s in range(2):
                for copy in fetch(s, s):
                    copy.start()

    def ffn(s, b):
        unit = me * USTRIDE + s
        lane = lax.broadcasted_iota(i32, (1, n_dev * WIN), 1)
        which = lax.shift_right_logical(lane, 6)
        off = jnp.zeros((1, n_dev * WIN), i32)
        num = jnp.zeros((1, n_dev * WIN), i32)
        for k in range(n_dev):
            src = lax.rem(me + n_dev - k, n_dev)
            load, start = meta[src, unit], meta[n_dev + src, unit]
            blk = lax.shift_right_logical(start, 4)
            base = blk * PACK
            for q in range(WIN // PACK):
                win[k * WIN + q * PACK:k * WIN + (q + 1) * PACK, :] = xbuf[k, blk + q]
            off = jnp.where(which == k, base - start, off)
            num = jnp.where(which == k, load, num)
        nth = (lane & (WIN - 1)) + off
        target = jnp.where((nth >= 0) & (nth < num), nth + which * part, -1)
        pick = (lax.broadcasted_iota(i32, (m_rows, n_dev * WIN), 0) == target).astype(bf16)
        xs[...] = jnp.dot(pick, win[...], preferred_element_type=f32).astype(bf16)
        tile = 512
        for t in range(d_ff // tile):
            pre = jnp.dot(xs[...], up[b, :, t * tile:(t + 1) * tile], preferred_element_type=f32)
            mix[:, t * tile:(t + 1) * tile] = gelu(pre).astype(bf16)
        tile = 256
        for t in range(d_model // tile):
            o = jnp.dot(mix[:, :d_ff], down[b, :, t * tile:(t + 1) * tile], preferred_element_type=f32).astype(bf16)
            for k in range(n_dev):
                ybuf[k, pl.ds(pl.multiple_of(s * part, PACK), part), t * tile:(t + 1) * tile] = o[k * part:(k + 1) * part]

    def give_back(j, k):
        rows = pl.ds(ret[j] // PACK, (ret[j + 1] - ret[j]) // PACK)
        peer = lax.rem(me + n_dev - k, n_dev)
        return pltpu.make_async_remote_copy(src_ref=recv.at[k, rows], dst_ref=back.at[k, rows], send_sem=rsend.at[j, k], recv_sem=rrecv.at[j, k], device_id={'ep': peer}, device_id_type=MESH)

    def give_own(j):
        rows = pl.ds(ret[j] // PACK, (ret[j + 1] - ret[j]) // PACK)
        return pltpu.make_async_copy(recv.at[0, rows], back.at[0, rows], rrecv.at[j, 0])

    def combine(j):
        n_rows = ret[j + 1] - ret[j]
        n_win = last[j] + 1 - ret_lo[j]
        width = n_win * part

        @pl.loop(0, n_dev)
        def _(i):
            k = lax.rem(n_dev // 2 + 3 * i, n_dev)
            src = lax.rem(me + n_dev - k, n_dev)
            lane = lax.broadcasted_iota(i32, (1, width), 1)
            target = jnp.full((1, width), -1, i32)
            for w in range(n_win):
                unit = me * USTRIDE + ret_lo[j] + w
                load, start = meta[src, unit], meta[n_dev + src, unit]
                nth = lane - w * part
                target = jnp.where((nth >= 0) & (nth < load), nth + start, target)
            pick = (lax.broadcasted_iota(i32, (n_rows, width), 0) + ret[j] == target).astype(bf16)
            rows = ybuf[k, ret_lo[j] * part:(last[j] + 1) * part, :]
            mixed = jnp.dot(pick, rows, preferred_element_type=f32).astype(bf16)
            recv[k, ret[j] // PACK:ret[j + 1] // PACK] = mixed.reshape(n_rows // PACK, PACK, d_model)

            @pl.when(k == 0)
            def _():
                give_own(j).start()

            @pl.when(k != 0)
            def _():
                give_back(j, k).start()

    @pl.loop(0, n_slot)
    def _(s):
        for j in range(len(first)):
            @pl.when(s == first[j])
            def _():
                for k in range(1, n_dev):
                    dispatched(j, k, lax.rem(me + n_dev - k, n_dev)).wait_recv()
                    dispatched(j, k, lax.rem(me + k, n_dev)).wait_send()

                @pl.loop(1, n_dev)
                def _(k):
                    @pl.loop(disp[j] // PACK, disp[j + 1] // PACK)
                    def _(b):
                        xbuf[k, b] = recv[k, b]

        b = lax.rem(s, 2)
        for copy in fetch(s, b):
            copy.wait()
        ffn(s, b)

        @pl.when(s + 2 < n_slot)
        def _():
            for copy in fetch(s + 2, b):
                copy.start()

        for j in range(len(last)):
            @pl.when(s == last[j])
            def _():
                combine(j)

    for k in range(1, n_dev):
        for j in range(len(last)):
            give_back(j, k).wait_send()
            give_back(j, k).wait_recv()
    for j in range(len(last)):
        give_own(j).wait()


def plan(n_dev, n_slot, n_pairs, bound, stride, z, cap, returns):
    mean = n_pairs / (n_dev * n_slot)
    spread = 9.3 * mean / 30.1
    hi = [bound * (s + 1) for s in range(n_slot)]
    lo = [0] * n_slot
    if z is not None:
        hi = [min(hi[s], math.ceil(mean * (s + 1) + z * spread * math.sqrt(s + 1)), cap) for s in range(n_slot)]
        lo = [max(0, math.floor(mean * (s + 1) - (z - 0.5) * spread * math.sqrt(s + 1))) if s in returns[:-1] else 0 for s in range(n_slot)]
    disp = [0, cap] if z is None else list(range(0, cap - CHUNK, CHUNK)) + [cap]
    pieces = [(0, STEP, 0), (STEP, 2 * STEP, 0), (2 * STEP, disp[1], 0)]
    pieces += [(disp[j], disp[j + 1], j) for j in range(1, len(disp) - 1)]
    ret = [0] + [lo[s] // PACK * PACK for s in returns[:-1]] + [cap]
    ret_lo = [min(s for s in range(n_slot) if hi[s] > ret[j]) for j in range(len(returns))]
    first = [min((s for s in range(n_slot) if hi[s] > d), default=n_slot - 1) for d in disp[:-1]]
    return dict(n_dev=n_dev, n_slot=n_slot, cap=cap, stride=stride, pieces=pieces, lo=lo, hi=hi, first=first, last=list(returns), disp=disp, ret=ret, ret_lo=ret_lo, part=up_to(bound, PACK))


def solution(mesh):
    n_dev = mesh.shape['ep']

    def group_layer(tokens, topk_idx, topk_w, w_up, w_down, slot_expert):
        n_tok, d_model = tokens.shape
        n_slot = slot_expert.shape[1]
        d_ff = w_up.shape[3]
        n_pairs = n_tok * topk_idx.shape[1]
        base_load = n_pairs // (n_dev * n_slot)
        bound = base_load + base_load // 2 + 1
        mean = n_pairs // n_dev
        stride = up_to(n_slot * bound, PACK)
        caps = [min(stride, up_to(math.ceil(mean * f), PACK)) for f in TIERS]
        cuts = [n_slot * c // 17 - 1 for c in (9, 12, 14, 16, 17)]
        plans = [plan(n_dev, n_slot, n_pairs, bound, stride, 4.0, c, cuts) for c in caps]
        plans.append(plan(n_dev, n_slot, n_pairs, bound, stride, None, stride, [n_slot - 1]))
        wide_bounds = plan(n_dev, n_slot, n_pairs, bound, stride, 4.0, stride, cuts)
        n_rows = n_pairs // LANES
        n_units = n_dev * USTRIDE
        f32, bf16, i32 = jnp.float32, jnp.bfloat16, jnp.int32
        vmem = pl.BlockSpec(memory_space=pltpu.VMEM)
        smem = pl.BlockSpec(memory_space=pltpu.SMEM)
        hbm = pl.BlockSpec(memory_space=pl.ANY)
        big = 63 * 1024 * 1024

        addr, meta, flag = pl.pallas_call(
            functools.partial(route_kernel, n_dev, n_slot, stride, bound, wide_bounds['lo'], wide_bounds['hi'], caps),
            out_shape=[jax.ShapeDtypeStruct((n_rows, LANES), i32), jax.ShapeDtypeStruct((2 * n_dev, n_units), i32), jax.ShapeDtypeStruct((1, 1), i32)],
            in_specs=[vmem, smem],
            out_specs=[vmem, vmem, smem],
            scratch_shapes=[pltpu.VMEM((SUB, LANES), i32), pltpu.VMEM((n_dev, SUB, LANES), i32), pltpu.VMEM((n_rows, LANES), f32), pltpu.VMEM((n_units, LANES), i32), pltpu.VMEM((4 * n_dev, LANES), f32), pltpu.SemaphoreType.DMA((n_dev,)), pltpu.SemaphoreType.DMA((n_dev,))],
            compiler_params=pltpu.CompilerParams(collective_id=0, has_side_effects=True),
            name='route',
        )(topk_idx.reshape(n_rows, LANES), slot_expert)

        d_tiles = d_model // LANES
        wide = pltpu.VMEM((n_dev * stride * d_tiles, LANES), f32)
        tmp = pltpu.VMEM((LANES * d_tiles, LANES), f32)
        block = pltpu.VMEM((n_dev, stride // PACK, PACK, d_model), bf16)
        rows_vmem = pltpu.VMEM((n_tok, d_model), bf16)
        sem, sems = pltpu.SemaphoreType.DMA, pltpu.SemaphoreType.DMA((n_dev,))
        def run(cfg, meta, addr, tokens, w_up, w_down):
            part, cap = cfg['part'], cfg['cap']
            m_rows = n_dev * part
            sent = pltpu.SemaphoreType.DMA((len(cfg['first']), n_dev))
            given = pltpu.SemaphoreType.DMA((len(cfg['last']), n_dev))
            return pl.pallas_call(
                functools.partial(expert_kernel, cfg),
                out_shape=jax.ShapeDtypeStruct((n_dev, stride // PACK, PACK, d_model), bf16),
                in_specs=[smem, vmem, hbm, hbm, hbm],
                out_specs=hbm,
                scratch_shapes=[
                    rows_vmem,
                    pltpu.VMEM((n_dev, cap // PACK, PACK, d_model), bf16),
                    pltpu.VMEM((n_dev, (up_to(cap, STEP) + WIN) // PACK, PACK, d_model), bf16),
                    pltpu.VMEM((n_dev, n_slot * part, d_model), bf16),
                    pltpu.VMEM((2, d_model, d_ff), bf16),
                    pltpu.VMEM((2, d_ff, d_model), bf16),
                    pltpu.VMEM((m_rows, max(d_ff, n_tok)), bf16),
                    pltpu.VMEM((m_rows, d_model), bf16),
                    pltpu.VMEM((n_dev * WIN, d_model), bf16),
                    sent, sent, given, given,
                    pltpu.SemaphoreType.DMA((2, 2)),
                    sem,
                ],
                compiler_params=pltpu.CompilerParams(collective_id=1, has_side_effects=True, vmem_limit_bytes=big),
                name='experts',
            )(meta, addr, tokens, w_up, w_down)

        back = lax.switch(flag[0, 0], [functools.partial(run, p) for p in plans], meta, addr, tokens, w_up[0], w_down[0])

        return pl.pallas_call(
            functools.partial(unpack_kernel, caps[-1], len(caps)),
            out_shape=jax.ShapeDtypeStruct((n_tok, d_model), bf16),
            in_specs=[smem, smem, vmem, hbm],
            out_specs=hbm,
            scratch_shapes=[block, wide, tmp, rows_vmem, sems, sem],
            compiler_params=pltpu.CompilerParams(vmem_limit_bytes=big),
            name='unpack',
        )(addr, flag, topk_w.reshape(n_rows, LANES), back)

    row_spec = P(('dp', 'ep'), None)
    weight_spec = P('ep', None, None, None)
    return jax.shard_map(group_layer, mesh=mesh, in_specs=(row_spec, row_spec, row_spec, weight_spec, weight_spec, P(None, None)), out_specs=row_spec, check_vma=False)
```
